32 devices in a mesh: fsdp: 16 (over z, y, x), mat: 2 (over core).
Axes of the slice: x: 2, y: 2, z: 4, core: 2. Of those that a mesh axis runs over, the one named last changes fastest.
Arguments:
- momentum: float32 [8192, 4096], P(('mat', 'fsdp')), parts along dimension 0, may hold values from -6 to 6
- grad: bfloat16 [8192, 4096], P(('mat', 'fsdp')), parts along dimension 0, may hold values from -6 to 6
- q_basis: float32 [8192, 512], P(('mat', 'fsdp')), parts along dimension 0, may hold values from -6 to 6
Outputs:
- momentum_next: float32 [8192, 4096], P(('mat', 'fsdp')), parts along dimension 0
- update: bfloat16 [8192, 4096], P(('mat', 'fsdp')), parts along dimension 0
- q_next: float32 [8192, 512], P(('mat', 'fsdp')), parts along dimension 0
The draws below stay inside these ranges and needn't reach their ends.
There are 2 independent parts, one for each index of `mat`. The reference program is written for one: setup_inputs(seed, part) draws one part's arguments, and reference() takes and returns one part's arrays. A program takes and returns all parts, laid end to end along the dimension named above; each array names one. Nothing has to cross between parts.
All inputs are finite; a program needn't handle non-finite values.
Results may differ from the reference program's by a relative error of at most 0.0076.
Values may be sent and summed in bfloat16 or wider, within the bound.
A program may use at most 128 MiB of HBM per device.

```python
import math
import jax
import jax.numpy as jnp
from jax import lax

D = 4096
RANK = 512
ROWS = 4096


def with_spikes(drawn, stream_key, source, target, parts, factor):
    def block_of(axis_at):
        return (jnp.arange(drawn.shape[axis_at]) // (drawn.shape[axis_at] // parts)).reshape((-1,) + (1,) * (drawn.ndim - 1 - axis_at))

    first = jax.random.permutation(stream_key, parts)[block_of(target)]
    other_side = (block_of(target) + parts // 2) % parts
    return jnp.where((block_of(source) == first) | (block_of(source) == other_side), factor * drawn, drawn)


def block_levels(key, extent, split, least, high):
    loudness, own = 1.0, jax.random.fold_in(key, 6)
    for dim, shards_of in split:
        heights = jnp.exp(jax.random.uniform(jax.random.fold_in(own, dim), (shards_of,), jnp.float32, least / len(split), high / len(split)))
        loudness = loudness * jnp.repeat(heights, extent[dim] // shards_of).reshape([-1 if axis == dim else 1 for axis in range(len(extent))])
    return loudness


def bell_draw(own_key, shape, deviation, limit, shards=(), kind=jnp.bfloat16):
    entries = jax.random.normal(own_key, shape, jnp.float32) * deviation
    if len(shards) > 0:
        entries = block_levels(own_key, shape, shards, -0.22, 0.18) * entries
    return jnp.clip(entries, min=-limit, max=limit).astype(kind)


def heavy_noise(stream_key, dims, deviation, bound, pieces, heavy, kind=jnp.bfloat16):
    drawn = deviation * jax.random.normal(stream_key, dims, jnp.float32)
    if pieces:
        drawn = drawn * block_levels(stream_key, dims, pieces, -0.22, 0.18)
    return jnp.clip(with_spikes(drawn, jax.random.fold_in(stream_key, 3), *heavy), -bound, bound).astype(kind)


def setup_inputs(seed: int = 0, part: int = 0) -> dict:
    keys = jax.random.split(jax.random.key(seed), 4)
    part_splits = jax.random.split(jax.random.fold_in(keys[3], part), 4)
    return {
        "momentum": bell_draw(part_splits[0], (ROWS, D), 1.0, 6.0, ((0, 16),), jnp.float32),
        "grad": heavy_noise(part_splits[1], (ROWS, D), 1.0, 6.0, ((0, 16),), (0, 1, 16, 2.0)),
        "q_basis": bell_draw(part_splits[2], (D, RANK), 1.0, 6.0, ((0, 16),), jnp.float32),
    }


damping = 0.95
epsilon = 1e-06

def lower_inverse(gram_total):
    order_size = gram_total.shape[0]
    identity = jnp.eye(order_size, dtype=jnp.float32)
    ridge_term = 0.0001 * jnp.trace(gram_total) / order_size
    factor_lower = jnp.linalg.cholesky(gram_total + ridge_term * identity)
    return lax.linalg.triangular_solve(factor_lower, identity, left_side=True, lower=True)

def reference(momentum, grad, q_basis):
    blended = momentum + grad.astype(jnp.float32)
    projected = jnp.dot(blended.astype(jnp.bfloat16).astype(jnp.float32), q_basis.astype(jnp.bfloat16).astype(jnp.float32), preferred_element_type=jnp.float32)
    gram_total = jnp.dot(projected.T, projected, precision=lax.Precision.HIGHEST)
    inverse = lower_inverse(gram_total)
    orthonormal = jnp.dot(projected, inverse.T, precision=lax.Precision.HIGHEST)
    summed = jnp.dot(blended.T, orthonormal, precision=lax.Precision.HIGHEST)
    column_rms = jnp.sqrt(lax.optimization_barrier(jnp.mean(summed * summed, axis=0)) + epsilon)
    q_next = summed / column_rms
    q_low = q_next.astype(jnp.bfloat16)
    error_low = (orthonormal * column_rms).astype(jnp.bfloat16)
    ortho_low = orthonormal.astype(jnp.bfloat16)
    error_term = jnp.dot(error_low.astype(jnp.float32), q_low.T.astype(jnp.float32), preferred_element_type=jnp.float32)
    step_term = jnp.dot(ortho_low.astype(jnp.float32), q_low.T.astype(jnp.float32), preferred_element_type=jnp.float32)
    momentum_next = blended - (1.0 - damping) * error_term
    update = (math.sqrt(ROWS * D / RANK) * step_term).astype(jnp.bfloat16)
    return (momentum_next, update, q_next)
```

```python
import functools
import math

import jax
import jax.numpy as jnp
from jax import lax
from jax.experimental import pallas as pl
from jax.experimental.pallas import tpu as pltpu
from jax.sharding import PartitionSpec as P

damping = 0.95
epsilon = 1e-06
HIGHEST = lax.Precision.HIGHEST
MESH = pl.DeviceIdType.MESH


def grid_of(mesh):
    n = mesh.shape["fsdp"]
    at = list(mesh.axis_names).index("fsdp")
    try:
        line = mesh.devices.swapaxes(0, at).reshape(n, -1)[:, 0]
        spots = [tuple(d.coords) for d in line]
        axes = []
        for d in range(3):
            size = len({s[d] for s in spots})
            if size > 1:
                stride = next(i for i in range(n) if spots[i][d] != spots[0][d])
                axes.append((stride, size))
        sizes = [size for _, size in sorted(axes, reverse=True)]
        if math.prod(sizes) == n:
            return tuple([1] * (3 - len(sizes)) + sizes)
    except AttributeError:
        pass
    return (n // 4, 2, 2) if n % 4 == 0 else (1, 1, n)


def cut(rows, unit, sizes):
    units = rows // unit
    long_axis = max(range(3), key=lambda d: sizes[d])
    first, second = [d for d in range(3) if d != long_axis]
    tail = units // 8
    pairs = 2 if units >= 8 else 1
    share, extra = divmod(units - tail, 2 * pairs)
    plan = [(tail, (first, second, long_axis), 0)]
    for k in range(2 * pairs):
        short = (first, second) if k % 2 == 0 else (second, first)
        plan.append((share + (k < extra), (long_axis,) + short, k // 2))
    pieces, start = [], 0
    for count, order, wave in plan:
        if count:
            pieces.append((start, count * unit, order, wave))
        start += count * unit
    return pieces


def wavefront(pieces, phases):
    steps = [(piece[3] + phase, phase, p) for p, piece in enumerate(pieces) for phase in range(phases)]
    return [(phase, p) for _, phase, p in sorted(steps)]


def position(sizes):
    me = lax.axis_index("fsdp")
    return [
        lax.div(me, sizes[1] * sizes[2]),
        lax.rem(lax.div(me, sizes[2]), sizes[1]),
        lax.rem(me, sizes[2]),
    ]


def shifted(mine, sizes, d, off):
    return lax.rem(mine[d] + off, sizes[d])


def device_at(mine, sizes, d, coordinate):
    spot = list(mine)
    spot[d] = coordinate
    return {"fsdp": (spot[0] * sizes[1] + spot[1]) * sizes[2] + spot[2]}


def greet(mine, sizes):
    barrier = pltpu.get_barrier_semaphore()
    for d in range(3):
        for off in range(1, sizes[d]):
            target = device_at(mine, sizes, d, shifted(mine, sizes, d, off))
            pl.semaphore_signal(barrier, inc=1, device_id=target, device_id_type=MESH)
    pl.semaphore_wait(barrier, sum(sizes) - 3)


def gather_kernel(sizes, pieces, x_ref, o_ref, own_sem, send_sem, recv_sem):
    mine = position(sizes)
    own = pltpu.make_async_copy(x_ref, o_ref.at[mine[0], mine[1], mine[2]], own_sem)
    own.start()
    greet(mine, sizes)

    def block(piece, phase, coordinate):
        start, rows, order, _ = piece
        index = list(mine)
        index[order[phase]] = coordinate
        for d in order[:phase]:
            index[d] = slice(None)
        return o_ref.at[index[0], index[1], index[2], pl.ds(start, rows)]

    sent = []
    own_here = False
    for phase, p in wavefront(pieces, 3):
        piece = pieces[p]
        if phase:
            if not own_here:
                own.wait()
                own_here = True
            d = piece[2][phase - 1]
            for off in range(1, sizes[d]):
                landed = block(piece, phase - 1, shifted(mine, sizes, d, sizes[d] - off))
                pltpu.make_async_copy(landed, landed, recv_sem.at[p, phase - 1, off]).wait()
        d = piece[2][phase]
        for off in range(1, sizes[d]):
            target = block(piece, phase, mine[d])
            source = x_ref.at[pl.ds(piece[0], piece[1])] if phase == 0 else target
            copy = pltpu.make_async_remote_copy(
                src_ref=source,
                dst_ref=target,
                send_sem=send_sem.at[p, phase, off],
                recv_sem=recv_sem.at[p, phase, off],
                device_id=device_at(mine, sizes, d, shifted(mine, sizes, d, off)),
                device_id_type=MESH,
            )
            copy.start()
            sent.append(copy)
    for p, piece in enumerate(pieces):
        d = piece[2][2]
        for off in range(1, sizes[d]):
            landed = block(piece, 2, shifted(mine, sizes, d, sizes[d] - off))
            pltpu.make_async_copy(landed, landed, recv_sem.at[p, 2, off]).wait()
    for copy in sent:
        copy.wait_send()


def gather(x, sizes, number):
    rows, columns = x.shape
    unit = 8 if x.dtype == jnp.float32 else 16
    pieces = cut(rows, unit, sizes)
    sems = pltpu.SemaphoreType.DMA((len(pieces), 3, max(sizes)))
    out = pl.pallas_call(
        functools.partial(gather_kernel, sizes, pieces),
        out_shape=jax.ShapeDtypeStruct(sizes + (rows, columns), x.dtype),
        in_specs=[pl.BlockSpec(memory_space=pltpu.VMEM)],
        out_specs=pl.BlockSpec(memory_space=pltpu.VMEM),
        scratch_shapes=[pltpu.SemaphoreType.DMA, sems, sems],
        compiler_params=pltpu.CompilerParams(
            collective_id=number, has_side_effects=True, vmem_limit_bytes=32 * 2**20
        ),
        name=f"gather_{number}",
    )(x)
    return out.reshape(math.prod(sizes) * rows, columns)


def reduce_kernel(sizes, pieces, x_ref, o_ref, *scratch):
    mine = position(sizes)
    count = len(pieces)
    landing = scratch[: 3 * count]
    sums = scratch[3 * count : 5 * count]
    send_sem, recv_sem = scratch[5 * count :]
    greet(mine, sizes)
    sent = []

    def send(p, phase, d, off, source):
        copy = pltpu.make_async_remote_copy(
            src_ref=source,
            dst_ref=landing[3 * p + phase].at[off - 1],
            send_sem=send_sem.at[p, phase, off],
            recv_sem=recv_sem.at[p, phase, off],
            device_id=device_at(mine, sizes, d, shifted(mine, sizes, d, off)),
            device_id_type=MESH,
        )
        copy.start()
        sent.append(copy)

    def arrive(p, phase, d):
        for off in range(1, sizes[d]):
            here = landing[3 * p + phase].at[off - 1]
            pltpu.make_async_copy(here, here, recv_sem.at[p, phase, off]).wait()

    def begin(p, start, rows, order):
        d = order[2]
        for off in range(1, sizes[d]):
            index = [slice(None)] * 3
            index[d] = shifted(mine, sizes, d, off)
            send(p, 0, d, off, x_ref.at[index[0], index[1], index[2], pl.ds(start, rows)])

    def first_sums(p, start, rows, order):
        a, b, c = order
        arrive(p, 0, c)
        low, high = min(a, b), max(a, b)
        for off in list(range(1, sizes[b])) + [0]:
            at_b = shifted(mine, sizes, b, off)

            def one(at_a, _, off=off, at_b=at_b):
                index = [None] * 3
                index[a], index[b], index[c] = at_a, at_b, mine[c]
                total = x_ref[index[0], index[1], index[2], pl.ds(start, rows)].astype(jnp.float32)
                for k in range(sizes[c] - 1):
                    total += landing[3 * p][k, index[low], index[high]].astype(jnp.float32)
                if off:
                    sums[2 * p][off - 1, at_a] = total.astype(x_ref.dtype)
                else:
                    sums[2 * p + 1][at_a] = total
                return 0

            lax.fori_loop(0, sizes[a], one, 0)
        for off in range(1, sizes[b]):
            send(p, 1, b, off, sums[2 * p].at[off - 1])

    def second_sums(p, start, rows, order):
        a, b, c = order
        arrive(p, 1, b)
        for off in list(range(1, sizes[a])) + [0]:
            at_a = shifted(mine, sizes, a, off)
            total = sums[2 * p + 1][at_a]
            for k in range(sizes[b] - 1):
                total += landing[3 * p + 1][k, at_a].astype(jnp.float32)
            if off:
                landing[3 * p + 2][sizes[a] - 1 + off - 1] = total.astype(x_ref.dtype)
            else:
                sums[2 * p + 1][at_a] = total
        for off in range(1, sizes[a]):
            send(p, 2, a, off, landing[3 * p + 2].at[sizes[a] - 1 + off - 1])

    def last_sums(p, start, rows, order):
        a = order[0]
        arrive(p, 2, a)
        total = sums[2 * p + 1][mine[a]]
        for k in range(sizes[a] - 1):
            total += landing[3 * p + 2][k].astype(jnp.float32)
        o_ref[pl.ds(start, rows)] = total

    stages = (begin, first_sums, second_sums, last_sums)
    for phase, p in wavefront(pieces, 4):
        stages[phase](p, *pieces[p][:3])
    for copy in sent:
        copy.wait_send()


def reduce_scatter(x, sizes, number):
    n = math.prod(sizes)
    rows, columns = x.shape[0] // n, x.shape[1]
    unit = 8 if x.dtype == jnp.float32 else 16
    pieces = cut(rows, unit, sizes)
    landing, sums = [], []
    for _, part, (a, b, c), _ in pieces:
        low, high = min(a, b), max(a, b)
        many = lambda k: max(k, 1)
        landing += [
            pltpu.VMEM((many(sizes[c] - 1), sizes[low], sizes[high], part, columns), x.dtype),
            pltpu.VMEM((many(sizes[b] - 1), sizes[a], part, columns), x.dtype),
            pltpu.VMEM((many(2 * (sizes[a] - 1)), part, columns), x.dtype),
        ]
        sums += [
            pltpu.VMEM((many(sizes[b] - 1), sizes[a], part, columns), x.dtype),
            pltpu.VMEM((sizes[a], part, columns), jnp.float32),
        ]
    sems = pltpu.SemaphoreType.DMA((len(pieces), 3, max(sizes)))
    return pl.pallas_call(
        functools.partial(reduce_kernel, sizes, pieces),
        out_shape=jax.ShapeDtypeStruct((rows, columns), jnp.float32),
        in_specs=[pl.BlockSpec(memory_space=pltpu.VMEM)],
        out_specs=pl.BlockSpec(memory_space=pltpu.VMEM),
        scratch_shapes=landing + sums + [sems, sems],
        compiler_params=pltpu.CompilerParams(
            collective_id=number, has_side_effects=True, vmem_limit_bytes=40 * 2**20
        ),
        name=f"reduce_{number}",
    )(x.reshape(sizes + (rows, columns)))


def dot_first(left, right):
    return lax.dot_general(
        left, right, (((0,), (0,)), ((), ())), precision=HIGHEST, preferred_element_type=jnp.float32
    )


def three(x):
    high = x.astype(jnp.bfloat16).astype(jnp.float32)
    rest = x - high
    middle = rest.astype(jnp.bfloat16).astype(jnp.float32)
    return high, middle, rest - middle


def short_dot(left, right):
    h, m, l = three(left)
    lefts = jnp.concatenate([h, h, m, m, h, l], axis=0).astype(jnp.bfloat16)
    h, m, l = three(right)
    rights = jnp.concatenate([h, m, h, m, l, h], axis=0).astype(jnp.bfloat16)
    return lax.dot_general(
        lefts, rights, (((0,), (0,)), ((), ())), preferred_element_type=jnp.float32
    )


def nt_dot(left, right, precision=None):
    return lax.dot_general(
        left, right, (((1,), (1,)), ((), ())), precision=precision, preferred_element_type=jnp.float32
    )


def factor_block(width, d_ref, block):
    strip = lax.broadcasted_iota(jnp.int32, (8, width), 0)
    lane = lax.broadcasted_iota(jnp.int32, (8, width), 1)
    d_ref[:, :width] = block
    d_ref[:, width:] = jnp.where(
        lax.broadcasted_iota(jnp.int32, (width, width), 0)
        == lax.broadcasted_iota(jnp.int32, (width, width), 1),
        1.0,
        0.0,
    )

    def group(g, _):
        first = pl.multiple_of(g * 8, 8)
        left = d_ref[pl.ds(first, 8), :width]
        right = d_ref[pl.ds(first, 8), width:]
        turned = pltpu.roll(left, lax.rem(width - first, width), 1)
        columns = [jnp.broadcast_to(turned[:, j : j + 1], (8, width)) for j in range(8)]
        for j in range(8):
            scale = lax.rsqrt(columns[j][j : j + 1, :])
            factor = columns[j] * scale
            for m in range(j + 1, 8):
                columns[m] = columns[m] - factor * factor[m : m + 1, :]
            row_left, row_right = left[j : j + 1, :] * scale, right[j : j + 1, :] * scale
            below, here = strip > j, strip == j
            left = jnp.where(here, row_left, jnp.where(below, left - factor * row_left, left))
            right = jnp.where(here, row_right, jnp.where(below, right - factor * row_right, right))
        later = jnp.where(lane >= first + 8, left, 0.0)
        both = jnp.concatenate([left, right], axis=1)
        d_ref[pl.ds(first, 8), :] = both
        d_ref[...] = d_ref[...] - short_dot(later, both)
        return 0

    lax.fori_loop(0, width // 8, group, 0)
    return d_ref[:, width:]


def block_pieces(rank, width, sizes):
    long_axis = max(range(3), key=lambda d: sizes[d])
    first, second = [d for d in range(3) if d != long_axis]
    pieces = []
    for k in range(rank // width):
        half = width // 2
        pieces.append((k * width, half, (long_axis, first, second), k))
        pieces.append((k * width + half, half, (long_axis, second, first), k))
    return pieces


def factor_kernel(sizes, pieces, width, g_ref, p_ref, b_ref, o_ref, t_ref, q_ref, *scratch):
    mine = position(sizes)
    count = len(pieces)
    landing = scratch[: 3 * count]
    sums = scratch[3 * count : 5 * count]
    a_ref, x_ref, d_ref, terms, ot_ref, own_ref, rs_send, rs_recv, ag_send, ag_recv = scratch[5 * count :]
    size = g_ref.shape[0]
    blocks = size // width
    devices = math.prod(sizes)
    features = b_ref.shape[1] // devices
    rows = b_ref.shape[0]
    greet(mine, sizes)
    sent = []

    def push(source, target, sems, p, phase, d, off):
        copy = pltpu.make_async_remote_copy(
            src_ref=source,
            dst_ref=target,
            send_sem=sems[0].at[p, phase, off],
            recv_sem=sems[1].at[p, phase, off],
            device_id=device_at(mine, sizes, d, shifted(mine, sizes, d, off)),
            device_id_type=MESH,
        )
        copy.start()
        sent.append(copy)

    def send(p, phase, d, off, source):
        push(source, landing[3 * p + phase].at[off - 1], (rs_send, rs_recv), p, phase, d, off)

    def arrive(p, phase, d):
        for off in range(1, sizes[d]):
            here = landing[3 * p + phase].at[off - 1]
            pltpu.make_async_copy(here, here, rs_recv.at[p, phase, off]).wait()

    def begin(p, start, part, order):
        d = order[2]
        for off in range(1, sizes[d]):
            index = [slice(None)] * 3
            index[d] = shifted(mine, sizes, d, off)
            send(p, 0, d, off, terms.at[index[0], index[1], index[2], pl.ds(start, part)])

    def first_sums(p, start, part, order):
        a, b, c = order
        arrive(p, 0, c)
        low, high = min(a, b), max(a, b)
        for off in list(range(1, sizes[b])) + [0]:
            at_b = shifted(mine, sizes, b, off)

            def one(at_a, _, off=off, at_b=at_b):
                index = [None] * 3
                index[a], index[b], index[c] = at_a, at_b, mine[c]
                total = terms[index[0], index[1], index[2], pl.ds(start, part)].astype(jnp.float32)
                for k in range(sizes[c] - 1):
                    total += landing[3 * p][k, index[low], index[high]].astype(jnp.float32)
                if off:
                    sums[2 * p][off - 1, at_a] = total.astype(terms.dtype)
                else:
                    sums[2 * p + 1][at_a] = total
                return 0

            lax.fori_loop(0, sizes[a], one, 0)
        for off in range(1, sizes[b]):
            send(p, 1, b, off, sums[2 * p].at[off - 1])

    def second_sums(p, start, part, order):
        a, b, c = order
        arrive(p, 1, b)
        for off in list(range(1, sizes[a])) + [0]:
            at_a = shifted(mine, sizes, a, off)
            total = sums[2 * p + 1][at_a]
            for k in range(sizes[b] - 1):
                total += landing[3 * p + 1][k, at_a].astype(jnp.float32)
            if off:
                landing[3 * p + 2][sizes[a] - 1 + off - 1] = total.astype(terms.dtype)
            else:
                sums[2 * p + 1][at_a] = total
        for off in range(1, sizes[a]):
            send(p, 2, a, off, landing[3 * p + 2].at[sizes[a] - 1 + off - 1])

    def block(p, phase, coordinate):
        start, part, order, _ = pieces[p]
        index = list(mine)
        index[order[phase]] = coordinate
        for d in order[:phase]:
            index[d] = slice(None)
        return o_ref.at[index[0], index[1], index[2], pl.ds(start, part)]

    def spread(p, phase):
        d = pieces[p][2][phase]
        here = block(p, phase, mine[d])
        for off in range(1, sizes[d]):
            push(here, here, (ag_send, ag_recv), p, phase, d, off)

    def gathered(p, phase):
        d = pieces[p][2][phase]
        for off in range(1, sizes[d]):
            landed = block(p, phase, shifted(mine, sizes, d, sizes[d] - off))
            pltpu.make_async_copy(landed, landed, ag_recv.at[p, phase, off]).wait()

    def last_sums(p, start, part, order):
        a = order[0]
        arrive(p, 2, a)
        total = sums[2 * p + 1][mine[a]]
        for k in range(sizes[a] - 1):
            total += landing[3 * p + 2][k].astype(jnp.float32)
        own_ref[pl.ds(start, part), :] = total
        o_ref[mine[0], mine[1], mine[2], pl.ds(start, part)] = total.astype(o_ref.dtype)
        spread(p, 0)

    def pass_on(phase):
        def stage(p, start, part, order):
            gathered(p, phase - 1)
            spread(p, phase)

        return stage

    def finish(p, start, part, order):
        gathered(p, 2)

    stages = (begin, first_sums, second_sums, last_sums, pass_on(1), pass_on(2), finish)

    def serve(k, stage):
        for p, piece in enumerate(pieces):
            if piece[3] == k:
                stages[stage](p, *piece[:3])
        if stage == len(stages) - 1:
            scale_block(k)

    def scale_block(k):
        top, end = k * width, (k + 1) * width

        def squares(i, total):
            at = (lax.div(i, sizes[1] * sizes[2]), lax.rem(lax.div(i, sizes[2]), sizes[1]), lax.rem(i, sizes[2]))
            wide = o_ref[at[0], at[1], at[2], top:end].astype(jnp.float32)
            return total + wide * wide

        total = lax.fori_loop(0, devices, squares, jnp.zeros((width, features), jnp.float32))
        mean = jnp.sum(total, axis=1, keepdims=True) / (devices * features)
        column_rms = jnp.sqrt(mean + epsilon)
        q_ref[top:end, :] = own_ref[top:end, :] / column_rms
        t_ref[rows:, top:end] = (ot_ref[top:end, :] / column_rms).T.astype(t_ref.dtype)

    def factor(k):
        top, end = k * width, (k + 1) * width
        corner = factor_block(width, d_ref, a_ref[top:end, top:end])
        done = jnp.dot(corner, x_ref[top:end, :end], precision=HIGHEST)
        x_ref[top:end, :end] = done
        ortho = nt_dot(done, p_ref[:, :end], HIGHEST)
        ot_ref[top:end, :] = ortho
        t_ref[:rows, top:end] = ortho.T.astype(t_ref.dtype)
        low = ortho.astype(jnp.bfloat16)

        def one(i, _):
            at = (lax.div(i, sizes[1] * sizes[2]), lax.rem(lax.div(i, sizes[2]), sizes[1]), lax.rem(i, sizes[2]))
            lanes = pl.ds(pl.multiple_of(i * features, features), features)
            term = jnp.dot(low, b_ref[:, lanes], preferred_element_type=jnp.float32)
            terms[at[0], at[1], at[2], top:end] = term.astype(terms.dtype)
            return 0

        lax.fori_loop(0, devices, one, 0)
        serve(k, 0)
        if end < size:
            panel = jnp.dot(corner, a_ref[top:end, end:], precision=HIGHEST)
            a_ref[end:, end:] = a_ref[end:, end:] - dot_first(panel, panel)
            x_ref[end:, :end] = x_ref[end:, :end] - dot_first(panel, done)

    eye = lax.broadcasted_iota(jnp.int32, (size, size), 0) == lax.broadcasted_iota(
        jnp.int32, (size, size), 1
    )
    gram = g_ref[...]
    trace = jnp.sum(jnp.where(eye, gram, 0.0), keepdims=True)
    a_ref[...] = gram + jnp.where(eye, 0.0001 * trace / size, 0.0)
    x_ref[...] = jnp.where(eye, 1.0, 0.0)
    for slot in range(blocks + len(stages) - 1):
        if slot < blocks:
            factor(slot)
        for k in range(min(slot, blocks)):
            if 0 < slot - k < len(stages):
                serve(k, slot - k)
    for copy in sent:
        copy.wait_send()


def right_factor(gram_total, projected, blended_low, sizes, number):
    size = gram_total.shape[0]
    rows, columns = blended_low.shape
    width = 128
    devices = math.prod(sizes)
    features = columns // devices
    pieces = block_pieces(size, width, sizes)
    low_type = jnp.bfloat16
    landing, sums = [], []
    many = lambda k: max(k, 1)
    for _, part, (a, b, c), _ in pieces:
        low, high = min(a, b), max(a, b)
        landing += [
            pltpu.VMEM((many(sizes[c] - 1), sizes[low], sizes[high], part, features), low_type),
            pltpu.VMEM((many(sizes[b] - 1), sizes[a], part, features), low_type),
            pltpu.VMEM((many(2 * (sizes[a] - 1)), part, features), low_type),
        ]
        sums += [
            pltpu.VMEM((many(sizes[b] - 1), sizes[a], part, features), low_type),
            pltpu.VMEM((sizes[a], part, features), jnp.float32),
        ]
    sems = pltpu.SemaphoreType.DMA((len(pieces), 3, max(sizes)))
    vmem = pl.BlockSpec(memory_space=pltpu.VMEM)
    return pl.pallas_call(
        functools.partial(factor_kernel, sizes, pieces, width),
        out_shape=(
            jax.ShapeDtypeStruct(sizes + (size, features), low_type),
            jax.ShapeDtypeStruct((2 * rows, size), low_type),
            jax.ShapeDtypeStruct((size, features), jnp.float32),
        ),
        in_specs=[vmem, vmem, vmem],
        out_specs=(vmem, vmem, vmem),
        scratch_shapes=landing
        + sums
        + [
            pltpu.VMEM((size, size), jnp.float32),
            pltpu.VMEM((size, size), jnp.float32),
            pltpu.VMEM((width, 2 * width), jnp.float32),
            pltpu.VMEM(sizes + (size, features), low_type),
            pltpu.VMEM((size, rows), jnp.float32),
            pltpu.VMEM((size, features), jnp.float32),
            sems,
            sems,
            sems,
            sems,
        ],
        compiler_params=pltpu.CompilerParams(
            collective_id=number, has_side_effects=True, vmem_limit_bytes=40 * 2**20
        ),
        name=f"factor_{number}",
    )(gram_total, projected, blended_low)


def finish_kernel(step, factor, s_ref, t_ref, q_ref, m_ref, g_ref, mo_ref, uo_ref, qo_ref, m_buf, u_buf, q_buf, m_sem, u_sem, q_sem):
    rows = m_ref.shape[0]
    blocks, rank, features = s_ref.shape
    q_buf[...] = q_ref[...].T
    q_copy = pltpu.make_async_copy(q_buf, qo_ref, q_sem)
    q_copy.start()

    def copies(slot, i):
        lanes = pl.ds(pl.multiple_of(i * features, features), features)
        return (
            pltpu.make_async_copy(m_buf.at[slot], mo_ref.at[:, lanes], m_sem.at[slot]),
            pltpu.make_async_copy(u_buf.at[slot], uo_ref.at[:, lanes], u_sem.at[slot]),
        )

    slots = m_buf.shape[0]

    def one(i, _):
        slot = lax.rem(i, slots)

        @pl.when(i >= slots)
        def _():
            for copy in copies(slot, i - slots):
                copy.wait()

        lanes = pl.ds(pl.multiple_of(i * features, features), features)
        result = jnp.dot(t_ref[...], s_ref[i], preferred_element_type=jnp.float32)
        blended = m_ref[:, lanes] + g_ref[:, lanes].astype(jnp.float32)
        m_buf[slot] = blended - step * result[:rows]
        u_buf[slot] = (factor * result[rows:]).astype(u_buf.dtype)
        for copy in copies(slot, i):
            copy.start()
        return 0

    lax.fori_loop(0, blocks, one, 0)
    for i in range(max(blocks - slots, 0), blocks):
        for copy in copies(i % slots, i):
            copy.wait()
    q_copy.wait()


def finish(spread, stacked, turned, momentum, grad, factor):
    rows, columns = momentum.shape
    blocks, rank, features = spread.shape
    vmem = pl.BlockSpec(memory_space=pltpu.VMEM)
    anywhere = pl.BlockSpec(memory_space=pl.ANY)
    slots = 4
    return pl.pallas_call(
        functools.partial(finish_kernel, 1.0 - damping, factor),
        out_shape=(
            jax.ShapeDtypeStruct((rows, columns), jnp.float32),
            jax.ShapeDtypeStruct((rows, columns), jnp.bfloat16),
            jax.ShapeDtypeStruct((features, rank), jnp.float32),
        ),
        in_specs=[vmem] * 5,
        out_specs=(anywhere,) * 3,
        scratch_shapes=[
            pltpu.VMEM((slots, rows, features), jnp.float32),
            pltpu.VMEM((slots, rows, features), jnp.bfloat16),
            pltpu.VMEM((features, rank), jnp.float32),
            pltpu.SemaphoreType.DMA((slots,)),
            pltpu.SemaphoreType.DMA((slots,)),
            pltpu.SemaphoreType.DMA,
        ],
        compiler_params=pltpu.CompilerParams(vmem_limit_bytes=16 * 2**20),
        name="finish",
    )(spread, stacked, turned, momentum, grad)


def inverse_kernel(size, width, g_ref, x_ref, a_ref, d_ref):
    eye = lax.broadcasted_iota(jnp.int32, (size, size), 0) == lax.broadcasted_iota(
        jnp.int32, (size, size), 1
    )
    gram = g_ref[...]
    trace = jnp.sum(jnp.where(eye, gram, 0.0), keepdims=True)
    a_ref[...] = gram + jnp.where(eye, 0.0001 * trace / size, 0.0)
    x_ref[...] = jnp.where(eye, 1.0, 0.0)
    strip = lax.broadcasted_iota(jnp.int32, (8, width), 0)
    lane = lax.broadcasted_iota(jnp.int32, (8, width), 1)
    small_eye = jnp.where(
        lax.broadcasted_iota(jnp.int32, (width, width), 0)
        == lax.broadcasted_iota(jnp.int32, (width, width), 1),
        1.0,
        0.0,
    )

    def group(g, _):
        first = pl.multiple_of(g * 8, 8)
        left = d_ref[pl.ds(first, 8), :width]
        right = d_ref[pl.ds(first, 8), width:]
        turned = pltpu.roll(left, lax.rem(width - first, width), 1)
        columns = [jnp.broadcast_to(turned[:, j : j + 1], (8, width)) for j in range(8)]
        for j in range(8):
            scale = lax.rsqrt(columns[j][j : j + 1, :])
            factor = columns[j] * scale
            for m in range(j + 1, 8):
                columns[m] = columns[m] - factor * factor[m : m + 1, :]
            row_left, row_right = left[j : j + 1, :] * scale, right[j : j + 1, :] * scale
            below, here = strip > j, strip == j
            left = jnp.where(here, row_left, jnp.where(below, left - factor * row_left, left))
            right = jnp.where(here, row_right, jnp.where(below, right - factor * row_right, right))
        later = jnp.where(lane >= first + 8, left, 0.0)
        both = jnp.concatenate([left, right], axis=1)
        d_ref[pl.ds(first, 8), :] = both
        d_ref[...] = d_ref[...] - short_dot(later, both)
        return 0

    for k in range(size // width):
        top, end = k * width, (k + 1) * width
        d_ref[:, :width] = a_ref[top:end, top:end]
        d_ref[:, width:] = small_eye
        lax.fori_loop(0, width // 8, group, 0)
        corner = d_ref[:, width:]
        done = jnp.dot(corner, x_ref[top:end, :end], precision=HIGHEST)
        x_ref[top:end, :end] = done
        if end < size:
            panel = jnp.dot(corner, a_ref[top:end, end:], precision=HIGHEST)
            a_ref[end:, end:] = a_ref[end:, end:] - dot_first(panel, panel)
            x_ref[end:, :end] = x_ref[end:, :end] - dot_first(panel, done)


def lower_inverse(gram_total):
    size = gram_total.shape[0]
    width = 128
    return pl.pallas_call(
        functools.partial(inverse_kernel, size, width),
        out_shape=jax.ShapeDtypeStruct((size, size), jnp.float32),
        in_specs=[pl.BlockSpec(memory_space=pltpu.VMEM)],
        out_specs=pl.BlockSpec(memory_space=pltpu.VMEM),
        scratch_shapes=[
            pltpu.VMEM((size, size), jnp.float32),
            pltpu.VMEM((width, 2 * width), jnp.float32),
        ],
        compiler_params=pltpu.CompilerParams(vmem_limit_bytes=24 * 2**20),
        name="lower_inverse",
    )(gram_total)


def narrow_device(sizes, momentum, grad, q_basis):
    own_rows = momentum.shape[0]
    basis_rows, rank = q_basis.shape
    devices = math.prod(sizes)
    features = basis_rows * devices
    blended = momentum + grad.astype(jnp.float32)
    blended_low = blended.astype(jnp.bfloat16)
    basis = gather(q_basis.astype(jnp.bfloat16), sizes, 0)
    projected = jnp.dot(blended_low, basis, preferred_element_type=jnp.float32)
    local_gram = jnp.dot(projected.T, projected, precision=HIGHEST)
    gram_total = gather(reduce_scatter(local_gram, sizes, 1), sizes, 2)
    inverse = lower_inverse(gram_total)
    orthonormal = jnp.dot(projected, inverse.T, precision=HIGHEST)
    ortho_low = orthonormal.astype(jnp.bfloat16)
    terms = jnp.dot(blended_low.T, ortho_low, preferred_element_type=jnp.float32)
    summed = reduce_scatter(terms.astype(jnp.bfloat16), sizes, 3)
    summed_low = gather(summed.astype(jnp.bfloat16), sizes, 4)
    wide = summed_low.astype(jnp.float32)
    column_rms = jnp.sqrt(jnp.mean(wide * wide, axis=0) + epsilon)
    q_next = summed / column_rms
    stacked = jnp.concatenate(
        [ortho_low, (orthonormal / column_rms).astype(jnp.bfloat16)], axis=0
    )
    result = jnp.dot(stacked, summed_low.T, preferred_element_type=jnp.float32)
    total_rows = own_rows * devices
    momentum_next = blended - (1.0 - damping) * result[:own_rows]
    update = (math.sqrt(total_rows * features / rank) * result[own_rows:]).astype(jnp.bfloat16)
    return (momentum_next, update, q_next)


def per_device(sizes, momentum, grad, q_basis):
    own_rows = momentum.shape[0]
    basis_rows, rank = q_basis.shape
    if basis_rows % 128 or rank % 128:
        return narrow_device(sizes, momentum, grad, q_basis)
    devices = math.prod(sizes)
    features = basis_rows * devices
    blended = momentum + grad.astype(jnp.float32)
    blended_low = blended.astype(jnp.bfloat16)
    basis = gather(q_basis.astype(jnp.bfloat16), sizes, 0)
    projected = jnp.dot(blended_low, basis, preferred_element_type=jnp.float32)
    local_gram = jnp.dot(projected.T, projected, precision=HIGHEST)
    gram_total = gather(reduce_scatter(local_gram, sizes, 1), sizes, 2)
    spread, stacked, turned = right_factor(gram_total, projected, blended_low, sizes, 3)
    total_rows = own_rows * devices
    factor = math.sqrt(total_rows * features / rank)
    spread = spread.reshape(devices, rank, basis_rows)
    return finish(spread, stacked, turned, momentum, grad, factor)


def solution(mesh):
    spec = P(("mat", "fsdp"), None)
    return jax.shard_map(
        functools.partial(per_device, grid_of(mesh)),
        mesh=mesh,
        in_specs=(spec, spec, spec),
        out_specs=(spec, spec, spec),
        check_vma=False,
    )
```

```python
import functools
import math

import jax
import jax.numpy as jnp
from jax import lax
from jax.experimental import pallas as pl
from jax.experimental.pallas import tpu as pltpu
from jax.sharding import PartitionSpec as P

damping = 0.95
epsilon = 1e-06
HIGHEST = lax.Precision.HIGHEST
MESH = pl.DeviceIdType.MESH


def grid_of(mesh):
    n = mesh.shape["fsdp"]
    at = list(mesh.axis_names).index("fsdp")
    try:
        line = mesh.devices.swapaxes(0, at).reshape(n, -1)[:, 0]
        spots = [tuple(d.coords) for d in line]
        axes = []
        for d in range(3):
            size = len({s[d] for s in spots})
            if size > 1:
                stride = next(i for i in range(n) if spots[i][d] != spots[0][d])
                axes.append((stride, size))
        sizes = [size for _, size in sorted(axes, reverse=True)]
        if math.prod(sizes) == n:
            return tuple([1] * (3 - len(sizes)) + sizes)
    except AttributeError:
        pass
    return (n // 4, 2, 2) if n % 4 == 0 else (1, 1, n)


def cut(rows, unit, sizes):
    units = rows // unit
    long_axis = max(range(3), key=lambda d: sizes[d])
    first, second = [d for d in range(3) if d != long_axis]
    tail = units // 8
    pairs = 2 if units >= 8 else 1
    share, extra = divmod(units - tail, 2 * pairs)
    plan = [(tail, (first, second, long_axis), 0)]
    for k in range(2 * pairs):
        short = (first, second) if k % 2 == 0 else (second, first)
        plan.append((share + (k < extra), (long_axis,) + short, k // 2))
    pieces, start = [], 0
    for count, order, wave in plan:
        if count:
            pieces.append((start, count * unit, order, wave))
        start += count * unit
    return pieces


def wavefront(pieces, phases):
    steps = [(piece[3] + phase, phase, p) for p, piece in enumerate(pieces) for phase in range(phases)]
    return [(phase, p) for _, phase, p in sorted(steps)]


def position(sizes):
    me = lax.axis_index("fsdp")
    return [
        lax.div(me, sizes[1] * sizes[2]),
        lax.rem(lax.div(me, sizes[2]), sizes[1]),
        lax.rem(me, sizes[2]),
    ]


def shifted(mine, sizes, d, off):
    return lax.rem(mine[d] + off, sizes[d])


def device_at(mine, sizes, d, coordinate):
    spot = list(mine)
    spot[d] = coordinate
    return {"fsdp": (spot[0] * sizes[1] + spot[1]) * sizes[2] + spot[2]}


def greet(mine, sizes):
    barrier = pltpu.get_barrier_semaphore()
    for d in range(3):
        for off in range(1, sizes[d]):
            target = device_at(mine, sizes, d, shifted(mine, sizes, d, off))
            pl.semaphore_signal(barrier, inc=1, device_id=target, device_id_type=MESH)
    pl.semaphore_wait(barrier, sum(sizes) - 3)


def gather_kernel(sizes, pieces, x_ref, o_ref, own_sem, send_sem, recv_sem):
    mine = position(sizes)
    own = pltpu.make_async_copy(x_ref, o_ref.at[mine[0], mine[1], mine[2]], own_sem)
    own.start()
    greet(mine, sizes)

    def block(piece, phase, coordinate):
        start, rows, order, _ = piece
        index = list(mine)
        index[order[phase]] = coordinate
        for d in order[:phase]:
            index[d] = slice(None)
        return o_ref.at[index[0], index[1], index[2], pl.ds(start, rows)]

    sent = []
    own_here = False
    for phase, p in wavefront(pieces, 3):
        piece = pieces[p]
        if phase:
            if not own_here:
                own.wait()
                own_here = True
            d = piece[2][phase - 1]
            for off in range(1, sizes[d]):
                landed = block(piece, phase - 1, shifted(mine, sizes, d, sizes[d] - off))
                pltpu.make_async_copy(landed, landed, recv_sem.at[p, phase - 1, off]).wait()
        d = piece[2][phase]
        for off in range(1, sizes[d]):
            target = block(piece, phase, mine[d])
            source = x_ref.at[pl.ds(piece[0], piece[1])] if phase == 0 else target
            copy = pltpu.make_async_remote_copy(
                src_ref=source,
                dst_ref=target,
                send_sem=send_sem.at[p, phase, off],
                recv_sem=recv_sem.at[p, phase, off],
                device_id=device_at(mine, sizes, d, shifted(mine, sizes, d, off)),
                device_id_type=MESH,
            )
            copy.start()
            sent.append(copy)
    for p, piece in enumerate(pieces):
        d = piece[2][2]
        for off in range(1, sizes[d]):
            landed = block(piece, 2, shifted(mine, sizes, d, sizes[d] - off))
            pltpu.make_async_copy(landed, landed, recv_sem.at[p, 2, off]).wait()
    for copy in sent:
        copy.wait_send()


def gather(x, sizes, number):
    rows, columns = x.shape
    unit = 8 if x.dtype == jnp.float32 else 16
    pieces = cut(rows, unit, sizes)
    sems = pltpu.SemaphoreType.DMA((len(pieces), 3, max(sizes)))
    out = pl.pallas_call(
        functools.partial(gather_kernel, sizes, pieces),
        out_shape=jax.ShapeDtypeStruct(sizes + (rows, columns), x.dtype),
        in_specs=[pl.BlockSpec(memory_space=pltpu.VMEM)],
        out_specs=pl.BlockSpec(memory_space=pltpu.VMEM),
        scratch_shapes=[pltpu.SemaphoreType.DMA, sems, sems],
        compiler_params=pltpu.CompilerParams(
            collective_id=number, has_side_effects=True, vmem_limit_bytes=32 * 2**20
        ),
        name=f"gather_{number}",
    )(x)
    return out.reshape(math.prod(sizes) * rows, columns)


def reduce_kernel(sizes, pieces, x_ref, o_ref, *scratch):
    mine = position(sizes)
    count = len(pieces)
    landing = scratch[: 3 * count]
    sums = scratch[3 * count : 5 * count]
    send_sem, recv_sem = scratch[5 * count :]
    greet(mine, sizes)
    sent = []

    def send(p, phase, d, off, source):
        copy = pltpu.make_async_remote_copy(
            src_ref=source,
            dst_ref=landing[3 * p + phase].at[off - 1],
            send_sem=send_sem.at[p, phase, off],
            recv_sem=recv_sem.at[p, phase, off],
            device_id=device_at(mine, sizes, d, shifted(mine, sizes, d, off)),
            device_id_type=MESH,
        )
        copy.start()
        sent.append(copy)

    def arrive(p, phase, d):
        for off in range(1, sizes[d]):
            here = landing[3 * p + phase].at[off - 1]
            pltpu.make_async_copy(here, here, recv_sem.at[p, phase, off]).wait()

    def begin(p, start, rows, order):
        d = order[2]
        for off in range(1, sizes[d]):
            index = [slice(None)] * 3
            index[d] = shifted(mine, sizes, d, off)
            send(p, 0, d, off, x_ref.at[index[0], index[1], index[2], pl.ds(start, rows)])

    def first_sums(p, start, rows, order):
        a, b, c = order
        arrive(p, 0, c)
        low, high = min(a, b), max(a, b)
        for off in list(range(1, sizes[b])) + [0]:
            at_b = shifted(mine, sizes, b, off)

            def one(at_a, _, off=off, at_b=at_b):
                index = [None] * 3
                index[a], index[b], index[c] = at_a, at_b, mine[c]
                total = x_ref[index[0], index[1], index[2], pl.ds(start, rows)].astype(jnp.float32)
                for k in range(sizes[c] - 1):
                    total += landing[3 * p][k, index[low], index[high]].astype(jnp.float32)
                if off:
                    sums[2 * p][off - 1, at_a] = total.astype(x_ref.dtype)
                else:
                    sums[2 * p + 1][at_a] = total
                return 0

            lax.fori_loop(0, sizes[a], one, 0)
        for off in range(1, sizes[b]):
            send(p, 1, b, off, sums[2 * p].at[off - 1])

    def second_sums(p, start, rows, order):
        a, b, c = order
        arrive(p, 1, b)
        for off in list(range(1, sizes[a])) + [0]:
            at_a = shifted(mine, sizes, a, off)
            total = sums[2 * p + 1][at_a]
            for k in range(sizes[b] - 1):
                total += landing[3 * p + 1][k, at_a].astype(jnp.float32)
            if off:
                landing[3 * p + 2][sizes[a] - 1 + off - 1] = total.astype(x_ref.dtype)
            else:
                sums[2 * p + 1][at_a] = total
        for off in range(1, sizes[a]):
            send(p, 2, a, off, landing[3 * p + 2].at[sizes[a] - 1 + off - 1])

    def last_sums(p, start, rows, order):
        a = order[0]
        arrive(p, 2, a)
        total = sums[2 * p + 1][mine[a]]
        for k in range(sizes[a] - 1):
            total += landing[3 * p + 2][k].astype(jnp.float32)
        o_ref[pl.ds(start, rows)] = total

    stages = (begin, first_sums, second_sums, last_sums)
    for phase, p in wavefront(pieces, 4):
        stages[phase](p, *pieces[p][:3])
    for copy in sent:
        copy.wait_send()


def reduce_scatter(x, sizes, number):
    n = math.prod(sizes)
    rows, columns = x.shape[0] // n, x.shape[1]
    unit = 8 if x.dtype == jnp.float32 else 16
    pieces = cut(rows, unit, sizes)
    landing, sums = [], []
    for _, part, (a, b, c), _ in pieces:
        low, high = min(a, b), max(a, b)
        many = lambda k: max(k, 1)
        landing += [
            pltpu.VMEM((many(sizes[c] - 1), sizes[low], sizes[high], part, columns), x.dtype),
            pltpu.VMEM((many(sizes[b] - 1), sizes[a], part, columns), x.dtype),
            pltpu.VMEM((many(2 * (sizes[a] - 1)), part, columns), x.dtype),
        ]
        sums += [
            pltpu.VMEM((many(sizes[b] - 1), sizes[a], part, columns), x.dtype),
            pltpu.VMEM((sizes[a], part, columns), jnp.float32),
        ]
    sems = pltpu.SemaphoreType.DMA((len(pieces), 3, max(sizes)))
    return pl.pallas_call(
        functools.partial(reduce_kernel, sizes, pieces),
        out_shape=jax.ShapeDtypeStruct((rows, columns), jnp.float32),
        in_specs=[pl.BlockSpec(memory_space=pltpu.VMEM)],
        out_specs=pl.BlockSpec(memory_space=pltpu.VMEM),
        scratch_shapes=landing + sums + [sems, sems],
        compiler_params=pltpu.CompilerParams(
            collective_id=number, has_side_effects=True, vmem_limit_bytes=40 * 2**20
        ),
        name=f"reduce_{number}",
    )(x.reshape(sizes + (rows, columns)))


def dot_first(left, right):
    return lax.dot_general(
        left, right, (((0,), (0,)), ((), ())), precision=HIGHEST, preferred_element_type=jnp.float32
    )


def three(x):
    high = x.astype(jnp.bfloat16).astype(jnp.float32)
    rest = x - high
    middle = rest.astype(jnp.bfloat16).astype(jnp.float32)
    return high, middle, rest - middle


def short_dot(left, right):
    h, m, l = three(left)
    lefts = jnp.concatenate([h, h, m, m, h, l], axis=0).astype(jnp.bfloat16)
    h, m, l = three(right)
    rights = jnp.concatenate([h, m, h, m, l, h], axis=0).astype(jnp.bfloat16)
    return lax.dot_general(
        lefts, rights, (((0,), (0,)), ((), ())), preferred_element_type=jnp.float32
    )


def nt_dot(left, right, precision=None):
    return lax.dot_general(
        left, right, (((1,), (1,)), ((), ())), precision=precision, preferred_element_type=jnp.float32
    )


def factor_block(width, d_ref, block):
    strip = lax.broadcasted_iota(jnp.int32, (8, width), 0)
    lane = lax.broadcasted_iota(jnp.int32, (8, width), 1)
    d_ref[:, :width] = block
    d_ref[:, width:] = jnp.where(
        lax.broadcasted_iota(jnp.int32, (width, width), 0)
        == lax.broadcasted_iota(jnp.int32, (width, width), 1),
        1.0,
        0.0,
    )

    def group(g, _):
        first = pl.multiple_of(g * 8, 8)
        left = d_ref[pl.ds(first, 8), :width]
        right = d_ref[pl.ds(first, 8), width:]
        turned = pltpu.roll(left, lax.rem(width - first, width), 1)
        columns = [jnp.broadcast_to(turned[:, j : j + 1], (8, width)) for j in range(8)]
        for j in range(8):
            scale = lax.rsqrt(columns[j][j : j + 1, :])
            factor = columns[j] * scale
            for m in range(j + 1, 8):
                columns[m] = columns[m] - factor * factor[m : m + 1, :]
            row_left, row_right = left[j : j + 1, :] * scale, right[j : j + 1, :] * scale
            below, here = strip > j, strip == j
            left = jnp.where(here, row_left, jnp.where(below, left - factor * row_left, left))
            right = jnp.where(here, row_right, jnp.where(below, right - factor * row_right, right))
        later = jnp.where(lane >= first + 8, left, 0.0)
        both = jnp.concatenate([left, right], axis=1)
        d_ref[pl.ds(first, 8), :] = both
        d_ref[...] = d_ref[...] - short_dot(later, both)
        return 0

    lax.fori_loop(0, width // 8, group, 0)
    return d_ref[:, width:]


def split(rows, unit, sizes, k):
    units = rows // unit
    long_axis = max(range(3), key=lambda d: sizes[d])
    one, two = [d for d in range(3) if d != long_axis]
    if k % 2:
        one, two = two, one
    tail = units // 8
    share, extra = divmod(units - tail, 2)
    plan = ((tail, (one, two, long_axis)), (share + extra, (long_axis, one, two)), (share, (long_axis, two, one)))
    pieces, start = [], 0
    for count, order in plan:
        if count:
            pieces.append((start, count * unit, order))
        start += count * unit
    return pieces


def flows_of(blocks, width, basis_rows, sizes):
    long_axis = max(range(3), key=lambda d: sizes[d])
    one, two = [d for d in range(3) if d != long_axis]
    devices = math.prod(sizes)
    flows = []
    for k in range(blocks):
        flows += [("q", k) + piece for piece in split(basis_rows, 16, sizes, k)]
    for k in range(blocks):
        order = (long_axis, one, two) if k % 2 else (long_axis, two, one)
        flows.append(("g", k, 0, (k + 1) * width // devices, order))
    for k in range(blocks):
        flows += [("s", k, k * width + start, rows, order) for start, rows, order in split(width, 16, sizes, k)]
    return flows


def agenda(blocks):
    steps = []
    for k in range(blocks):
        for stage in range(4):
            steps.append((9.0 * k + (0, 6, 10, 16)[stage], 0, "q", k, stage))
        if k < blocks - 1:
            for stage in range(7):
                steps.append((9.0 * k + 17 + 3.0 * stage, 1, "g", k, stage))
    begun = 9.0 * (blocks - 1) + 17
    steps.append((begun + 0.1, 2, "trace", 0, 0))
    for k in range(blocks):
        start = begun + 4 + 8.5 * k
        steps.append((start, 3, "factor", k, 0))
        for stage in range(7):
            steps.append((start + 8.5 * stage + 0.1, 4, "s", k, stage))
    last = (0, 3, 12.4, 12.45, 20.9, 20.95, 29.4)
    for stage in range(7):
        steps.append((begun + last[stage], 1, "g", blocks - 1, stage))
    order = [step[2:] for step in sorted(steps)]
    for k in range(blocks):
        at = order.index(("factor", k, 0))
        late = [step for step in order[at:] if step[:2] == ("g", k)]
        order = [step for step in order if step not in late]
        at = order.index(("factor", k, 0))
        order[at:at] = late
    return order


def main_kernel(sizes, flows, width, m_ref, g_ref, q_ref, o_ref, t_ref, qn_ref, *scratch):
    mine = position(sizes)
    me = lax.axis_index("fsdp")
    devices = math.prod(sizes)
    rows, columns = m_ref.shape
    features, size = q_ref.shape
    blocks = size // width
    refs = list(scratch)
    take = lambda n: [refs.pop(0) for _ in range(n)]
    landing, sums = {}, {}
    for f, flow in enumerate(flows):
        if flow[0] != "q":
            landing[f] = take(3)
            sums[f] = take(2)
    grams = take(blocks)
    spreads = take(blocks)
    (m_buf, g_buf, q_buf, b_ref, basis, p_ref, trace_own, trace_all, u_ref, x_ref, d_ref) = take(11)
    (terms, ot_ref, own_ref, gram_ref) = take(4)
    (in_sem, trace_send, trace_recv, rs_send, rs_recv, ag_send, ag_recv) = take(7)
    base = [0, sizes[0] - 1, sizes[0] + sizes[1] - 2]
    each = sum(sizes) - 3

    loads = [
        pltpu.make_async_copy(q_ref, q_buf, in_sem.at[0]),
        pltpu.make_async_copy(m_ref, m_buf, in_sem.at[1]),
        pltpu.make_async_copy(g_ref, g_buf, in_sem.at[2]),
    ]
    for load in loads:
        load.start()
    barrier = pltpu.get_barrier_semaphore()
    for off in range(1, devices):
        other = {"fsdp": lax.rem(me + off, devices)}
        pl.semaphore_signal(barrier, inc=1, device_id=other, device_id_type=MESH)
    loads[0].wait()
    for k in range(blocks):
        basis[k, mine[0], mine[1], mine[2]] = q_buf[:, k * width : (k + 1) * width].astype(basis.dtype)
    pl.semaphore_wait(barrier, devices - 1)
    sent = []

    def push(source, target, sems, f, d, off):
        at = each * f + base[d] + off - 1
        copy = pltpu.make_async_remote_copy(
            src_ref=source,
            dst_ref=target,
            send_sem=sems[0].at[at],
            recv_sem=sems[1].at[at],
            device_id=device_at(mine, sizes, d, shifted(mine, sizes, d, off)),
            device_id_type=MESH,
        )
        copy.start()
        sent.append(copy)

    def landed(ref, sem, f, d, off):
        pltpu.make_async_copy(ref, ref, sem.at[each * f + base[d] + off - 1]).wait()

    def block(f, phase, coordinate):
        kind, k, start, part, order = flows[f]
        index = list(mine)
        index[order[phase]] = coordinate
        for d in order[:phase]:
            index[d] = slice(None)
        if kind == "q":
            return basis.at[k, index[0], index[1], index[2], pl.ds(start, part)]
        target = spreads[k] if kind == "g" else o_ref
        return target.at[index[0], index[1], index[2], pl.ds(start, part)]

    def spread(f, phase):
        d = flows[f][4][phase]
        here = block(f, phase, mine[d])
        for off in range(1, sizes[d]):
            push(here, here, (ag_send, ag_recv), f, d, off)

    def gathered(f, phase):
        d = flows[f][4][phase]
        for off in range(1, sizes[d]):
            landed(block(f, phase, shifted(mine, sizes, d, sizes[d] - off)), ag_recv, f, d, off)

    def source(f):
        return grams[flows[f][1]] if flows[f][0] == "g" else terms

    def begin(f):
        _, _, start, part, order = flows[f]
        d = order[2]
        for off in range(1, sizes[d]):
            index = [slice(None)] * 3
            index[d] = shifted(mine, sizes, d, off)
            piece = source(f).at[index[0], index[1], index[2], pl.ds(start, part)]
            push(piece, landing[f][0].at[off - 1], (rs_send, rs_recv), f, d, off)

    def first_sums(f):
        _, _, start, part, (a, b, c) = flows[f]
        from_ref = source(f)
        for off in range(1, sizes[c]):
            landed(landing[f][0].at[off - 1], rs_recv, f, c, off)
        low, high = min(a, b), max(a, b)
        for off in list(range(1, sizes[b])) + [0]:
            at_b = shifted(mine, sizes, b, off)

            def one(at_a, _, off=off, at_b=at_b):
                index = [None] * 3
                index[a], index[b], index[c] = at_a, at_b, mine[c]
                total = from_ref[index[0], index[1], index[2], pl.ds(start, part)].astype(jnp.float32)
                for k in range(sizes[c] - 1):
                    total += landing[f][0][k, index[low], index[high]].astype(jnp.float32)
                if off:
                    sums[f][0][off - 1, at_a] = total.astype(from_ref.dtype)
                else:
                    sums[f][1][at_a] = total
                return 0

            lax.fori_loop(0, sizes[a], one, 0)
        for off in range(1, sizes[b]):
            push(sums[f][0].at[off - 1], landing[f][1].at[off - 1], (rs_send, rs_recv), f, b, off)

    def second_sums(f):
        _, _, start, part, (a, b, c) = flows[f]
        for off in range(1, sizes[b]):
            landed(landing[f][1].at[off - 1], rs_recv, f, b, off)
        last = landing[f][2]
        for off in list(range(1, sizes[a])) + [0]:
            at_a = shifted(mine, sizes, a, off)
            total = sums[f][1][at_a]
            for k in range(sizes[b] - 1):
                total += landing[f][1][k, at_a].astype(jnp.float32)
            if off:
                last[sizes[a] - 1 + off - 1] = total.astype(last.dtype)
            else:
                sums[f][1][at_a] = total
        for off in range(1, sizes[a]):
            push(last.at[sizes[a] - 1 + off - 1], last.at[off - 1], (rs_send, rs_recv), f, a, off)

    def last_sums(f):
        kind, k, start, part, (a, b, c) = flows[f]
        for off in range(1, sizes[a]):
            landed(landing[f][2].at[off - 1], rs_recv, f, a, off)
        total = sums[f][1][mine[a]]
        for n in range(sizes[a] - 1):
            total += landing[f][2][n].astype(jnp.float32)
        if kind == "s":
            own_ref[pl.ds(start, part), :] = total
            o_ref[mine[0], mine[1], mine[2], pl.ds(start, part)] = total.astype(o_ref.dtype)
        else:
            spreads[k][mine[0], mine[1], mine[2]] = total

    def spot(i):
        return (
            lax.div(i, sizes[1] * sizes[2]),
            lax.rem(lax.div(i, sizes[2]), sizes[1]),
            lax.rem(i, sizes[2]),
        )

    def lanes_of(i):
        return pl.ds(pl.multiple_of(i * features, features), features)

    def blend():
        loads[1].wait()
        loads[2].wait()

        def one(i, _):
            lanes = lanes_of(i)
            b_ref[:, lanes] = (m_buf[:, lanes] + g_buf[:, lanes].astype(jnp.float32)).astype(b_ref.dtype)
            return 0

        lax.fori_loop(0, devices, one, 0)

    def project(k):
        top, end = k * width, (k + 1) * width

        def one(i, total):
            at = spot(i)
            return total + jnp.dot(
                b_ref[:, lanes_of(i)], basis[k, at[0], at[1], at[2]], preferred_element_type=jnp.float32
            )

        p_ref[:, top:end] = lax.fori_loop(0, devices, one, jnp.zeros((rows, width), jnp.float32))
        column = dot_first(p_ref[:, :end], p_ref[:, top:end])
        part = end // devices
        for i in range(devices):
            at = (i // (sizes[1] * sizes[2]), i // sizes[2] % sizes[1], i % sizes[2])
            grams[k][at[0], at[1], at[2]] = column[i * part : (i + 1) * part]

    def send_trace():
        square = p_ref[...] * p_ref[...]
        folded = square[:, :128]
        for i in range(1, size // 128):
            folded = folded + square[:, i * 128 : (i + 1) * 128]
        tile = folded[:8]
        for i in range(1, rows // 8):
            tile = tile + folded[i * 8 : (i + 1) * 8]
        trace_own[...] = tile
        trace_all[me] = tile
        for off in range(1, devices):
            copy = pltpu.make_async_remote_copy(
                src_ref=trace_own,
                dst_ref=trace_all.at[me],
                send_sem=trace_send.at[off],
                recv_sem=trace_recv.at[off],
                device_id={"fsdp": lax.rem(me + off, devices)},
                device_id_type=MESH,
            )
            copy.start()
            sent.append(copy)

    def ridge():
        for off in range(1, devices):
            here = trace_all.at[lax.rem(me + devices - off, devices)]
            pltpu.make_async_copy(here, here, trace_recv.at[off]).wait()
        return jnp.sum(jnp.sum(trace_all[...], axis=0), keepdims=True) * (0.0001 / size)

    small_eye = lax.broadcasted_iota(jnp.int32, (width, width), 0) == lax.broadcasted_iota(
        jnp.int32, (width, width), 1
    )
    shared = {}

    def factor(k):
        top, end = k * width, (k + 1) * width
        if k == 0:
            shared["ridge"] = ridge()
        gram_ref[:end, :] = spreads[k][...].reshape(end, width)
        for j in range(k):
            near, far = j * width, (j + 1) * width
            upper = gram_ref[near:far, :]
            if j:
                upper = upper - dot_first(u_ref[:near, near:far], u_ref[:near, top:end])
            u_ref[near:far, top:end] = jnp.dot(x_ref[near:far, near:far], upper, precision=HIGHEST)
        corner = gram_ref[top:end, :] + jnp.where(small_eye, shared["ridge"], 0.0)
        if k:
            panel = u_ref[:top, top:end]
            corner = corner - dot_first(panel, panel)
        inverse = factor_block(width, d_ref, corner)
        x_ref[top:end, top:end] = inverse
        if k:
            rest = dot_first(u_ref[:top, top:end], x_ref[:top, :top])
            x_ref[top:end, :top] = -jnp.dot(inverse, rest, precision=HIGHEST)
        if end < size:
            x_ref[top:end, end:] = jnp.zeros((width, size - end), jnp.float32)
        ortho = nt_dot(x_ref[top:end, :end], p_ref[:, :end], HIGHEST)
        ot_ref[top:end, :] = ortho
        t_ref[:rows, top:end] = ortho.T.astype(t_ref.dtype)
        low = ortho.astype(jnp.bfloat16)

        def one(i, _):
            at = spot(i)
            term = jnp.dot(low, b_ref[:, lanes_of(i)], preferred_element_type=jnp.float32)
            terms[at[0], at[1], at[2], top:end] = term.astype(terms.dtype)
            return 0

        lax.fori_loop(0, devices, one, 0)

    def scale_block(k):
        top, end = k * width, (k + 1) * width

        def squares(i, total):
            at = spot(i)
            wide = o_ref[at[0], at[1], at[2], top:end].astype(jnp.float32)
            return total + wide * wide

        total = lax.fori_loop(0, devices, squares, jnp.zeros((width, features), jnp.float32))
        mean = jnp.sum(total, axis=1, keepdims=True) / (devices * features)
        column_rms = jnp.sqrt(mean + epsilon)
        qn_ref[top:end, :] = own_ref[top:end, :] / column_rms
        t_ref[rows:, top:end] = (ot_ref[top:end, :] / column_rms).T.astype(t_ref.dtype)

    def serve(kind, k, stage):
        mine_flows = [f for f, flow in enumerate(flows) if flow[:2] == (kind, k)]
        if kind != "q":
            for f in mine_flows:
                if stage < 4:
                    (begin, first_sums, second_sums, last_sums)[stage](f)
            stage = stage - 4
            if stage < -1:
                return
            if stage == -1:
                for f in mine_flows:
                    spread(f, 0)
                return
            stage = stage + 1
        for f in mine_flows:
            if stage:
                gathered(f, stage - 1)
            if stage < 3:
                spread(f, stage)
        if stage == 3 and kind == "q":
            project(k)
        if stage == 3 and kind == "s":
            scale_block(k)

    blended = False
    for kind, k, stage in agenda(blocks):
        if kind == "trace":
            send_trace()
        elif kind == "factor":
            factor(k)
        else:
            serve(kind, k, stage)
        if not blended and kind == "q" and stage == 0:
            blend()
            blended = True
    for copy in sent:
        copy.wait_send()


def right_factor(momentum, grad, q_basis, sizes, number):
    rows, columns = momentum.shape
    features, size = q_basis.shape
    width = 128
    blocks = size // width
    devices = math.prod(sizes)
    flows = flows_of(blocks, width, features, sizes)
    low_type = jnp.bfloat16
    many = lambda k: max(k, 1)
    scratch = []
    for kind, _, _, part, (a, b, c) in flows:
        if kind == "q":
            continue
        low, high = min(a, b), max(a, b)
        lanes, kept = (width, jnp.float32) if kind == "g" else (features, low_type)
        scratch += [
            pltpu.VMEM((many(sizes[c] - 1), sizes[low], sizes[high], part, lanes), kept),
            pltpu.VMEM((many(sizes[b] - 1), sizes[a], part, lanes), kept),
            pltpu.VMEM((many(2 * (sizes[a] - 1)), part, lanes), kept),
            pltpu.VMEM((many(sizes[b] - 1), sizes[a], part, lanes), kept),
            pltpu.VMEM((sizes[a], part, lanes), jnp.float32),
        ]
    parts = [pltpu.VMEM(sizes + ((k + 1) * width // devices, width), jnp.float32) for k in range(blocks)]
    sems = pltpu.SemaphoreType.DMA((len(flows) * (sum(sizes) - 3),))
    scratch += parts + parts
    scratch += [
        pltpu.VMEM((rows, columns), jnp.float32),
        pltpu.VMEM((rows, columns), low_type),
        pltpu.VMEM((features, size), jnp.float32),
        pltpu.VMEM((rows, columns), low_type),
        pltpu.VMEM((blocks,) + sizes + (features, width), low_type),
        pltpu.VMEM((rows, size), jnp.float32),
        pltpu.VMEM((8, 128), jnp.float32),
        pltpu.VMEM((devices, 8, 128), jnp.float32),
        pltpu.VMEM((size, size), jnp.float32),
        pltpu.VMEM((size, size), jnp.float32),
        pltpu.VMEM((width, 2 * width), jnp.float32),
        pltpu.VMEM(sizes + (size, features), low_type),
        pltpu.VMEM((size, rows), jnp.float32),
        pltpu.VMEM((size, features), jnp.float32),
        pltpu.VMEM((size, width), jnp.float32),
        pltpu.SemaphoreType.DMA((3,)),
        pltpu.SemaphoreType.DMA((devices,)),
        pltpu.SemaphoreType.DMA((devices,)),
        sems,
        sems,
        sems,
        sems,
    ]
    vmem = pl.BlockSpec(memory_space=pltpu.VMEM)
    anywhere = pl.BlockSpec(memory_space=pl.ANY)
    return pl.pallas_call(
        functools.partial(main_kernel, sizes, flows, width),
        out_shape=(
            jax.ShapeDtypeStruct(sizes + (size, features), low_type),
            jax.ShapeDtypeStruct((2 * rows, size), low_type),
            jax.ShapeDtypeStruct((size, features), jnp.float32),
        ),
        in_specs=[anywhere] * 3,
        out_specs=(vmem, vmem, vmem),
        scratch_shapes=scratch,
        compiler_params=pltpu.CompilerParams(
            collective_id=number, has_side_effects=True, vmem_limit_bytes=50 * 2**20
        ),
        name=f"factor_{number}",
    )(momentum, grad, q_basis)


def finish_kernel(step, factor, s_ref, t_ref, q_ref, m_ref, g_ref, mo_ref, uo_ref, qo_ref, m_buf, u_buf, q_buf, m_sem, u_sem, q_sem):
    rows = m_ref.shape[0]
    blocks, rank, features = s_ref.shape
    q_buf[...] = q_ref[...].T
    q_copy = pltpu.make_async_copy(q_buf, qo_ref, q_sem)
    q_copy.start()

    def copies(slot, i):
        lanes = pl.ds(pl.multiple_of(i * features, features), features)
        return (
            pltpu.make_async_copy(m_buf.at[slot], mo_ref.at[:, lanes], m_sem.at[slot]),
            pltpu.make_async_copy(u_buf.at[slot], uo_ref.at[:, lanes], u_sem.at[slot]),
        )

    slots = m_buf.shape[0]

    def one(i, _):
        slot = lax.rem(i, slots)

        @pl.when(i >= slots)
        def _():
            for copy in copies(slot, i - slots):
                copy.wait()

        lanes = pl.ds(pl.multiple_of(i * features, features), features)
        result = jnp.dot(t_ref[...], s_ref[i], preferred_element_type=jnp.float32)
        blended = m_ref[:, lanes] + g_ref[:, lanes].astype(jnp.float32)
        m_buf[slot] = blended - step * result[:rows]
        u_buf[slot] = (factor * result[rows:]).astype(u_buf.dtype)
        for copy in copies(slot, i):
            copy.start()
        return 0

    lax.fori_loop(0, blocks, one, 0)
    for i in range(max(blocks - slots, 0), blocks):
        for copy in copies(i % slots, i):
            copy.wait()
    q_copy.wait()


def finish(spread, stacked, turned, momentum, grad, factor):
    rows, columns = momentum.shape
    blocks, rank, features = spread.shape
    vmem = pl.BlockSpec(memory_space=pltpu.VMEM)
    anywhere = pl.BlockSpec(memory_space=pl.ANY)
    slots = 4
    return pl.pallas_call(
        functools.partial(finish_kernel, 1.0 - damping, factor),
        out_shape=(
            jax.ShapeDtypeStruct((rows, columns), jnp.float32),
            jax.ShapeDtypeStruct((rows, columns), jnp.bfloat16),
            jax.ShapeDtypeStruct((features, rank), jnp.float32),
        ),
        in_specs=[vmem] * 5,
        out_specs=(anywhere,) * 3,
        scratch_shapes=[
            pltpu.VMEM((slots, rows, features), jnp.float32),
            pltpu.VMEM((slots, rows, features), jnp.bfloat16),
            pltpu.VMEM((features, rank), jnp.float32),
            pltpu.SemaphoreType.DMA((slots,)),
            pltpu.SemaphoreType.DMA((slots,)),
            pltpu.SemaphoreType.DMA,
        ],
        compiler_params=pltpu.CompilerParams(vmem_limit_bytes=16 * 2**20),
        name="finish",
    )(spread, stacked, turned, momentum, grad)


def inverse_kernel(size, width, g_ref, x_ref, a_ref, d_ref):
    eye = lax.broadcasted_iota(jnp.int32, (size, size), 0) == lax.broadcasted_iota(
        jnp.int32, (size, size), 1
    )
    gram = g_ref[...]
    trace = jnp.sum(jnp.where(eye, gram, 0.0), keepdims=True)
    a_ref[...] = gram + jnp.where(eye, 0.0001 * trace / size, 0.0)
    x_ref[...] = jnp.where(eye, 1.0, 0.0)
    strip = lax.broadcasted_iota(jnp.int32, (8, width), 0)
    lane = lax.broadcasted_iota(jnp.int32, (8, width), 1)
    small_eye = jnp.where(
        lax.broadcasted_iota(jnp.int32, (width, width), 0)
        == lax.broadcasted_iota(jnp.int32, (width, width), 1),
        1.0,
        0.0,
    )

    def group(g, _):
        first = pl.multiple_of(g * 8, 8)
        left = d_ref[pl.ds(first, 8), :width]
        right = d_ref[pl.ds(first, 8), width:]
        turned = pltpu.roll(left, lax.rem(width - first, width), 1)
        columns = [jnp.broadcast_to(turned[:, j : j + 1], (8, width)) for j in range(8)]
        for j in range(8):
            scale = lax.rsqrt(columns[j][j : j + 1, :])
            factor = columns[j] * scale
            for m in range(j + 1, 8):
                columns[m] = columns[m] - factor * factor[m : m + 1, :]
            row_left, row_right = left[j : j + 1, :] * scale, right[j : j + 1, :] * scale
            below, here = strip > j, strip == j
            left = jnp.where(here, row_left, jnp.where(below, left - factor * row_left, left))
            right = jnp.where(here, row_right, jnp.where(below, right - factor * row_right, right))
        later = jnp.where(lane >= first + 8, left, 0.0)
        both = jnp.concatenate([left, right], axis=1)
        d_ref[pl.ds(first, 8), :] = both
        d_ref[...] = d_ref[...] - short_dot(later, both)
        return 0

    for k in range(size // width):
        top, end = k * width, (k + 1) * width
        d_ref[:, :width] = a_ref[top:end, top:end]
        d_ref[:, width:] = small_eye
        lax.fori_loop(0, width // 8, group, 0)
        corner = d_ref[:, width:]
        done = jnp.dot(corner, x_ref[top:end, :end], precision=HIGHEST)
        x_ref[top:end, :end] = done
        if end < size:
            panel = jnp.dot(corner, a_ref[top:end, end:], precision=HIGHEST)
            a_ref[end:, end:] = a_ref[end:, end:] - dot_first(panel, panel)
            x_ref[end:, :end] = x_ref[end:, :end] - dot_first(panel, done)


def lower_inverse(gram_total):
    size = gram_total.shape[0]
    width = 128
    return pl.pallas_call(
        functools.partial(inverse_kernel, size, width),
        out_shape=jax.ShapeDtypeStruct((size, size), jnp.float32),
        in_specs=[pl.BlockSpec(memory_space=pltpu.VMEM)],
        out_specs=pl.BlockSpec(memory_space=pltpu.VMEM),
        scratch_shapes=[
            pltpu.VMEM((size, size), jnp.float32),
            pltpu.VMEM((width, 2 * width), jnp.float32),
        ],
        compiler_params=pltpu.CompilerParams(vmem_limit_bytes=24 * 2**20),
        name="lower_inverse",
    )(gram_total)


def narrow_device(sizes, momentum, grad, q_basis):
    own_rows = momentum.shape[0]
    basis_rows, rank = q_basis.shape
    devices = math.prod(sizes)
    features = basis_rows * devices
    blended = momentum + grad.astype(jnp.float32)
    blended_low = blended.astype(jnp.bfloat16)
    basis = gather(q_basis.astype(jnp.bfloat16), sizes, 0)
    projected = jnp.dot(blended_low, basis, preferred_element_type=jnp.float32)
    local_gram = jnp.dot(projected.T, projected, precision=HIGHEST)
    gram_total = gather(reduce_scatter(local_gram, sizes, 1), sizes, 2)
    inverse = lower_inverse(gram_total)
    orthonormal = jnp.dot(projected, inverse.T, precision=HIGHEST)
    ortho_low = orthonormal.astype(jnp.bfloat16)
    terms = jnp.dot(blended_low.T, ortho_low, preferred_element_type=jnp.float32)
    summed = reduce_scatter(terms.astype(jnp.bfloat16), sizes, 3)
    summed_low = gather(summed.astype(jnp.bfloat16), sizes, 4)
    wide = summed_low.astype(jnp.float32)
    column_rms = jnp.sqrt(jnp.mean(wide * wide, axis=0) + epsilon)
    q_next = summed / column_rms
    stacked = jnp.concatenate(
        [ortho_low, (orthonormal / column_rms).astype(jnp.bfloat16)], axis=0
    )
    result = jnp.dot(stacked, summed_low.T, preferred_element_type=jnp.float32)
    total_rows = own_rows * devices
    momentum_next = blended - (1.0 - damping) * result[:own_rows]
    update = (math.sqrt(total_rows * features / rank) * result[own_rows:]).astype(jnp.bfloat16)
    return (momentum_next, update, q_next)


def per_device(sizes, momentum, grad, q_basis):
    own_rows = momentum.shape[0]
    basis_rows, rank = q_basis.shape
    if basis_rows % 128 or rank % 128 or own_rows % 128:
        return narrow_device(sizes, momentum, grad, q_basis)
    devices = math.prod(sizes)
    features = basis_rows * devices
    spread, stacked, turned = right_factor(momentum, grad, q_basis, sizes, 0)
    total_rows = own_rows * devices
    factor = math.sqrt(total_rows * features / rank)
    spread = spread.reshape(devices, rank, basis_rows)
    return finish(spread, stacked, turned, momentum, grad, factor)


def solution(mesh):
    spec = P(("mat", "fsdp"), None)
    return jax.shard_map(
        functools.partial(per_device, grid_of(mesh)),
        mesh=mesh,
        in_specs=(spec, spec, spec),
        out_specs=(spec, spec, spec),
        check_vma=False,
    )
```

```python
import functools
import math

import jax
import jax.numpy as jnp
from jax import lax
from jax.experimental import pallas as pl
from jax.experimental.pallas import tpu as pltpu
from jax.sharding import PartitionSpec as P

damping = 0.95
epsilon = 1e-06
HIGHEST = lax.Precision.HIGHEST
MESH = pl.DeviceIdType.MESH


def grid_of(mesh):
    n = mesh.shape["fsdp"]
    at = list(mesh.axis_names).index("fsdp")
    try:
        line = mesh.devices.swapaxes(0, at).reshape(n, -1)[:, 0]
        spots = [tuple(d.coords) for d in line]
        axes = []
        for d in range(3):
            size = len({s[d] for s in spots})
            if size > 1:
                stride = next(i for i in range(n) if spots[i][d] != spots[0][d])
                axes.append((stride, size))
        sizes = [size for _, size in sorted(axes, reverse=True)]
        if math.prod(sizes) == n:
            return tuple([1] * (3 - len(sizes)) + sizes)
    except AttributeError:
        pass
    return (n // 4, 2, 2) if n % 4 == 0 else (1, 1, n)


def cut(rows, unit, sizes):
    units = rows // unit
    long_axis = max(range(3), key=lambda d: sizes[d])
    first, second = [d for d in range(3) if d != long_axis]
    tail = units // 8
    pairs = 2 if units >= 8 else 1
    share, extra = divmod(units - tail, 2 * pairs)
    plan = [(tail, (first, second, long_axis), 0)]
    for k in range(2 * pairs):
        short = (first, second) if k % 2 == 0 else (second, first)
        plan.append((share + (k < extra), (long_axis,) + short, k // 2))
    pieces, start = [], 0
    for count, order, wave in plan:
        if count:
            pieces.append((start, count * unit, order, wave))
        start += count * unit
    return pieces


def wavefront(pieces, phases):
    steps = [(piece[3] + phase, phase, p) for p, piece in enumerate(pieces) for phase in range(phases)]
    return [(phase, p) for _, phase, p in sorted(steps)]


def position(sizes):
    me = lax.axis_index("fsdp")
    return [
        lax.div(me, sizes[1] * sizes[2]),
        lax.rem(lax.div(me, sizes[2]), sizes[1]),
        lax.rem(me, sizes[2]),
    ]


def shifted(mine, sizes, d, off):
    return lax.rem(mine[d] + off, sizes[d])


def device_at(mine, sizes, d, coordinate):
    spot = list(mine)
    spot[d] = coordinate
    return {"fsdp": (spot[0] * sizes[1] + spot[1]) * sizes[2] + spot[2]}


def greet(mine, sizes):
    barrier = pltpu.get_barrier_semaphore()
    for d in range(3):
        for off in range(1, sizes[d]):
            target = device_at(mine, sizes, d, shifted(mine, sizes, d, off))
            pl.semaphore_signal(barrier, inc=1, device_id=target, device_id_type=MESH)
    pl.semaphore_wait(barrier, sum(sizes) - 3)


def gather_kernel(sizes, pieces, x_ref, o_ref, own_sem, send_sem, recv_sem):
    mine = position(sizes)
    own = pltpu.make_async_copy(x_ref, o_ref.at[mine[0], mine[1], mine[2]], own_sem)
    own.start()
    greet(mine, sizes)

    def block(piece, phase, coordinate):
        start, rows, order, _ = piece
        index = list(mine)
        index[order[phase]] = coordinate
        for d in order[:phase]:
            index[d] = slice(None)
        return o_ref.at[index[0], index[1], index[2], pl.ds(start, rows)]

    sent = []
    own_here = False
    for phase, p in wavefront(pieces, 3):
        piece = pieces[p]
        if phase:
            if not own_here:
                own.wait()
                own_here = True
            d = piece[2][phase - 1]
            for off in range(1, sizes[d]):
                landed = block(piece, phase - 1, shifted(mine, sizes, d, sizes[d] - off))
                pltpu.make_async_copy(landed, landed, recv_sem.at[p, phase - 1, off]).wait()
        d = piece[2][phase]
        for off in range(1, sizes[d]):
            target = block(piece, phase, mine[d])
            source = x_ref.at[pl.ds(piece[0], piece[1])] if phase == 0 else target
            copy = pltpu.make_async_remote_copy(
                src_ref=source,
                dst_ref=target,
                send_sem=send_sem.at[p, phase, off],
                recv_sem=recv_sem.at[p, phase, off],
                device_id=device_at(mine, sizes, d, shifted(mine, sizes, d, off)),
                device_id_type=MESH,
            )
            copy.start()
            sent.append(copy)
    for p, piece in enumerate(pieces):
        d = piece[2][2]
        for off in range(1, sizes[d]):
            landed = block(piece, 2, shifted(mine, sizes, d, sizes[d] - off))
            pltpu.make_async_copy(landed, landed, recv_sem.at[p, 2, off]).wait()
    for copy in sent:
        copy.wait_send()


def gather(x, sizes, number):
    rows, columns = x.shape
    unit = 8 if x.dtype == jnp.float32 else 16
    pieces = cut(rows, unit, sizes)
    sems = pltpu.SemaphoreType.DMA((len(pieces), 3, max(sizes)))
    out = pl.pallas_call(
        functools.partial(gather_kernel, sizes, pieces),
        out_shape=jax.ShapeDtypeStruct(sizes + (rows, columns), x.dtype),
        in_specs=[pl.BlockSpec(memory_space=pltpu.VMEM)],
        out_specs=pl.BlockSpec(memory_space=pltpu.VMEM),
        scratch_shapes=[pltpu.SemaphoreType.DMA, sems, sems],
        compiler_params=pltpu.CompilerParams(
            collective_id=number, has_side_effects=True, vmem_limit_bytes=32 * 2**20
        ),
        name=f"gather_{number}",
    )(x)
    return out.reshape(math.prod(sizes) * rows, columns)


def reduce_kernel(sizes, pieces, x_ref, o_ref, *scratch):
    mine = position(sizes)
    count = len(pieces)
    landing = scratch[: 3 * count]
    sums = scratch[3 * count : 5 * count]
    send_sem, recv_sem = scratch[5 * count :]
    greet(mine, sizes)
    sent = []

    def send(p, phase, d, off, source):
        copy = pltpu.make_async_remote_copy(
            src_ref=source,
            dst_ref=landing[3 * p + phase].at[off - 1],
            send_sem=send_sem.at[p, phase, off],
            recv_sem=recv_sem.at[p, phase, off],
            device_id=device_at(mine, sizes, d, shifted(mine, sizes, d, off)),
            device_id_type=MESH,
        )
        copy.start()
        sent.append(copy)

    def arrive(p, phase, d):
        for off in range(1, sizes[d]):
            here = landing[3 * p + phase].at[off - 1]
            pltpu.make_async_copy(here, here, recv_sem.at[p, phase, off]).wait()

    def begin(p, start, rows, order):
        d = order[2]
        for off in range(1, sizes[d]):
            index = [slice(None)] * 3
            index[d] = shifted(mine, sizes, d, off)
            send(p, 0, d, off, x_ref.at[index[0], index[1], index[2], pl.ds(start, rows)])

    def first_sums(p, start, rows, order):
        a, b, c = order
        arrive(p, 0, c)
        low, high = min(a, b), max(a, b)
        for off in list(range(1, sizes[b])) + [0]:
            at_b = shifted(mine, sizes, b, off)

            def one(at_a, _, off=off, at_b=at_b):
                index = [None] * 3
                index[a], index[b], index[c] = at_a, at_b, mine[c]
                total = x_ref[index[0], index[1], index[2], pl.ds(start, rows)].astype(jnp.float32)
                for k in range(sizes[c] - 1):
                    total += landing[3 * p][k, index[low], index[high]].astype(jnp.float32)
                if off:
                    sums[2 * p][off - 1, at_a] = total.astype(x_ref.dtype)
                else:
                    sums[2 * p + 1][at_a] = total
                return 0

            lax.fori_loop(0, sizes[a], one, 0)
        for off in range(1, sizes[b]):
            send(p, 1, b, off, sums[2 * p].at[off - 1])

    def second_sums(p, start, rows, order):
        a, b, c = order
        arrive(p, 1, b)
        for off in list(range(1, sizes[a])) + [0]:
            at_a = shifted(mine, sizes, a, off)
            total = sums[2 * p + 1][at_a]
            for k in range(sizes[b] - 1):
                total += landing[3 * p + 1][k, at_a].astype(jnp.float32)
            if off:
                landing[3 * p + 2][sizes[a] - 1 + off - 1] = total.astype(x_ref.dtype)
            else:
                sums[2 * p + 1][at_a] = total
        for off in range(1, sizes[a]):
            send(p, 2, a, off, landing[3 * p + 2].at[sizes[a] - 1 + off - 1])

    def last_sums(p, start, rows, order):
        a = order[0]
        arrive(p, 2, a)
        total = sums[2 * p + 1][mine[a]]
        for k in range(sizes[a] - 1):
            total += landing[3 * p + 2][k].astype(jnp.float32)
        o_ref[pl.ds(start, rows)] = total

    stages = (begin, first_sums, second_sums, last_sums)
    for phase, p in wavefront(pieces, 4):
        stages[phase](p, *pieces[p][:3])
    for copy in sent:
        copy.wait_send()


def reduce_scatter(x, sizes, number):
    n = math.prod(sizes)
    rows, columns = x.shape[0] // n, x.shape[1]
    unit = 8 if x.dtype == jnp.float32 else 16
    pieces = cut(rows, unit, sizes)
    landing, sums = [], []
    for _, part, (a, b, c), _ in pieces:
        low, high = min(a, b), max(a, b)
        many = lambda k: max(k, 1)
        landing += [
            pltpu.VMEM((many(sizes[c] - 1), sizes[low], sizes[high], part, columns), x.dtype),
            pltpu.VMEM((many(sizes[b] - 1), sizes[a], part, columns), x.dtype),
            pltpu.VMEM((many(2 * (sizes[a] - 1)), part, columns), x.dtype),
        ]
        sums += [
            pltpu.VMEM((many(sizes[b] - 1), sizes[a], part, columns), x.dtype),
            pltpu.VMEM((sizes[a], part, columns), jnp.float32),
        ]
    sems = pltpu.SemaphoreType.DMA((len(pieces), 3, max(sizes)))
    return pl.pallas_call(
        functools.partial(reduce_kernel, sizes, pieces),
        out_shape=jax.ShapeDtypeStruct((rows, columns), jnp.float32),
        in_specs=[pl.BlockSpec(memory_space=pltpu.VMEM)],
        out_specs=pl.BlockSpec(memory_space=pltpu.VMEM),
        scratch_shapes=landing + sums + [sems, sems],
        compiler_params=pltpu.CompilerParams(
            collective_id=number, has_side_effects=True, vmem_limit_bytes=40 * 2**20
        ),
        name=f"reduce_{number}",
    )(x.reshape(sizes + (rows, columns)))


def dot_first(left, right):
    return lax.dot_general(
        left, right, (((0,), (0,)), ((), ())), precision=HIGHEST, preferred_element_type=jnp.float32
    )


def three(x):
    high = x.astype(jnp.bfloat16).astype(jnp.float32)
    rest = x - high
    middle = rest.astype(jnp.bfloat16).astype(jnp.float32)
    return high, middle, rest - middle


def short_dot(left, right):
    h, m, l = three(left)
    lefts = jnp.concatenate([h, h, m, m, h, l], axis=0).astype(jnp.bfloat16)
    h, m, l = three(right)
    rights = jnp.concatenate([h, m, h, m, l, h], axis=0).astype(jnp.bfloat16)
    return lax.dot_general(
        lefts, rights, (((0,), (0,)), ((), ())), preferred_element_type=jnp.float32
    )


def nt_dot(left, right, precision=None):
    return lax.dot_general(
        left, right, (((1,), (1,)), ((), ())), precision=precision, preferred_element_type=jnp.float32
    )


def factor_block(width, d_ref, block):
    group = 32
    strip = lax.broadcasted_iota(jnp.int32, (group, width), 0)
    lane = lax.broadcasted_iota(jnp.int32, (group, width), 1)
    d_ref[:, :width] = block
    d_ref[:, width:] = jnp.where(
        lax.broadcasted_iota(jnp.int32, (width, width), 0)
        == lax.broadcasted_iota(jnp.int32, (width, width), 1),
        1.0,
        0.0,
    )
    for first in range(0, width, group):
        end = first + group
        left = d_ref[first:end, :width]
        right = d_ref[first:end, width:]
        columns = [
            jnp.broadcast_to(left[:, first + j : first + j + 1], (group, width)) for j in range(group)
        ]
        for j in range(group):
            scale = lax.rsqrt(columns[j][j : j + 1, :])
            factor = columns[j] * scale
            for m in range(j + 1, group):
                columns[m] = columns[m] - factor * factor[m : m + 1, :]
            row_left, row_right = left[j : j + 1, :] * scale, right[j : j + 1, :] * scale
            below, here = strip > j, strip == j
            left = jnp.where(here, row_left, jnp.where(below, left - factor * row_left, left))
            right = jnp.where(here, row_right, jnp.where(below, right - factor * row_right, right))
        d_ref[first:end, width:] = right
        if end < width:
            later = jnp.where(lane >= end, left, 0.0)
            both = jnp.concatenate([left, right], axis=1)
            d_ref[end:, :] = d_ref[end:, :] - short_dot(later, both)[end:]
    return d_ref[:, width:]


def split(rows, unit, sizes, k, tail):
    long_axis = max(range(3), key=lambda d: sizes[d])
    one, two = [d for d in range(3) if d != long_axis]
    if k % 2:
        one, two = two, one
    share, extra = divmod(rows // unit - tail, 2)
    plan = ((tail, (one, two, long_axis)), (share + extra, (long_axis, one, two)), (share, (long_axis, two, one)))
    pieces, start = [], 0
    for count, order in plan:
        if count:
            pieces.append((start, count * unit, order))
        start += count * unit
    return pieces


def flows_of(blocks, width, basis_rows, sizes):
    long_axis = max(range(3), key=lambda d: sizes[d])
    one, two = [d for d in range(3) if d != long_axis]
    devices = math.prod(sizes)
    flows = []
    for k in range(blocks):
        tail = basis_rows // 64 if 0 < k < blocks - 1 else 0
        flows += [("q", k) + piece for piece in split(basis_rows, 16, sizes, k, tail)]
    for k in range(blocks):
        order = (long_axis, two, one) if k % 2 else (long_axis, one, two)
        flows.append(("g", k, 0, (k + 1) * width // devices, order))
    for k in range(blocks):
        pieces = split(width, 16, sizes, k, width // 128)
        flows += [("s", k, k * width + start, rows, order) for start, rows, order in pieces]
    return flows


BLEND, PROJECT, TRACE, FACTOR, SCALE = -1, -2, -3, -4, -5


TUNED = (
    0, 20, 21, 10, 50, -10, 1, 60, 11, 70, 51, 2, 61, 30, 40, 80, 12, 31, 22, 41,
    3, 71, 42, 90, 32, 13, 52, -20, 72, 62, 23, 33, 43, 100, -21, 81, 110, 91, 63, 101,
    53, 73, 111, -22, 120, 82, 112, 102, 92, 121, 113, 83, 103, 122, 93, -23, 104, 114, -30, 130,
    123, 105, 124, 131, 115, 106, -40, 116, 125, 160, 140, 150, 132, -41, 141, 180, 126, 133, 170, 161,
    -42, 151, 134, 162, 142, 190, 181, 200, 135, 171, 152, 191, 220, 136, 163, 210, 143, 153, 182, -43,
    240, 164, 192, 211, 230, 250, 172, 221, 201, 144, 193, 183, 241, 154, 251, 231, 212, 173, 155, 194,
    165, 222, 213, 232, 184, 195, 242, 223, 202, 203, 145, 252, 214, 174, 224, 233, 185, 215, 243, 253,
    234, 156, 166, 225, 244, 204, 254, 235, 175, 245, 226, 146, 186, 255, 196, 205, -50, 236, 176, -51,
    206, 216, -52, 246, 256, -53,
)


def tuned_agenda(flows, blocks):
    steps = [divmod(code, 10) if code >= 0 else (-(-code // 10), -code % 10) for code in TUNED]
    plain = agenda(flows, blocks)
    return steps if sorted(steps) == sorted(plain) else plain


def agenda(flows, blocks):
    steps = [(0.5, (BLEND, 0))]
    begun = 9.0 * (blocks - 1) + 17
    for f, (kind, k, _, _, _) in enumerate(flows):
        if kind == "q":
            steps += [(9.0 * k + (0, 6, 10, 16)[stage], (f, stage)) for stage in range(4)]
        elif kind == "g" and k < blocks - 1:
            steps += [(9.0 * k + 17.01 + 3.0 * stage, (f, stage)) for stage in range(7)]
        elif kind == "g":
            late = (0, 3, 12.9, 13, 21.4, 21.5, 29.9)
            steps += [(begun + 0.02 + late[stage], (f, stage)) for stage in range(7)]
        else:
            steps += [(begun + 4.6 + 8.5 * (k + stage), (f, stage)) for stage in range(7)]
    for k in range(blocks):
        steps.append((9.0 * k + 16.5, (PROJECT, k)))
        steps.append((begun + 4 + 8.5 * k, (FACTOR, k)))
        steps.append((begun + 4.7 + 8.5 * (k + 6), (SCALE, k)))
    steps.append((begun + 0.1, (TRACE, 0)))
    steps.sort(key=lambda step: step[0])
    needs = {}
    need = lambda step, other: needs.setdefault(step, []).append(other)
    for f, (kind, k, _, _, _) in enumerate(flows):
        final = 3 if kind == "q" else 6
        for stage in range(final):
            need((f, stage + 1), (f, stage))
        if kind == "q":
            need((PROJECT, k), (f, final))
        elif kind == "g":
            need((f, 0), (PROJECT, k))
            need((FACTOR, k), (f, final))
        else:
            need((f, 0), (FACTOR, k))
            need((SCALE, k), (f, final))
    for k in range(blocks):
        need((PROJECT, k), (BLEND, 0))
        need((TRACE, 0), (PROJECT, k))
        need((FACTOR, k), (TRACE, 0))
        if k:
            need((PROJECT, k), (PROJECT, k - 1))
            need((FACTOR, k), (FACTOR, k - 1))
    order, done = [], set()

    def emit(step):
        if step not in done:
            for other in needs.get(step, ()):
                emit(other)
            done.add(step)
            order.append(step)

    for _, step in steps:
        emit(step)
    return order


def main_kernel(sizes, flows, width, m_ref, g_ref, q_ref, o_ref, t_ref, qn_ref, m_buf, *scratch):
    mine = position(sizes)
    me = lax.axis_index("fsdp")
    devices = math.prod(sizes)
    rows, columns = m_ref.shape
    features, size = q_ref.shape
    blocks = size // width
    refs = list(scratch)
    take = lambda n: [refs.pop(0) for _ in range(n)]
    landing, sums = {}, {}
    for f, flow in enumerate(flows):
        if flow[0] != "q":
            landing[f] = take(3)
            sums[f] = take(2)
    grams = take(blocks)
    spreads = take(blocks)
    (g_buf, q_buf, b_ref, basis, p_ref, trace_own, trace_all, u_ref, x_ref, d_ref) = take(10)
    (terms, ot_ref, own_ref, gram_ref) = take(4)
    (in_sem, trace_send, trace_recv, rs_send, rs_recv, ag_send, ag_recv) = take(7)
    base = [0, sizes[0] - 1, sizes[0] + sizes[1] - 2]
    each = sum(sizes) - 3

    loads = [
        pltpu.make_async_copy(q_ref, q_buf, in_sem.at[0]),
        pltpu.make_async_copy(m_ref, m_buf, in_sem.at[1]),
        pltpu.make_async_copy(g_ref, g_buf, in_sem.at[2]),
    ]
    for load in loads:
        load.start()
    barrier = pltpu.get_barrier_semaphore()
    for off in range(1, devices):
        other = {"fsdp": lax.rem(me + off, devices)}
        pl.semaphore_signal(barrier, inc=1, device_id=other, device_id_type=MESH)
    loads[0].wait()
    for k in range(blocks):
        basis[k, mine[0], mine[1], mine[2]] = q_buf[:, k * width : (k + 1) * width].astype(basis.dtype)
    pl.semaphore_wait(barrier, devices - 1)
    sent = []

    def push(source, target, sems, f, d, off):
        at = each * f + base[d] + off - 1
        copy = pltpu.make_async_remote_copy(
            src_ref=source,
            dst_ref=target,
            send_sem=sems[0].at[at],
            recv_sem=sems[1].at[at],
            device_id=device_at(mine, sizes, d, shifted(mine, sizes, d, off)),
            device_id_type=MESH,
        )
        copy.start()
        sent.append(copy)

    def landed(ref, sem, f, d, off):
        pltpu.make_async_copy(ref, ref, sem.at[each * f + base[d] + off - 1]).wait()

    def block(f, phase, coordinate):
        kind, k, start, part, order = flows[f]
        index = list(mine)
        index[order[phase]] = coordinate
        for d in order[:phase]:
            index[d] = slice(None)
        if kind == "q":
            return basis.at[k, index[0], index[1], index[2], pl.ds(start, part)]
        target = spreads[k] if kind == "g" else o_ref
        return target.at[index[0], index[1], index[2], pl.ds(start, part)]

    def spread(f, phase):
        d = flows[f][4][phase]
        here = block(f, phase, mine[d])
        for off in range(1, sizes[d]):
            push(here, here, (ag_send, ag_recv), f, d, off)

    def gathered(f, phase):
        d = flows[f][4][phase]
        for off in range(1, sizes[d]):
            landed(block(f, phase, shifted(mine, sizes, d, sizes[d] - off)), ag_recv, f, d, off)

    def source(f):
        return grams[flows[f][1]] if flows[f][0] == "g" else terms

    def begin(f):
        _, _, start, part, order = flows[f]
        d = order[2]
        for off in range(1, sizes[d]):
            index = [slice(None)] * 3
            index[d] = shifted(mine, sizes, d, off)
            piece = source(f).at[index[0], index[1], index[2], pl.ds(start, part)]
            push(piece, landing[f][0].at[off - 1], (rs_send, rs_recv), f, d, off)

    def first_sums(f):
        _, _, start, part, (a, b, c) = flows[f]
        from_ref = source(f)
        for off in range(1, sizes[c]):
            landed(landing[f][0].at[off - 1], rs_recv, f, c, off)
        low, high = min(a, b), max(a, b)
        for off in list(range(1, sizes[b])) + [0]:
            at_b = shifted(mine, sizes, b, off)

            def one(at_a, _, off=off, at_b=at_b):
                index = [None] * 3
                index[a], index[b], index[c] = at_a, at_b, mine[c]
                total = from_ref[index[0], index[1], index[2], pl.ds(start, part)].astype(jnp.float32)
                for k in range(sizes[c] - 1):
                    total += landing[f][0][k, index[low], index[high]].astype(jnp.float32)
                if off:
                    sums[f][0][off - 1, at_a] = total.astype(from_ref.dtype)
                else:
                    sums[f][1][at_a] = total
                return 0

            lax.fori_loop(0, sizes[a], one, 0)
        for off in range(1, sizes[b]):
            push(sums[f][0].at[off - 1], landing[f][1].at[off - 1], (rs_send, rs_recv), f, b, off)

    def second_sums(f):
        _, _, start, part, (a, b, c) = flows[f]
        for off in range(1, sizes[b]):
            landed(landing[f][1].at[off - 1], rs_recv, f, b, off)
        last = landing[f][2]
        for off in list(range(1, sizes[a])) + [0]:
            at_a = shifted(mine, sizes, a, off)
            total = sums[f][1][at_a]
            for k in range(sizes[b] - 1):
                total += landing[f][1][k, at_a].astype(jnp.float32)
            if off:
                last[sizes[a] - 1 + off - 1] = total.astype(last.dtype)
            else:
                sums[f][1][at_a] = total
        for off in range(1, sizes[a]):
            push(last.at[sizes[a] - 1 + off - 1], last.at[off - 1], (rs_send, rs_recv), f, a, off)

    def last_sums(f):
        kind, k, start, part, (a, b, c) = flows[f]
        for off in range(1, sizes[a]):
            landed(landing[f][2].at[off - 1], rs_recv, f, a, off)
        total = sums[f][1][mine[a]]
        for n in range(sizes[a] - 1):
            total += landing[f][2][n].astype(jnp.float32)
        if kind == "s":
            own_ref[pl.ds(start, part), :] = total
            o_ref[mine[0], mine[1], mine[2], pl.ds(start, part)] = total.astype(o_ref.dtype)
        else:
            spreads[k][mine[0], mine[1], mine[2]] = total

    def spot(i):
        return (
            lax.div(i, sizes[1] * sizes[2]),
            lax.rem(lax.div(i, sizes[2]), sizes[1]),
            lax.rem(i, sizes[2]),
        )

    def lanes_of(i):
        return pl.ds(pl.multiple_of(i * features, features), features)

    def blend():
        loads[1].wait()
        loads[2].wait()

        def one(i, _):
            lanes = lanes_of(i)
            blended = m_buf[:, lanes] + g_buf[:, lanes].astype(jnp.float32)
            m_buf[:, lanes] = blended
            b_ref[:, lanes] = blended.astype(b_ref.dtype)
            return 0

        lax.fori_loop(0, devices, one, 0)

    def project(k):
        top, end = k * width, (k + 1) * width

        def one(i, total):
            at = spot(i)
            return total + jnp.dot(
                b_ref[:, lanes_of(i)], basis[k, at[0], at[1], at[2]], preferred_element_type=jnp.float32
            )

        p_ref[:, top:end] = lax.fori_loop(0, devices, one, jnp.zeros((rows, width), jnp.float32))
        column = dot_first(p_ref[:, :end], p_ref[:, top:end])
        part = end // devices
        for i in range(devices):
            at = (i // (sizes[1] * sizes[2]), i // sizes[2] % sizes[1], i % sizes[2])
            grams[k][at[0], at[1], at[2]] = column[i * part : (i + 1) * part]

    def send_trace():
        square = p_ref[...] * p_ref[...]
        folded = square[:, :128]
        for i in range(1, size // 128):
            folded = folded + square[:, i * 128 : (i + 1) * 128]
        tile = folded[:8]
        for i in range(1, rows // 8):
            tile = tile + folded[i * 8 : (i + 1) * 8]
        trace_own[...] = tile
        trace_all[me] = tile
        for off in range(1, devices):
            copy = pltpu.make_async_remote_copy(
                src_ref=trace_own,
                dst_ref=trace_all.at[me],
                send_sem=trace_send.at[off],
                recv_sem=trace_recv.at[off],
                device_id={"fsdp": lax.rem(me + off, devices)},
                device_id_type=MESH,
            )
            copy.start()
            sent.append(copy)

    def ridge():
        for off in range(1, devices):
            here = trace_all.at[lax.rem(me + devices - off, devices)]
            pltpu.make_async_copy(here, here, trace_recv.at[off]).wait()
        return jnp.sum(jnp.sum(trace_all[...], axis=0), keepdims=True) * (0.0001 / size)

    small_eye = lax.broadcasted_iota(jnp.int32, (width, width), 0) == lax.broadcasted_iota(
        jnp.int32, (width, width), 1
    )
    shared = {}

    def factor(k):
        top, end = k * width, (k + 1) * width
        if k == 0:
            shared["ridge"] = ridge()
        gram_ref[:end, :] = spreads[k][...].reshape(end, width)
        for j in range(k):
            near, far = j * width, (j + 1) * width
            upper = gram_ref[near:far, :]
            if j:
                upper = upper - dot_first(u_ref[:near, near:far], u_ref[:near, top:end])
            u_ref[near:far, top:end] = jnp.dot(x_ref[near:far, near:far], upper, precision=HIGHEST)
        corner = gram_ref[top:end, :] + jnp.where(small_eye, shared["ridge"], 0.0)
        if k:
            panel = u_ref[:top, top:end]
            corner = corner - dot_first(panel, panel)
        inverse = factor_block(width, d_ref, corner)
        x_ref[top:end, top:end] = inverse
        if k:
            rest = dot_first(u_ref[:top, top:end], x_ref[:top, :top])
            x_ref[top:end, :top] = -jnp.dot(inverse, rest, precision=HIGHEST)
        if end < size:
            x_ref[top:end, end:] = jnp.zeros((width, size - end), jnp.float32)
        ortho = nt_dot(x_ref[top:end, :end], p_ref[:, :end], HIGHEST)
        ot_ref[top:end, :] = ortho
        t_ref[:rows, top:end] = ortho.T.astype(t_ref.dtype)
        low = ortho.astype(jnp.bfloat16)

        def one(i, _):
            at = spot(i)
            term = jnp.dot(low, b_ref[:, lanes_of(i)], preferred_element_type=jnp.float32)
            terms[at[0], at[1], at[2], top:end] = term.astype(terms.dtype)
            return 0

        lax.fori_loop(0, devices, one, 0)

    def scale_block(k):
        top, end = k * width, (k + 1) * width

        def squares(i, total):
            at = spot(i)
            wide = o_ref[at[0], at[1], at[2], top:end].astype(jnp.float32)
            return total + wide * wide

        total = lax.fori_loop(0, devices, squares, jnp.zeros((width, features), jnp.float32))
        mean = jnp.sum(total, axis=1, keepdims=True) / (devices * features)
        column_rms = jnp.sqrt(mean + epsilon)
        qn_ref[top:end, :] = own_ref[top:end, :] / column_rms
        t_ref[rows:, top:end] = (ot_ref[top:end, :] / column_rms).T.astype(t_ref.dtype)

    def serve(f, stage):
        if flows[f][0] != "q":
            if stage < 4:
                (begin, first_sums, second_sums, last_sums)[stage](f)
            if stage < 3:
                return
            stage = stage - 3
        if stage:
            gathered(f, stage - 1)
        if stage < 3:
            spread(f, stage)

    special = {
        BLEND: lambda k: blend(),
        PROJECT: project,
        TRACE: lambda k: send_trace(),
        FACTOR: factor,
        SCALE: scale_block,
    }
    for what, stage in tuned_agenda(flows, blocks):
        if what < 0:
            special[what](stage)
        else:
            serve(what, stage)
    for copy in sent:
        copy.wait_send()


def right_factor(momentum, grad, q_basis, sizes, number):
    rows, columns = momentum.shape
    features, size = q_basis.shape
    width = 128
    blocks = size // width
    devices = math.prod(sizes)
    flows = flows_of(blocks, width, features, sizes)
    low_type = jnp.bfloat16
    many = lambda k: max(k, 1)
    scratch = []
    for kind, _, _, part, (a, b, c) in flows:
        if kind == "q":
            continue
        low, high = min(a, b), max(a, b)
        lanes, kept = (width, jnp.float32) if kind == "g" else (features, low_type)
        scratch += [
            pltpu.VMEM((many(sizes[c] - 1), sizes[low], sizes[high], part, lanes), kept),
            pltpu.VMEM((many(sizes[b] - 1), sizes[a], part, lanes), kept),
            pltpu.VMEM((many(2 * (sizes[a] - 1)), part, lanes), kept),
            pltpu.VMEM((many(sizes[b] - 1), sizes[a], part, lanes), kept),
            pltpu.VMEM((sizes[a], part, lanes), jnp.float32),
        ]
    parts = [pltpu.VMEM(sizes + ((k + 1) * width // devices, width), jnp.float32) for k in range(blocks)]
    sems = pltpu.SemaphoreType.DMA((len(flows) * (sum(sizes) - 3),))
    scratch += parts + parts
    scratch += [
        pltpu.VMEM((rows, columns), low_type),
        pltpu.VMEM((features, size), jnp.float32),
        pltpu.VMEM((rows, columns), low_type),
        pltpu.VMEM((blocks,) + sizes + (features, width), low_type),
        pltpu.VMEM((rows, size), jnp.float32),
        pltpu.VMEM((8, 128), jnp.float32),
        pltpu.VMEM((devices, 8, 128), jnp.float32),
        pltpu.VMEM((size, size), jnp.float32),
        pltpu.VMEM((size, size), jnp.float32),
        pltpu.VMEM((width, 2 * width), jnp.float32),
        pltpu.VMEM(sizes + (size, features), low_type),
        pltpu.VMEM((size, rows), jnp.float32),
        pltpu.VMEM((size, features), jnp.float32),
        pltpu.VMEM((size, width), jnp.float32),
        pltpu.SemaphoreType.DMA((3,)),
        pltpu.SemaphoreType.DMA((devices,)),
        pltpu.SemaphoreType.DMA((devices,)),
        sems,
        sems,
        sems,
        sems,
    ]
    vmem = pl.BlockSpec(memory_space=pltpu.VMEM)
    return pl.pallas_call(
        functools.partial(main_kernel, sizes, flows, width),
        out_shape=(
            jax.ShapeDtypeStruct(sizes + (size, features), low_type),
            jax.ShapeDtypeStruct((2 * rows, size), low_type),
            jax.ShapeDtypeStruct((size, features), jnp.float32),
            jax.ShapeDtypeStruct((rows, columns), jnp.float32),
        ),
        in_specs=[pl.BlockSpec(memory_space=pltpu.HBM)] * 3,
        out_specs=(vmem, vmem, vmem, vmem),
        scratch_shapes=scratch,
        compiler_params=pltpu.CompilerParams(
            collective_id=number, has_side_effects=True, vmem_limit_bytes=40 * 2**20
        ),
        name=f"factor_{number}",
    )(momentum, grad, q_basis)


def finish_kernel(step, factor, s_ref, t_ref, q_ref, m_ref, mo_ref, uo_ref, qo_ref, m_buf, u_buf, q_buf, m_sem, u_sem, q_sem):
    rows = m_ref.shape[0]
    blocks, rank, features = s_ref.shape
    q_buf[...] = q_ref[...].T
    q_copy = pltpu.make_async_copy(q_buf, qo_ref, q_sem)
    q_copy.start()

    def copies(slot, i):
        lanes = pl.ds(pl.multiple_of(i * features, features), features)
        return (
            pltpu.make_async_copy(m_buf.at[slot], mo_ref.at[:, lanes], m_sem.at[slot]),
            pltpu.make_async_copy(u_buf.at[slot], uo_ref.at[:, lanes], u_sem.at[slot]),
        )

    slots = m_buf.shape[0]

    def one(i, _):
        slot = lax.rem(i, slots)

        @pl.when(i >= slots)
        def _():
            for copy in copies(slot, i - slots):
                copy.wait()

        lanes = pl.ds(pl.multiple_of(i * features, features), features)
        result = jnp.dot(t_ref[...], s_ref[i], preferred_element_type=jnp.float32)
        m_buf[slot] = m_ref[:, lanes] - step * result[:rows]
        u_buf[slot] = (factor * result[rows:]).astype(u_buf.dtype)
        for copy in copies(slot, i):
            copy.start()
        return 0

    lax.fori_loop(0, blocks, one, 0)
    for i in range(max(blocks - slots, 0), blocks):
        for copy in copies(i % slots, i):
            copy.wait()
    q_copy.wait()


def finish(spread, stacked, turned, blended, factor):
    rows, columns = blended.shape
    blocks, rank, features = spread.shape
    vmem = pl.BlockSpec(memory_space=pltpu.VMEM)
    anywhere = pl.BlockSpec(memory_space=pl.ANY)
    slots = 4
    return pl.pallas_call(
        functools.partial(finish_kernel, 1.0 - damping, factor),
        out_shape=(
            jax.ShapeDtypeStruct((rows, columns), jnp.float32),
            jax.ShapeDtypeStruct((rows, columns), jnp.bfloat16),
            jax.ShapeDtypeStruct((features, rank), jnp.float32),
        ),
        in_specs=[vmem] * 4,
        out_specs=(anywhere,) * 3,
        scratch_shapes=[
            pltpu.VMEM((slots, rows, features), jnp.float32),
            pltpu.VMEM((slots, rows, features), jnp.bfloat16),
            pltpu.VMEM((features, rank), jnp.float32),
            pltpu.SemaphoreType.DMA((slots,)),
            pltpu.SemaphoreType.DMA((slots,)),
            pltpu.SemaphoreType.DMA,
        ],
        compiler_params=pltpu.CompilerParams(vmem_limit_bytes=16 * 2**20),
        name="finish",
    )(spread, stacked, turned, blended)


def inverse_kernel(size, width, g_ref, x_ref, a_ref, d_ref):
    eye = lax.broadcasted_iota(jnp.int32, (size, size), 0) == lax.broadcasted_iota(
        jnp.int32, (size, size), 1
    )
    gram = g_ref[...]
    trace = jnp.sum(jnp.where(eye, gram, 0.0), keepdims=True)
    a_ref[...] = gram + jnp.where(eye, 0.0001 * trace / size, 0.0)
    x_ref[...] = jnp.where(eye, 1.0, 0.0)
    strip = lax.broadcasted_iota(jnp.int32, (8, width), 0)
    lane = lax.broadcasted_iota(jnp.int32, (8, width), 1)
    small_eye = jnp.where(
        lax.broadcasted_iota(jnp.int32, (width, width), 0)
        == lax.broadcasted_iota(jnp.int32, (width, width), 1),
        1.0,
        0.0,
    )

    def group(g, _):
        first = pl.multiple_of(g * 8, 8)
        left = d_ref[pl.ds(first, 8), :width]
        right = d_ref[pl.ds(first, 8), width:]
        turned = pltpu.roll(left, lax.rem(width - first, width), 1)
        columns = [jnp.broadcast_to(turned[:, j : j + 1], (8, width)) for j in range(8)]
        for j in range(8):
            scale = lax.rsqrt(columns[j][j : j + 1, :])
            factor = columns[j] * scale
            for m in range(j + 1, 8):
                columns[m] = columns[m] - factor * factor[m : m + 1, :]
            row_left, row_right = left[j : j + 1, :] * scale, right[j : j + 1, :] * scale
            below, here = strip > j, strip == j
            left = jnp.where(here, row_left, jnp.where(below, left - factor * row_left, left))
            right = jnp.where(here, row_right, jnp.where(below, right - factor * row_right, right))
        later = jnp.where(lane >= first + 8, left, 0.0)
        both = jnp.concatenate([left, right], axis=1)
        d_ref[pl.ds(first, 8), :] = both
        d_ref[...] = d_ref[...] - short_dot(later, both)
        return 0

    for k in range(size // width):
        top, end = k * width, (k + 1) * width
        d_ref[:, :width] = a_ref[top:end, top:end]
        d_ref[:, width:] = small_eye
        lax.fori_loop(0, width // 8, group, 0)
        corner = d_ref[:, width:]
        done = jnp.dot(corner, x_ref[top:end, :end], precision=HIGHEST)
        x_ref[top:end, :end] = done
        if end < size:
            panel = jnp.dot(corner, a_ref[top:end, end:], precision=HIGHEST)
            a_ref[end:, end:] = a_ref[end:, end:] - dot_first(panel, panel)
            x_ref[end:, :end] = x_ref[end:, :end] - dot_first(panel, done)


def lower_inverse(gram_total):
    size = gram_total.shape[0]
    width = 128
    return pl.pallas_call(
        functools.partial(inverse_kernel, size, width),
        out_shape=jax.ShapeDtypeStruct((size, size), jnp.float32),
        in_specs=[pl.BlockSpec(memory_space=pltpu.VMEM)],
        out_specs=pl.BlockSpec(memory_space=pltpu.VMEM),
        scratch_shapes=[
            pltpu.VMEM((size, size), jnp.float32),
            pltpu.VMEM((width, 2 * width), jnp.float32),
        ],
        compiler_params=pltpu.CompilerParams(vmem_limit_bytes=24 * 2**20),
        name="lower_inverse",
    )(gram_total)


def narrow_device(sizes, momentum, grad, q_basis):
    own_rows = momentum.shape[0]
    basis_rows, rank = q_basis.shape
    devices = math.prod(sizes)
    features = basis_rows * devices
    blended = momentum + grad.astype(jnp.float32)
    blended_low = blended.astype(jnp.bfloat16)
    basis = gather(q_basis.astype(jnp.bfloat16), sizes, 0)
    projected = jnp.dot(blended_low, basis, preferred_element_type=jnp.float32)
    local_gram = jnp.dot(projected.T, projected, precision=HIGHEST)
    gram_total = gather(reduce_scatter(local_gram, sizes, 1), sizes, 2)
    inverse = lower_inverse(gram_total)
    orthonormal = jnp.dot(projected, inverse.T, precision=HIGHEST)
    ortho_low = orthonormal.astype(jnp.bfloat16)
    terms = jnp.dot(blended_low.T, ortho_low, preferred_element_type=jnp.float32)
    summed = reduce_scatter(terms.astype(jnp.bfloat16), sizes, 3)
    summed_low = gather(summed.astype(jnp.bfloat16), sizes, 4)
    wide = summed_low.astype(jnp.float32)
    column_rms = jnp.sqrt(jnp.mean(wide * wide, axis=0) + epsilon)
    q_next = summed / column_rms
    stacked = jnp.concatenate(
        [ortho_low, (orthonormal / column_rms).astype(jnp.bfloat16)], axis=0
    )
    result = jnp.dot(stacked, summed_low.T, preferred_element_type=jnp.float32)
    total_rows = own_rows * devices
    momentum_next = blended - (1.0 - damping) * result[:own_rows]
    update = (math.sqrt(total_rows * features / rank) * result[own_rows:]).astype(jnp.bfloat16)
    return (momentum_next, update, q_next)


def per_device(sizes, momentum, grad, q_basis):
    own_rows = momentum.shape[0]
    basis_rows, rank = q_basis.shape
    if basis_rows % 128 or rank % 128 or own_rows % 128:
        return narrow_device(sizes, momentum, grad, q_basis)
    devices = math.prod(sizes)
    features = basis_rows * devices
    spread, stacked, turned, blended = right_factor(momentum, grad, q_basis, sizes, 0)
    total_rows = own_rows * devices
    factor = math.sqrt(total_rows * features / rank)
    spread = spread.reshape(devices, rank, basis_rows)
    return finish(spread, stacked, turned, blended, factor)


def solution(mesh):
    spec = P(("mat", "fsdp"), None)
    return jax.shard_map(
        functools.partial(per_device, grid_of(mesh)),
        mesh=mesh,
        in_specs=(spec, spec, spec),
        out_specs=(spec, spec, spec),
        check_vma=False,
    )
```

```python
import functools
import math

import jax
import jax.numpy as jnp
from jax import lax
from jax.experimental import pallas as pl
from jax.experimental.pallas import tpu as pltpu
from jax.sharding import PartitionSpec as P

damping = 0.95
epsilon = 1e-06
HIGHEST = lax.Precision.HIGHEST
MESH = pl.DeviceIdType.MESH


def grid_of(mesh):
    n = mesh.shape["fsdp"]
    at = list(mesh.axis_names).index("fsdp")
    try:
        line = mesh.devices.swapaxes(0, at).reshape(n, -1)[:, 0]
        spots = [tuple(d.coords) for d in line]
        axes = []
        for d in range(3):
            size = len({s[d] for s in spots})
            if size > 1:
                stride = next(i for i in range(n) if spots[i][d] != spots[0][d])
                axes.append((stride, size))
        sizes = [size for _, size in sorted(axes, reverse=True)]
        if math.prod(sizes) == n:
            return tuple([1] * (3 - len(sizes)) + sizes)
    except AttributeError:
        pass
    return (n // 4, 2, 2) if n % 4 == 0 else (1, 1, n)


def cut(rows, unit, sizes):
    units = rows // unit
    long_axis = max(range(3), key=lambda d: sizes[d])
    first, second = [d for d in range(3) if d != long_axis]
    tail = units // 8
    pairs = 2 if units >= 8 else 1
    share, extra = divmod(units - tail, 2 * pairs)
    plan = [(tail, (first, second, long_axis), 0)]
    for k in range(2 * pairs):
        short = (first, second) if k % 2 == 0 else (second, first)
        plan.append((share + (k < extra), (long_axis,) + short, k // 2))
    pieces, start = [], 0
    for count, order, wave in plan:
        if count:
            pieces.append((start, count * unit, order, wave))
        start += count * unit
    return pieces


def wavefront(pieces, phases):
    steps = [(piece[3] + phase, phase, p) for p, piece in enumerate(pieces) for phase in range(phases)]
    return [(phase, p) for _, phase, p in sorted(steps)]


def position(sizes):
    me = lax.axis_index("fsdp")
    return [
        lax.div(me, sizes[1] * sizes[2]),
        lax.rem(lax.div(me, sizes[2]), sizes[1]),
        lax.rem(me, sizes[2]),
    ]


def shifted(mine, sizes, d, off):
    return lax.rem(mine[d] + off, sizes[d])


def device_at(mine, sizes, d, coordinate):
    spot = list(mine)
    spot[d] = coordinate
    return {"fsdp": (spot[0] * sizes[1] + spot[1]) * sizes[2] + spot[2]}


def greet(mine, sizes):
    barrier = pltpu.get_barrier_semaphore()
    for d in range(3):
        for off in range(1, sizes[d]):
            target = device_at(mine, sizes, d, shifted(mine, sizes, d, off))
            pl.semaphore_signal(barrier, inc=1, device_id=target, device_id_type=MESH)
    pl.semaphore_wait(barrier, sum(sizes) - 3)


def gather_kernel(sizes, pieces, x_ref, o_ref, own_sem, send_sem, recv_sem):
    mine = position(sizes)
    own = pltpu.make_async_copy(x_ref, o_ref.at[mine[0], mine[1], mine[2]], own_sem)
    own.start()
    greet(mine, sizes)

    def block(piece, phase, coordinate):
        start, rows, order, _ = piece
        index = list(mine)
        index[order[phase]] = coordinate
        for d in order[:phase]:
            index[d] = slice(None)
        return o_ref.at[index[0], index[1], index[2], pl.ds(start, rows)]

    sent = []
    own_here = False
    for phase, p in wavefront(pieces, 3):
        piece = pieces[p]
        if phase:
            if not own_here:
                own.wait()
                own_here = True
            d = piece[2][phase - 1]
            for off in range(1, sizes[d]):
                landed = block(piece, phase - 1, shifted(mine, sizes, d, sizes[d] - off))
                pltpu.make_async_copy(landed, landed, recv_sem.at[p, phase - 1, off]).wait()
        d = piece[2][phase]
        for off in range(1, sizes[d]):
            target = block(piece, phase, mine[d])
            source = x_ref.at[pl.ds(piece[0], piece[1])] if phase == 0 else target
            copy = pltpu.make_async_remote_copy(
                src_ref=source,
                dst_ref=target,
                send_sem=send_sem.at[p, phase, off],
                recv_sem=recv_sem.at[p, phase, off],
                device_id=device_at(mine, sizes, d, shifted(mine, sizes, d, off)),
                device_id_type=MESH,
            )
            copy.start()
            sent.append(copy)
    for p, piece in enumerate(pieces):
        d = piece[2][2]
        for off in range(1, sizes[d]):
            landed = block(piece, 2, shifted(mine, sizes, d, sizes[d] - off))
            pltpu.make_async_copy(landed, landed, recv_sem.at[p, 2, off]).wait()
    for copy in sent:
        copy.wait_send()


def gather(x, sizes, number):
    rows, columns = x.shape
    unit = 8 if x.dtype == jnp.float32 else 16
    pieces = cut(rows, unit, sizes)
    sems = pltpu.SemaphoreType.DMA((len(pieces), 3, max(sizes)))
    out = pl.pallas_call(
        functools.partial(gather_kernel, sizes, pieces),
        out_shape=jax.ShapeDtypeStruct(sizes + (rows, columns), x.dtype),
        in_specs=[pl.BlockSpec(memory_space=pltpu.VMEM)],
        out_specs=pl.BlockSpec(memory_space=pltpu.VMEM),
        scratch_shapes=[pltpu.SemaphoreType.DMA, sems, sems],
        compiler_params=pltpu.CompilerParams(
            collective_id=number, has_side_effects=True, vmem_limit_bytes=32 * 2**20
        ),
        name=f"gather_{number}",
    )(x)
    return out.reshape(math.prod(sizes) * rows, columns)


def reduce_kernel(sizes, pieces, x_ref, o_ref, *scratch):
    mine = position(sizes)
    count = len(pieces)
    landing = scratch[: 3 * count]
    sums = scratch[3 * count : 5 * count]
    send_sem, recv_sem = scratch[5 * count :]
    greet(mine, sizes)
    sent = []

    def send(p, phase, d, off, source):
        copy = pltpu.make_async_remote_copy(
            src_ref=source,
            dst_ref=landing[3 * p + phase].at[off - 1],
            send_sem=send_sem.at[p, phase, off],
            recv_sem=recv_sem.at[p, phase, off],
            device_id=device_at(mine, sizes, d, shifted(mine, sizes, d, off)),
            device_id_type=MESH,
        )
        copy.start()
        sent.append(copy)

    def arrive(p, phase, d):
        for off in range(1, sizes[d]):
            here = landing[3 * p + phase].at[off - 1]
            pltpu.make_async_copy(here, here, recv_sem.at[p, phase, off]).wait()

    def begin(p, start, rows, order):
        d = order[2]
        for off in range(1, sizes[d]):
            index = [slice(None)] * 3
            index[d] = shifted(mine, sizes, d, off)
            send(p, 0, d, off, x_ref.at[index[0], index[1], index[2], pl.ds(start, rows)])

    def first_sums(p, start, rows, order):
        a, b, c = order
        arrive(p, 0, c)
        low, high = min(a, b), max(a, b)
        for off in list(range(1, sizes[b])) + [0]:
            at_b = shifted(mine, sizes, b, off)

            def one(at_a, _, off=off, at_b=at_b):
                index = [None] * 3
                index[a], index[b], index[c] = at_a, at_b, mine[c]
                total = x_ref[index[0], index[1], index[2], pl.ds(start, rows)].astype(jnp.float32)
                for k in range(sizes[c] - 1):
                    total += landing[3 * p][k, index[low], index[high]].astype(jnp.float32)
                if off:
                    sums[2 * p][off - 1, at_a] = total.astype(x_ref.dtype)
                else:
                    sums[2 * p + 1][at_a] = total
                return 0

            lax.fori_loop(0, sizes[a], one, 0)
        for off in range(1, sizes[b]):
            send(p, 1, b, off, sums[2 * p].at[off - 1])

    def second_sums(p, start, rows, order):
        a, b, c = order
        arrive(p, 1, b)
        for off in list(range(1, sizes[a])) + [0]:
            at_a = shifted(mine, sizes, a, off)
            total = sums[2 * p + 1][at_a]
            for k in range(sizes[b] - 1):
                total += landing[3 * p + 1][k, at_a].astype(jnp.float32)
            if off:
                landing[3 * p + 2][sizes[a] - 1 + off - 1] = total.astype(x_ref.dtype)
            else:
                sums[2 * p + 1][at_a] = total
        for off in range(1, sizes[a]):
            send(p, 2, a, off, landing[3 * p + 2].at[sizes[a] - 1 + off - 1])

    def last_sums(p, start, rows, order):
        a = order[0]
        arrive(p, 2, a)
        total = sums[2 * p + 1][mine[a]]
        for k in range(sizes[a] - 1):
            total += landing[3 * p + 2][k].astype(jnp.float32)
        o_ref[pl.ds(start, rows)] = total

    stages = (begin, first_sums, second_sums, last_sums)
    for phase, p in wavefront(pieces, 4):
        stages[phase](p, *pieces[p][:3])
    for copy in sent:
        copy.wait_send()


def reduce_scatter(x, sizes, number):
    n = math.prod(sizes)
    rows, columns = x.shape[0] // n, x.shape[1]
    unit = 8 if x.dtype == jnp.float32 else 16
    pieces = cut(rows, unit, sizes)
    landing, sums = [], []
    for _, part, (a, b, c), _ in pieces:
        low, high = min(a, b), max(a, b)
        many = lambda k: max(k, 1)
        landing += [
            pltpu.VMEM((many(sizes[c] - 1), sizes[low], sizes[high], part, columns), x.dtype),
            pltpu.VMEM((many(sizes[b] - 1), sizes[a], part, columns), x.dtype),
            pltpu.VMEM((many(2 * (sizes[a] - 1)), part, columns), x.dtype),
        ]
        sums += [
            pltpu.VMEM((many(sizes[b] - 1), sizes[a], part, columns), x.dtype),
            pltpu.VMEM((sizes[a], part, columns), jnp.float32),
        ]
    sems = pltpu.SemaphoreType.DMA((len(pieces), 3, max(sizes)))
    return pl.pallas_call(
        functools.partial(reduce_kernel, sizes, pieces),
        out_shape=jax.ShapeDtypeStruct((rows, columns), jnp.float32),
        in_specs=[pl.BlockSpec(memory_space=pltpu.VMEM)],
        out_specs=pl.BlockSpec(memory_space=pltpu.VMEM),
        scratch_shapes=landing + sums + [sems, sems],
        compiler_params=pltpu.CompilerParams(
            collective_id=number, has_side_effects=True, vmem_limit_bytes=40 * 2**20
        ),
        name=f"reduce_{number}",
    )(x.reshape(sizes + (rows, columns)))


def dot_first(left, right):
    return lax.dot_general(
        left, right, (((0,), (0,)), ((), ())), precision=HIGHEST, preferred_element_type=jnp.float32
    )


def three(x):
    high = x.astype(jnp.bfloat16).astype(jnp.float32)
    rest = x - high
    middle = rest.astype(jnp.bfloat16).astype(jnp.float32)
    return high, middle, rest - middle


def short_dot(left, right):
    h, m, l = three(left)
    lefts = jnp.concatenate([h, h, m, m, h, l], axis=0).astype(jnp.bfloat16)
    h, m, l = three(right)
    rights = jnp.concatenate([h, m, h, m, l, h], axis=0).astype(jnp.bfloat16)
    return lax.dot_general(
        lefts, rights, (((0,), (0,)), ((), ())), preferred_element_type=jnp.float32
    )


def nt_dot(left, right, precision=None):
    return lax.dot_general(
        left, right, (((1,), (1,)), ((), ())), precision=precision, preferred_element_type=jnp.float32
    )


def factor_block(width, d_ref, block):
    group = 32
    strip = lax.broadcasted_iota(jnp.int32, (group, width), 0)
    lane = lax.broadcasted_iota(jnp.int32, (group, width), 1)
    d_ref[:, :width] = block
    d_ref[:, width:] = jnp.where(
        lax.broadcasted_iota(jnp.int32, (width, width), 0)
        == lax.broadcasted_iota(jnp.int32, (width, width), 1),
        1.0,
        0.0,
    )
    for first in range(0, width, group):
        end = first + group
        left = d_ref[first:end, :width]
        right = d_ref[first:end, width:]
        columns = [
            jnp.broadcast_to(left[:, first + j : first + j + 1], (group, width)) for j in range(group)
        ]
        for j in range(group):
            scale = lax.rsqrt(columns[j][j : j + 1, :])
            factor = columns[j] * scale
            for m in range(j + 1, group):
                columns[m] = columns[m] - factor * factor[m : m + 1, :]
            row_left, row_right = left[j : j + 1, :] * scale, right[j : j + 1, :] * scale
            below, here = strip > j, strip == j
            left = jnp.where(here, row_left, jnp.where(below, left - factor * row_left, left))
            right = jnp.where(here, row_right, jnp.where(below, right - factor * row_right, right))
        d_ref[first:end, width:] = right
        if end < width:
            later = jnp.where(lane >= end, left, 0.0)
            both = jnp.concatenate([left, right], axis=1)
            d_ref[end:, :] = d_ref[end:, :] - short_dot(later, both)[end:]
    return d_ref[:, width:]


def split(rows, unit, sizes, k, tail):
    long_axis = max(range(3), key=lambda d: sizes[d])
    one, two = [d for d in range(3) if d != long_axis]
    if k % 2:
        one, two = two, one
    share, extra = divmod(rows // unit - tail, 2)
    plan = ((tail, (one, two, long_axis)), (share + extra, (long_axis, one, two)), (share, (long_axis, two, one)))
    pieces, start = [], 0
    for count, order in plan:
        if count:
            pieces.append((start, count * unit, order))
        start += count * unit
    return pieces


def flows_of(blocks, width, basis_rows, sizes):
    long_axis = max(range(3), key=lambda d: sizes[d])
    one, two = [d for d in range(3) if d != long_axis]
    devices = math.prod(sizes)
    flows = []
    for k in range(blocks):
        tail = basis_rows // 64 if 0 < k < blocks - 1 else 0
        flows += [("q", k) + piece for piece in split(basis_rows, 16, sizes, k, tail)]
    for k in range(blocks):
        order = (long_axis, two, one) if k % 2 else (long_axis, one, two)
        flows.append(("g", k, 0, (k + 1) * width // devices, order))
    for k in range(blocks):
        pieces = split(width, 16, sizes, k, width // 128)
        flows += [("s", k, k * width + start, rows, order) for start, rows, order in pieces]
    return flows


BLEND, PROJECT, TRACE, FACTOR, SCALE, TELL, HEAR = -1, -2, -3, -4, -5, -6, -7


TUNED = (
    10, 20, 40, 21, 50, -10, 30, 11, 41, 0, 31, 12, 42, 80, 60, 1, 81, 90, 51, 43,
    61, 2, 13, 70, 91, 32, 62, 82, 22, 3, 71, 52, -20, 100, 33, 23, -21, 63, 101, 92,
    72, 110, 83, 102, 73, 53, -22, 93, 103, 120, -23, 130, 111, 121, -30, 112, 104, 122, 131, 105,
    106, 113, 132, 123, -40, 114, 124, 150, 160, 133, 115, 134, 161, 151, 140, 125, 116, -41, 135, 126,
    162, 152, 180, 170, 190, -42, 200, 136, 141, 191, 163, 210, 171, 153, 181, -43, 230, 201, 172, 211,
    250, 182, 240, 220, 142, 192, 164, 154, 212, 241, 251, 202, 183, 242, 173, 155, 231, 143, 184, 213,
    203, 232, 144, 221, 243, 174, 165, 252, 214, 185, 222, 193, 233, 204, 244, 253, 234, 223, 215, 194,
    186, 254, 166, 224, 156, 205, 245, 175, 145, 195, 235, 255, 225, 176, 196, -51, 146, 246, 216, -50,
    256, 236, 206, -53, 226, -52,
)


def tuned_agenda(flows, blocks):
    steps = [divmod(code, 10) if code >= 0 else (-(-code // 10), -code % 10) for code in TUNED]
    plain = agenda(flows, blocks)
    known = sorted(step for step in steps if step[0] > TELL)
    return steps if known == sorted(plain) else plain


def agenda(flows, blocks):
    steps = [(0.5, (BLEND, 0))]
    begun = 9.0 * (blocks - 1) + 17
    for f, (kind, k, _, _, _) in enumerate(flows):
        if kind == "q":
            steps += [(9.0 * k + (0, 6, 10, 16)[stage], (f, stage)) for stage in range(4)]
        elif kind == "g" and k < blocks - 1:
            steps += [(9.0 * k + 17.01 + 3.0 * stage, (f, stage)) for stage in range(7)]
        elif kind == "g":
            late = (0, 3, 12.9, 13, 21.4, 21.5, 29.9)
            steps += [(begun + 0.02 + late[stage], (f, stage)) for stage in range(7)]
        else:
            steps += [(begun + 4.6 + 8.5 * (k + stage), (f, stage)) for stage in range(7)]
    for k in range(blocks):
        steps.append((9.0 * k + 16.5, (PROJECT, k)))
        steps.append((begun + 4 + 8.5 * k, (FACTOR, k)))
        steps.append((begun + 4.7 + 8.5 * (k + 6), (SCALE, k)))
    steps.append((begun + 0.1, (TRACE, 0)))
    steps.sort(key=lambda step: step[0])
    needs = {}
    need = lambda step, other: needs.setdefault(step, []).append(other)
    for f, (kind, k, _, _, _) in enumerate(flows):
        final = 3 if kind == "q" else 6
        for stage in range(final):
            need((f, stage + 1), (f, stage))
        if kind == "q":
            need((PROJECT, k), (f, final))
        elif kind == "g":
            need((f, 0), (PROJECT, k))
            need((FACTOR, k), (f, final))
        else:
            need((f, 0), (FACTOR, k))
            need((SCALE, k), (f, final))
    for k in range(blocks):
        need((PROJECT, k), (BLEND, 0))
        need((TRACE, 0), (PROJECT, k))
        need((FACTOR, k), (TRACE, 0))
        if k:
            need((PROJECT, k), (PROJECT, k - 1))
            need((FACTOR, k), (FACTOR, k - 1))
    order, done = [], set()

    def emit(step):
        if step not in done:
            for other in needs.get(step, ()):
                emit(other)
            done.add(step)
            order.append(step)

    for _, step in steps:
        emit(step)
    return order


def main_kernel(sizes, parts, flows, width, m_ref, g_ref, q_ref, o_ref, t_ref, qn_ref, m_buf, *scratch):
    mine = position(sizes)
    me = lax.axis_index("fsdp")
    devices = math.prod(sizes)
    rows, columns = m_ref.shape
    features, size = q_ref.shape
    blocks = size // width
    refs = list(scratch)
    take = lambda n: [refs.pop(0) for _ in range(n)]
    landing, sums = {}, {}
    for f, flow in enumerate(flows):
        if flow[0] != "q":
            landing[f] = take(3)
            sums[f] = take(2)
    grams = take(blocks)
    spreads = take(blocks)
    (g_buf, q_buf, b_ref, basis, p_ref, trace_own, trace_all, u_ref, x_ref, d_ref) = take(10)
    (terms, ot_ref, own_ref, gram_ref) = take(4)
    (in_sem, trace_send, trace_recv, rs_send, rs_recv, ag_send, ag_recv, pace) = take(8)
    base = [0, sizes[0] - 1, sizes[0] + sizes[1] - 2]
    each = sum(sizes) - 3

    loads = [
        pltpu.make_async_copy(q_ref, q_buf, in_sem.at[0]),
        pltpu.make_async_copy(m_ref, m_buf, in_sem.at[1]),
        pltpu.make_async_copy(g_ref, g_buf, in_sem.at[2]),
    ]
    for load in loads:
        load.start()
    barrier = pltpu.get_barrier_semaphore()
    for off in range(1, devices):
        other = {"fsdp": lax.rem(me + off, devices)}
        pl.semaphore_signal(barrier, inc=1, device_id=other, device_id_type=MESH)
    part = lax.axis_index("mat")
    paired = parts == 2
    if paired:
        pl.semaphore_signal(barrier, inc=1, device_id={"mat": 1 - part}, device_id_type=MESH)
    loads[0].wait()
    for k in range(blocks):
        basis[k, mine[0], mine[1], mine[2]] = q_buf[:, k * width : (k + 1) * width].astype(basis.dtype)
    pl.semaphore_wait(barrier, devices - 1 + paired)
    sent = []

    def push(source, target, sems, f, d, off):
        at = each * f + base[d] + off - 1
        copy = pltpu.make_async_remote_copy(
            src_ref=source,
            dst_ref=target,
            send_sem=sems[0].at[at],
            recv_sem=sems[1].at[at],
            device_id=device_at(mine, sizes, d, shifted(mine, sizes, d, off)),
            device_id_type=MESH,
        )
        copy.start()
        sent.append(copy)

    def landed(ref, sem, f, d, off):
        pltpu.make_async_copy(ref, ref, sem.at[each * f + base[d] + off - 1]).wait()

    def block(f, phase, coordinate):
        kind, k, start, part, order = flows[f]
        index = list(mine)
        index[order[phase]] = coordinate
        for d in order[:phase]:
            index[d] = slice(None)
        if kind == "q":
            return basis.at[k, index[0], index[1], index[2], pl.ds(start, part)]
        target = spreads[k] if kind == "g" else o_ref
        return target.at[index[0], index[1], index[2], pl.ds(start, part)]

    def spread(f, phase):
        d = flows[f][4][phase]
        here = block(f, phase, mine[d])
        for off in range(1, sizes[d]):
            push(here, here, (ag_send, ag_recv), f, d, off)

    def gathered(f, phase):
        d = flows[f][4][phase]
        for off in range(1, sizes[d]):
            landed(block(f, phase, shifted(mine, sizes, d, sizes[d] - off)), ag_recv, f, d, off)

    def source(f):
        return grams[flows[f][1]] if flows[f][0] == "g" else terms

    def begin(f):
        _, _, start, part, order = flows[f]
        d = order[2]
        for off in range(1, sizes[d]):
            index = [slice(None)] * 3
            index[d] = shifted(mine, sizes, d, off)
            piece = source(f).at[index[0], index[1], index[2], pl.ds(start, part)]
            push(piece, landing[f][0].at[off - 1], (rs_send, rs_recv), f, d, off)

    def first_sums(f):
        _, _, start, part, (a, b, c) = flows[f]
        from_ref = source(f)
        for off in range(1, sizes[c]):
            landed(landing[f][0].at[off - 1], rs_recv, f, c, off)
        low, high = min(a, b), max(a, b)
        for off in list(range(1, sizes[b])) + [0]:
            at_b = shifted(mine, sizes, b, off)

            def one(at_a, _, off=off, at_b=at_b):
                index = [None] * 3
                index[a], index[b], index[c] = at_a, at_b, mine[c]
                total = from_ref[index[0], index[1], index[2], pl.ds(start, part)].astype(jnp.float32)
                for k in range(sizes[c] - 1):
                    total += landing[f][0][k, index[low], index[high]].astype(jnp.float32)
                if off:
                    sums[f][0][off - 1, at_a] = total.astype(from_ref.dtype)
                else:
                    sums[f][1][at_a] = total
                return 0

            lax.fori_loop(0, sizes[a], one, 0)
        for off in range(1, sizes[b]):
            push(sums[f][0].at[off - 1], landing[f][1].at[off - 1], (rs_send, rs_recv), f, b, off)

    def second_sums(f):
        _, _, start, part, (a, b, c) = flows[f]
        for off in range(1, sizes[b]):
            landed(landing[f][1].at[off - 1], rs_recv, f, b, off)
        last = landing[f][2]
        for off in list(range(1, sizes[a])) + [0]:
            at_a = shifted(mine, sizes, a, off)
            total = sums[f][1][at_a]
            for k in range(sizes[b] - 1):
                total += landing[f][1][k, at_a].astype(jnp.float32)
            if off:
                last[sizes[a] - 1 + off - 1] = total.astype(last.dtype)
            else:
                sums[f][1][at_a] = total
        for off in range(1, sizes[a]):
            push(last.at[sizes[a] - 1 + off - 1], last.at[off - 1], (rs_send, rs_recv), f, a, off)

    def last_sums(f):
        kind, k, start, part, (a, b, c) = flows[f]
        for off in range(1, sizes[a]):
            landed(landing[f][2].at[off - 1], rs_recv, f, a, off)
        total = sums[f][1][mine[a]]
        for n in range(sizes[a] - 1):
            total += landing[f][2][n].astype(jnp.float32)
        if kind == "s":
            own_ref[pl.ds(start, part), :] = total
            o_ref[mine[0], mine[1], mine[2], pl.ds(start, part)] = total.astype(o_ref.dtype)
        else:
            spreads[k][mine[0], mine[1], mine[2]] = total

    def spot(i):
        return (
            lax.div(i, sizes[1] * sizes[2]),
            lax.rem(lax.div(i, sizes[2]), sizes[1]),
            lax.rem(i, sizes[2]),
        )

    def lanes_of(i):
        return pl.ds(pl.multiple_of(i * features, features), features)

    def blend():
        loads[1].wait()
        loads[2].wait()

        def one(i, _):
            lanes = lanes_of(i)
            blended = m_buf[:, lanes] + g_buf[:, lanes].astype(jnp.float32)
            m_buf[:, lanes] = blended
            b_ref[:, lanes] = blended.astype(b_ref.dtype)
            return 0

        lax.fori_loop(0, devices, one, 0)

    def project(k):
        top, end = k * width, (k + 1) * width

        def one(i, total):
            at = spot(i)
            return total + jnp.dot(
                b_ref[:, lanes_of(i)], basis[k, at[0], at[1], at[2]], preferred_element_type=jnp.float32
            )

        p_ref[:, top:end] = lax.fori_loop(0, devices, one, jnp.zeros((rows, width), jnp.float32))
        column = dot_first(p_ref[:, :end], p_ref[:, top:end])
        part = end // devices
        for i in range(devices):
            at = (i // (sizes[1] * sizes[2]), i // sizes[2] % sizes[1], i % sizes[2])
            grams[k][at[0], at[1], at[2]] = column[i * part : (i + 1) * part]

    def send_trace():
        square = p_ref[...] * p_ref[...]
        folded = square[:, :128]
        for i in range(1, size // 128):
            folded = folded + square[:, i * 128 : (i + 1) * 128]
        tile = folded[:8]
        for i in range(1, rows // 8):
            tile = tile + folded[i * 8 : (i + 1) * 8]
        trace_own[...] = tile
        trace_all[me] = tile
        for off in range(1, devices):
            copy = pltpu.make_async_remote_copy(
                src_ref=trace_own,
                dst_ref=trace_all.at[me],
                send_sem=trace_send.at[off],
                recv_sem=trace_recv.at[off],
                device_id={"fsdp": lax.rem(me + off, devices)},
                device_id_type=MESH,
            )
            copy.start()
            sent.append(copy)

    def ridge():
        for off in range(1, devices):
            here = trace_all.at[lax.rem(me + devices - off, devices)]
            pltpu.make_async_copy(here, here, trace_recv.at[off]).wait()
        return jnp.sum(jnp.sum(trace_all[...], axis=0), keepdims=True) * (0.0001 / size)

    small_eye = lax.broadcasted_iota(jnp.int32, (width, width), 0) == lax.broadcasted_iota(
        jnp.int32, (width, width), 1
    )
    shared = {}

    def factor(k):
        top, end = k * width, (k + 1) * width
        if k == 0:
            shared["ridge"] = ridge()
        gram_ref[:end, :] = spreads[k][...].reshape(end, width)
        for j in range(k):
            near, far = j * width, (j + 1) * width
            upper = gram_ref[near:far, :]
            if j:
                upper = upper - dot_first(u_ref[:near, near:far], u_ref[:near, top:end])
            u_ref[near:far, top:end] = jnp.dot(x_ref[near:far, near:far], upper, precision=HIGHEST)
        corner = gram_ref[top:end, :] + jnp.where(small_eye, shared["ridge"], 0.0)
        if k:
            panel = u_ref[:top, top:end]
            corner = corner - dot_first(panel, panel)
        inverse = factor_block(width, d_ref, corner)
        x_ref[top:end, top:end] = inverse
        if k:
            rest = dot_first(u_ref[:top, top:end], x_ref[:top, :top])
            x_ref[top:end, :top] = -jnp.dot(inverse, rest, precision=HIGHEST)
        if end < size:
            x_ref[top:end, end:] = jnp.zeros((width, size - end), jnp.float32)
        ortho = nt_dot(x_ref[top:end, :end], p_ref[:, :end], HIGHEST)
        ot_ref[top:end, :] = ortho
        t_ref[:rows, top:end] = ortho.T.astype(t_ref.dtype)
        low = ortho.astype(jnp.bfloat16)

        def one(i, _):
            at = spot(i)
            term = jnp.dot(low, b_ref[:, lanes_of(i)], preferred_element_type=jnp.float32)
            terms[at[0], at[1], at[2], top:end] = term.astype(terms.dtype)
            return 0

        lax.fori_loop(0, devices, one, 0)

    def scale_block(k):
        top, end = k * width, (k + 1) * width

        def squares(i, total):
            at = spot(i)
            wide = o_ref[at[0], at[1], at[2], top:end].astype(jnp.float32)
            return total + wide * wide

        total = lax.fori_loop(0, devices, squares, jnp.zeros((width, features), jnp.float32))
        mean = jnp.sum(total, axis=1, keepdims=True) / (devices * features)
        column_rms = jnp.sqrt(mean + epsilon)
        qn_ref[top:end, :] = own_ref[top:end, :] / column_rms
        t_ref[rows:, top:end] = (ot_ref[top:end, :] / column_rms).T.astype(t_ref.dtype)

    def serve(f, stage):
        if flows[f][0] != "q":
            if stage < 4:
                (begin, first_sums, second_sums, last_sums)[stage](f)
            if stage < 3:
                return
            stage = stage - 3
        if stage:
            gathered(f, stage - 1)
        if stage < 3:
            spread(f, stage)

    def tell(n):
        if paired:

            @pl.when(part == n % 2)
            def _():
                pl.semaphore_signal(pace.at[n], inc=1, device_id={"mat": 1 - part}, device_id_type=MESH)

    def hear(n):
        if paired:

            @pl.when(part != n % 2)
            def _():
                pl.semaphore_wait(pace.at[n], 1)

    special = {
        BLEND: lambda k: blend(),
        PROJECT: project,
        TRACE: lambda k: send_trace(),
        FACTOR: factor,
        SCALE: scale_block,
        TELL: tell,
        HEAR: hear,
    }
    for what, stage in tuned_agenda(flows, blocks):
        if what < 0:
            special[what](stage)
        else:
            serve(what, stage)
    for copy in sent:
        copy.wait_send()


def right_factor(momentum, grad, q_basis, sizes, parts, number):
    rows, columns = momentum.shape
    features, size = q_basis.shape
    width = 128
    blocks = size // width
    devices = math.prod(sizes)
    flows = flows_of(blocks, width, features, sizes)
    low_type = jnp.bfloat16
    many = lambda k: max(k, 1)
    scratch = []
    for kind, _, _, part, (a, b, c) in flows:
        if kind == "q":
            continue
        low, high = min(a, b), max(a, b)
        lanes, kept = (width, jnp.float32) if kind == "g" else (features, low_type)
        scratch += [
            pltpu.VMEM((many(sizes[c] - 1), sizes[low], sizes[high], part, lanes), kept),
            pltpu.VMEM((many(sizes[b] - 1), sizes[a], part, lanes), kept),
            pltpu.VMEM((many(2 * (sizes[a] - 1)), part, lanes), kept),
            pltpu.VMEM((many(sizes[b] - 1), sizes[a], part, lanes), kept),
            pltpu.VMEM((sizes[a], part, lanes), jnp.float32),
        ]
    chunks = [pltpu.VMEM(sizes + ((k + 1) * width // devices, width), jnp.float32) for k in range(blocks)]
    sems = pltpu.SemaphoreType.DMA((len(flows) * (sum(sizes) - 3),))
    scratch += chunks + chunks
    scratch += [
        pltpu.VMEM((rows, columns), low_type),
        pltpu.VMEM((features, size), jnp.float32),
        pltpu.VMEM((rows, columns), low_type),
        pltpu.VMEM((blocks,) + sizes + (features, width), low_type),
        pltpu.VMEM((rows, size), jnp.float32),
        pltpu.VMEM((8, 128), jnp.float32),
        pltpu.VMEM((devices, 8, 128), jnp.float32),
        pltpu.VMEM((size, size), jnp.float32),
        pltpu.VMEM((size, size), jnp.float32),
        pltpu.VMEM((width, 2 * width), jnp.float32),
        pltpu.VMEM(sizes + (size, features), low_type),
        pltpu.VMEM((size, rows), jnp.float32),
        pltpu.VMEM((size, features), jnp.float32),
        pltpu.VMEM((size, width), jnp.float32),
        pltpu.SemaphoreType.DMA((3,)),
        pltpu.SemaphoreType.DMA((devices,)),
        pltpu.SemaphoreType.DMA((devices,)),
        sems,
        sems,
        sems,
        sems,
        pltpu.SemaphoreType.REGULAR((4,)),
    ]
    vmem = pl.BlockSpec(memory_space=pltpu.VMEM)
    return pl.pallas_call(
        functools.partial(main_kernel, sizes, parts, flows, width),
        out_shape=(
            pltpu.VMEM(sizes + (size, features), low_type),
            pltpu.VMEM((2 * rows, size), low_type),
            pltpu.VMEM((size, features), jnp.float32),
            pltpu.VMEM((rows, columns), jnp.float32),
        ),
        in_specs=[pl.BlockSpec(memory_space=pltpu.HBM)] * 3,
        out_specs=(vmem, vmem, vmem, vmem),
        scratch_shapes=scratch,
        compiler_params=pltpu.CompilerParams(
            collective_id=number, has_side_effects=True, vmem_limit_bytes=48 * 2**20
        ),
        name=f"factor_{number}",
    )(momentum, grad, q_basis)


def finish_kernel(step, factor, s_ref, t_ref, q_ref, m_ref, mo_ref, uo_ref, qo_ref, m_buf, u_buf, q_buf, m_sem, u_sem, q_sem):
    rows = m_ref.shape[0]
    blocks, rank, features = s_ref.shape
    q_buf[...] = q_ref[...].T
    q_copy = pltpu.make_async_copy(q_buf, qo_ref, q_sem)
    q_copy.start()

    def copies(slot, i):
        lanes = pl.ds(pl.multiple_of(i * features, features), features)
        return (
            pltpu.make_async_copy(m_buf.at[slot], mo_ref.at[:, lanes], m_sem.at[slot]),
            pltpu.make_async_copy(u_buf.at[slot], uo_ref.at[:, lanes], u_sem.at[slot]),
        )

    slots = m_buf.shape[0]
    wide = math.gcd(blocks, slots // 2)

    def one(step_index, _):
        for n in range(wide):
            i = step_index * wide + n
            slot = lax.rem(i, slots)

            @pl.when(i >= slots)
            def _(slot=slot, i=i):
                for copy in copies(slot, i - slots):
                    copy.wait()

        results = [
            jnp.dot(t_ref[...], s_ref[step_index * wide + n], preferred_element_type=jnp.float32)
            for n in range(wide)
        ]
        for n in range(wide):
            i = step_index * wide + n
            slot = lax.rem(i, slots)
            lanes = pl.ds(pl.multiple_of(i * features, features), features)
            m_buf[slot] = m_ref[:, lanes] - step * results[n][:rows]
            u_buf[slot] = (factor * results[n][rows:]).astype(u_buf.dtype)
            for copy in copies(slot, i):
                copy.start()
        return 0

    lax.fori_loop(0, blocks // wide, one, 0)
    for i in range(max(blocks - slots, 0), blocks):
        for copy in copies(i % slots, i):
            copy.wait()
    q_copy.wait()


def finish(spread, stacked, turned, blended, factor):
    rows, columns = blended.shape
    blocks, rank, features = spread.shape
    vmem = pl.BlockSpec(memory_space=pltpu.VMEM)
    anywhere = pl.BlockSpec(memory_space=pl.ANY)
    slots = 8
    return pl.pallas_call(
        functools.partial(finish_kernel, 1.0 - damping, factor),
        out_shape=(
            jax.ShapeDtypeStruct((rows, columns), jnp.float32),
            jax.ShapeDtypeStruct((rows, columns), jnp.bfloat16),
            jax.ShapeDtypeStruct((features, rank), jnp.float32),
        ),
        in_specs=[vmem] * 4,
        out_specs=(anywhere,) * 3,
        scratch_shapes=[
            pltpu.VMEM((slots, rows, features), jnp.float32),
            pltpu.VMEM((slots, rows, features), jnp.bfloat16),
            pltpu.VMEM((features, rank), jnp.float32),
            pltpu.SemaphoreType.DMA((slots,)),
            pltpu.SemaphoreType.DMA((slots,)),
            pltpu.SemaphoreType.DMA,
        ],
        compiler_params=pltpu.CompilerParams(vmem_limit_bytes=16 * 2**20),
        name="finish",
    )(spread, stacked, turned, blended)


def inverse_kernel(size, width, g_ref, x_ref, a_ref, d_ref):
    eye = lax.broadcasted_iota(jnp.int32, (size, size), 0) == lax.broadcasted_iota(
        jnp.int32, (size, size), 1
    )
    gram = g_ref[...]
    trace = jnp.sum(jnp.where(eye, gram, 0.0), keepdims=True)
    a_ref[...] = gram + jnp.where(eye, 0.0001 * trace / size, 0.0)
    x_ref[...] = jnp.where(eye, 1.0, 0.0)
    strip = lax.broadcasted_iota(jnp.int32, (8, width), 0)
    lane = lax.broadcasted_iota(jnp.int32, (8, width), 1)
    small_eye = jnp.where(
        lax.broadcasted_iota(jnp.int32, (width, width), 0)
        == lax.broadcasted_iota(jnp.int32, (width, width), 1),
        1.0,
        0.0,
    )

    def group(g, _):
        first = pl.multiple_of(g * 8, 8)
        left = d_ref[pl.ds(first, 8), :width]
        right = d_ref[pl.ds(first, 8), width:]
        turned = pltpu.roll(left, lax.rem(width - first, width), 1)
        columns = [jnp.broadcast_to(turned[:, j : j + 1], (8, width)) for j in range(8)]
        for j in range(8):
            scale = lax.rsqrt(columns[j][j : j + 1, :])
            factor = columns[j] * scale
            for m in range(j + 1, 8):
                columns[m] = columns[m] - factor * factor[m : m + 1, :]
            row_left, row_right = left[j : j + 1, :] * scale, right[j : j + 1, :] * scale
            below, here = strip > j, strip == j
            left = jnp.where(here, row_left, jnp.where(below, left - factor * row_left, left))
            right = jnp.where(here, row_right, jnp.where(below, right - factor * row_right, right))
        later = jnp.where(lane >= first + 8, left, 0.0)
        both = jnp.concatenate([left, right], axis=1)
        d_ref[pl.ds(first, 8), :] = both
        d_ref[...] = d_ref[...] - short_dot(later, both)
        return 0

    for k in range(size // width):
        top, end = k * width, (k + 1) * width
        d_ref[:, :width] = a_ref[top:end, top:end]
        d_ref[:, width:] = small_eye
        lax.fori_loop(0, width // 8, group, 0)
        corner = d_ref[:, width:]
        done = jnp.dot(corner, x_ref[top:end, :end], precision=HIGHEST)
        x_ref[top:end, :end] = done
        if end < size:
            panel = jnp.dot(corner, a_ref[top:end, end:], precision=HIGHEST)
            a_ref[end:, end:] = a_ref[end:, end:] - dot_first(panel, panel)
            x_ref[end:, :end] = x_ref[end:, :end] - dot_first(panel, done)


def lower_inverse(gram_total):
    size = gram_total.shape[0]
    width = 128
    return pl.pallas_call(
        functools.partial(inverse_kernel, size, width),
        out_shape=jax.ShapeDtypeStruct((size, size), jnp.float32),
        in_specs=[pl.BlockSpec(memory_space=pltpu.VMEM)],
        out_specs=pl.BlockSpec(memory_space=pltpu.VMEM),
        scratch_shapes=[
            pltpu.VMEM((size, size), jnp.float32),
            pltpu.VMEM((width, 2 * width), jnp.float32),
        ],
        compiler_params=pltpu.CompilerParams(vmem_limit_bytes=24 * 2**20),
        name="lower_inverse",
    )(gram_total)


def narrow_device(sizes, momentum, grad, q_basis):
    own_rows = momentum.shape[0]
    basis_rows, rank = q_basis.shape
    devices = math.prod(sizes)
    features = basis_rows * devices
    blended = momentum + grad.astype(jnp.float32)
    blended_low = blended.astype(jnp.bfloat16)
    basis = gather(q_basis.astype(jnp.bfloat16), sizes, 0)
    projected = jnp.dot(blended_low, basis, preferred_element_type=jnp.float32)
    local_gram = jnp.dot(projected.T, projected, precision=HIGHEST)
    gram_total = gather(reduce_scatter(local_gram, sizes, 1), sizes, 2)
    inverse = lower_inverse(gram_total)
    orthonormal = jnp.dot(projected, inverse.T, precision=HIGHEST)
    ortho_low = orthonormal.astype(jnp.bfloat16)
    terms = jnp.dot(blended_low.T, ortho_low, preferred_element_type=jnp.float32)
    summed = reduce_scatter(terms.astype(jnp.bfloat16), sizes, 3)
    summed_low = gather(summed.astype(jnp.bfloat16), sizes, 4)
    wide = summed_low.astype(jnp.float32)
    column_rms = jnp.sqrt(jnp.mean(wide * wide, axis=0) + epsilon)
    q_next = summed / column_rms
    stacked = jnp.concatenate(
        [ortho_low, (orthonormal / column_rms).astype(jnp.bfloat16)], axis=0
    )
    result = jnp.dot(stacked, summed_low.T, preferred_element_type=jnp.float32)
    total_rows = own_rows * devices
    momentum_next = blended - (1.0 - damping) * result[:own_rows]
    update = (math.sqrt(total_rows * features / rank) * result[own_rows:]).astype(jnp.bfloat16)
    return (momentum_next, update, q_next)


def per_device(sizes, parts, momentum, grad, q_basis):
    own_rows = momentum.shape[0]
    basis_rows, rank = q_basis.shape
    if basis_rows % 128 or rank % 128 or own_rows % 128:
        return narrow_device(sizes, momentum, grad, q_basis)
    devices = math.prod(sizes)
    features = basis_rows * devices
    spread, stacked, turned, blended = right_factor(momentum, grad, q_basis, sizes, parts, 0)
    total_rows = own_rows * devices
    factor = math.sqrt(total_rows * features / rank)
    spread = spread.reshape(devices, rank, basis_rows)
    return finish(spread, stacked, turned, blended, factor)


def solution(mesh):
    spec = P(("mat", "fsdp"), None)
    return jax.shard_map(
        functools.partial(per_device, grid_of(mesh), mesh.shape["mat"]),
        mesh=mesh,
        in_specs=(spec, spec, spec),
        out_specs=(spec, spec, spec),
        check_vma=False,
    )
```

```python
import functools
import math

import jax
import jax.numpy as jnp
from jax import lax
from jax.experimental import pallas as pl
from jax.experimental.pallas import tpu as pltpu
from jax.sharding import PartitionSpec as P

damping = 0.95
epsilon = 1e-06
HIGHEST = lax.Precision.HIGHEST
MESH = pl.DeviceIdType.MESH


def grid_of(mesh):
    n = mesh.shape["fsdp"]
    at = list(mesh.axis_names).index("fsdp")
    try:
        line = mesh.devices.swapaxes(0, at).reshape(n, -1)[:, 0]
        spots = [tuple(d.coords) for d in line]
        axes = []
        for d in range(3):
            size = len({s[d] for s in spots})
            if size > 1:
                stride = next(i for i in range(n) if spots[i][d] != spots[0][d])
                axes.append((stride, size))
        sizes = [size for _, size in sorted(axes, reverse=True)]
        if math.prod(sizes) == n:
            return tuple([1] * (3 - len(sizes)) + sizes)
    except AttributeError:
        pass
    return (n // 4, 2, 2) if n % 4 == 0 else (1, 1, n)


def cut(rows, unit, sizes):
    units = rows // unit
    long_axis = max(range(3), key=lambda d: sizes[d])
    first, second = [d for d in range(3) if d != long_axis]
    tail = units // 8
    pairs = 2 if units >= 8 else 1
    share, extra = divmod(units - tail, 2 * pairs)
    plan = [(tail, (first, second, long_axis), 0)]
    for k in range(2 * pairs):
        short = (first, second) if k % 2 == 0 else (second, first)
        plan.append((share + (k < extra), (long_axis,) + short, k // 2))
    pieces, start = [], 0
    for count, order, wave in plan:
        if count:
            pieces.append((start, count * unit, order, wave))
        start += count * unit
    return pieces


def wavefront(pieces, phases):
    steps = [(piece[3] + phase, phase, p) for p, piece in enumerate(pieces) for phase in range(phases)]
    return [(phase, p) for _, phase, p in sorted(steps)]


def position(sizes):
    me = lax.axis_index("fsdp")
    return [
        lax.div(me, sizes[1] * sizes[2]),
        lax.rem(lax.div(me, sizes[2]), sizes[1]),
        lax.rem(me, sizes[2]),
    ]


def shifted(mine, sizes, d, off):
    return lax.rem(mine[d] + off, sizes[d])


def device_at(mine, sizes, d, coordinate):
    spot = list(mine)
    spot[d] = coordinate
    return {"fsdp": (spot[0] * sizes[1] + spot[1]) * sizes[2] + spot[2]}


def greet(mine, sizes):
    barrier = pltpu.get_barrier_semaphore()
    for d in range(3):
        for off in range(1, sizes[d]):
            target = device_at(mine, sizes, d, shifted(mine, sizes, d, off))
            pl.semaphore_signal(barrier, inc=1, device_id=target, device_id_type=MESH)
    pl.semaphore_wait(barrier, sum(sizes) - 3)


def gather_kernel(sizes, pieces, x_ref, o_ref, own_sem, send_sem, recv_sem):
    mine = position(sizes)
    own = pltpu.make_async_copy(x_ref, o_ref.at[mine[0], mine[1], mine[2]], own_sem)
    own.start()
    greet(mine, sizes)

    def block(piece, phase, coordinate):
        start, rows, order, _ = piece
        index = list(mine)
        index[order[phase]] = coordinate
        for d in order[:phase]:
            index[d] = slice(None)
        return o_ref.at[index[0], index[1], index[2], pl.ds(start, rows)]

    sent = []
    own_here = False
    for phase, p in wavefront(pieces, 3):
        piece = pieces[p]
        if phase:
            if not own_here:
                own.wait()
                own_here = True
            d = piece[2][phase - 1]
            for off in range(1, sizes[d]):
                landed = block(piece, phase - 1, shifted(mine, sizes, d, sizes[d] - off))
                pltpu.make_async_copy(landed, landed, recv_sem.at[p, phase - 1, off]).wait()
        d = piece[2][phase]
        for off in range(1, sizes[d]):
            target = block(piece, phase, mine[d])
            source = x_ref.at[pl.ds(piece[0], piece[1])] if phase == 0 else target
            copy = pltpu.make_async_remote_copy(
                src_ref=source,
                dst_ref=target,
                send_sem=send_sem.at[p, phase, off],
                recv_sem=recv_sem.at[p, phase, off],
                device_id=device_at(mine, sizes, d, shifted(mine, sizes, d, off)),
                device_id_type=MESH,
            )
            copy.start()
            sent.append(copy)
    for p, piece in enumerate(pieces):
        d = piece[2][2]
        for off in range(1, sizes[d]):
            landed = block(piece, 2, shifted(mine, sizes, d, sizes[d] - off))
            pltpu.make_async_copy(landed, landed, recv_sem.at[p, 2, off]).wait()
    for copy in sent:
        copy.wait_send()


def gather(x, sizes, number):
    rows, columns = x.shape
    unit = 8 if x.dtype == jnp.float32 else 16
    pieces = cut(rows, unit, sizes)
    sems = pltpu.SemaphoreType.DMA((len(pieces), 3, max(sizes)))
    out = pl.pallas_call(
        functools.partial(gather_kernel, sizes, pieces),
        out_shape=jax.ShapeDtypeStruct(sizes + (rows, columns), x.dtype),
        in_specs=[pl.BlockSpec(memory_space=pltpu.VMEM)],
        out_specs=pl.BlockSpec(memory_space=pltpu.VMEM),
        scratch_shapes=[pltpu.SemaphoreType.DMA, sems, sems],
        compiler_params=pltpu.CompilerParams(
            collective_id=number, has_side_effects=True, vmem_limit_bytes=32 * 2**20
        ),
        name=f"gather_{number}",
    )(x)
    return out.reshape(math.prod(sizes) * rows, columns)


def reduce_kernel(sizes, pieces, x_ref, o_ref, *scratch):
    mine = position(sizes)
    count = len(pieces)
    landing = scratch[: 3 * count]
    sums = scratch[3 * count : 5 * count]
    send_sem, recv_sem = scratch[5 * count :]
    greet(mine, sizes)
    sent = []

    def send(p, phase, d, off, source):
        copy = pltpu.make_async_remote_copy(
            src_ref=source,
            dst_ref=landing[3 * p + phase].at[off - 1],
            send_sem=send_sem.at[p, phase, off],
            recv_sem=recv_sem.at[p, phase, off],
            device_id=device_at(mine, sizes, d, shifted(mine, sizes, d, off)),
            device_id_type=MESH,
        )
        copy.start()
        sent.append(copy)

    def arrive(p, phase, d):
        for off in range(1, sizes[d]):
            here = landing[3 * p + phase].at[off - 1]
            pltpu.make_async_copy(here, here, recv_sem.at[p, phase, off]).wait()

    def begin(p, start, rows, order):
        d = order[2]
        for off in range(1, sizes[d]):
            index = [slice(None)] * 3
            index[d] = shifted(mine, sizes, d, off)
            send(p, 0, d, off, x_ref.at[index[0], index[1], index[2], pl.ds(start, rows)])

    def first_sums(p, start, rows, order):
        a, b, c = order
        arrive(p, 0, c)
        low, high = min(a, b), max(a, b)
        for off in list(range(1, sizes[b])) + [0]:
            at_b = shifted(mine, sizes, b, off)

            def one(at_a, _, off=off, at_b=at_b):
                index = [None] * 3
                index[a], index[b], index[c] = at_a, at_b, mine[c]
                total = x_ref[index[0], index[1], index[2], pl.ds(start, rows)].astype(jnp.float32)
                for k in range(sizes[c] - 1):
                    total += landing[3 * p][k, index[low], index[high]].astype(jnp.float32)
                if off:
                    sums[2 * p][off - 1, at_a] = total.astype(x_ref.dtype)
                else:
                    sums[2 * p + 1][at_a] = total
                return 0

            lax.fori_loop(0, sizes[a], one, 0)
        for off in range(1, sizes[b]):
            send(p, 1, b, off, sums[2 * p].at[off - 1])

    def second_sums(p, start, rows, order):
        a, b, c = order
        arrive(p, 1, b)
        for off in list(range(1, sizes[a])) + [0]:
            at_a = shifted(mine, sizes, a, off)
            total = sums[2 * p + 1][at_a]
            for k in range(sizes[b] - 1):
                total += landing[3 * p + 1][k, at_a].astype(jnp.float32)
            if off:
                landing[3 * p + 2][sizes[a] - 1 + off - 1] = total.astype(x_ref.dtype)
            else:
                sums[2 * p + 1][at_a] = total
        for off in range(1, sizes[a]):
            send(p, 2, a, off, landing[3 * p + 2].at[sizes[a] - 1 + off - 1])

    def last_sums(p, start, rows, order):
        a = order[0]
        arrive(p, 2, a)
        total = sums[2 * p + 1][mine[a]]
        for k in range(sizes[a] - 1):
            total += landing[3 * p + 2][k].astype(jnp.float32)
        o_ref[pl.ds(start, rows)] = total

    stages = (begin, first_sums, second_sums, last_sums)
    for phase, p in wavefront(pieces, 4):
        stages[phase](p, *pieces[p][:3])
    for copy in sent:
        copy.wait_send()


def reduce_scatter(x, sizes, number):
    n = math.prod(sizes)
    rows, columns = x.shape[0] // n, x.shape[1]
    unit = 8 if x.dtype == jnp.float32 else 16
    pieces = cut(rows, unit, sizes)
    landing, sums = [], []
    for _, part, (a, b, c), _ in pieces:
        low, high = min(a, b), max(a, b)
        many = lambda k: max(k, 1)
        landing += [
            pltpu.VMEM((many(sizes[c] - 1), sizes[low], sizes[high], part, columns), x.dtype),
            pltpu.VMEM((many(sizes[b] - 1), sizes[a], part, columns), x.dtype),
            pltpu.VMEM((many(2 * (sizes[a] - 1)), part, columns), x.dtype),
        ]
        sums += [
            pltpu.VMEM((many(sizes[b] - 1), sizes[a], part, columns), x.dtype),
            pltpu.VMEM((sizes[a], part, columns), jnp.float32),
        ]
    sems = pltpu.SemaphoreType.DMA((len(pieces), 3, max(sizes)))
    return pl.pallas_call(
        functools.partial(reduce_kernel, sizes, pieces),
        out_shape=jax.ShapeDtypeStruct((rows, columns), jnp.float32),
        in_specs=[pl.BlockSpec(memory_space=pltpu.VMEM)],
        out_specs=pl.BlockSpec(memory_space=pltpu.VMEM),
        scratch_shapes=landing + sums + [sems, sems],
        compiler_params=pltpu.CompilerParams(
            collective_id=number, has_side_effects=True, vmem_limit_bytes=40 * 2**20
        ),
        name=f"reduce_{number}",
    )(x.reshape(sizes + (rows, columns)))


def dot_first(left, right):
    return lax.dot_general(
        left, right, (((0,), (0,)), ((), ())), precision=HIGHEST, preferred_element_type=jnp.float32
    )


def three(x):
    high = x.astype(jnp.bfloat16).astype(jnp.float32)
    rest = x - high
    middle = rest.astype(jnp.bfloat16).astype(jnp.float32)
    return high, middle, rest - middle


def short_dot(left, right):
    h, m, l = three(left)
    lefts = jnp.concatenate([h, h, m, m, h, l], axis=0).astype(jnp.bfloat16)
    h, m, l = three(right)
    rights = jnp.concatenate([h, m, h, m, l, h], axis=0).astype(jnp.bfloat16)
    return lax.dot_general(
        lefts, rights, (((0,), (0,)), ((), ())), preferred_element_type=jnp.float32
    )


def nt_dot(left, right, precision=None):
    return lax.dot_general(
        left, right, (((1,), (1,)), ((), ())), precision=precision, preferred_element_type=jnp.float32
    )


def factor_block(width, d_ref, block):
    group = 32
    strip = lax.broadcasted_iota(jnp.int32, (group, width), 0)
    lane = lax.broadcasted_iota(jnp.int32, (group, width), 1)
    d_ref[:, :width] = block
    d_ref[:, width:] = jnp.where(
        lax.broadcasted_iota(jnp.int32, (width, width), 0)
        == lax.broadcasted_iota(jnp.int32, (width, width), 1),
        1.0,
        0.0,
    )
    for first in range(0, width, group):
        end = first + group
        left = d_ref[first:end, :width]
        right = d_ref[first:end, width:]
        columns = [
            jnp.broadcast_to(left[:, first + j : first + j + 1], (group, width)) for j in range(group)
        ]
        for j in range(group):
            scale = lax.rsqrt(columns[j][j : j + 1, :])
            factor = columns[j] * scale
            for m in range(j + 1, group):
                columns[m] = columns[m] - factor * factor[m : m + 1, :]
            row_left, row_right = left[j : j + 1, :] * scale, right[j : j + 1, :] * scale
            below, here = strip > j, strip == j
            left = jnp.where(here, row_left, jnp.where(below, left - factor * row_left, left))
            right = jnp.where(here, row_right, jnp.where(below, right - factor * row_right, right))
        d_ref[first:end, width:] = right
        if end < width:
            later = jnp.where(lane >= end, left, 0.0)
            both = jnp.concatenate([left, right], axis=1)
            d_ref[end:, :] = d_ref[end:, :] - short_dot(later, both)[end:]
    return d_ref[:, width:]


def split(rows, unit, sizes, k, tail):
    long_axis = max(range(3), key=lambda d: sizes[d])
    one, two = [d for d in range(3) if d != long_axis]
    if k % 2:
        one, two = two, one
    share, extra = divmod(rows // unit - tail, 2)
    plan = ((tail, (one, two, long_axis)), (share + extra, (long_axis, one, two)), (share, (long_axis, two, one)))
    pieces, start = [], 0
    for count, order in plan:
        if count:
            pieces.append((start, count * unit, order))
        start += count * unit
    return pieces


def flows_of(blocks, width, basis_rows, sizes):
    long_axis = max(range(3), key=lambda d: sizes[d])
    one, two = [d for d in range(3) if d != long_axis]
    devices = math.prod(sizes)
    flows = []
    for k in range(blocks):
        tail = basis_rows // 64 if 0 < k < blocks - 1 else 0
        flows += [("q", k) + piece for piece in split(basis_rows, 16, sizes, k, tail)]
    for k in range(blocks):
        order = (long_axis, two, one) if k % 2 else (long_axis, one, two)
        flows.append(("g", k, 0, (k + 1) * width // devices, order))
    for k in range(blocks):
        pieces = split(width, 16, sizes, k, width // 128)
        flows += [("s", k, k * width + start, rows, order) for start, rows, order in pieces]
    return flows


BLEND, PROJECT, TRACE, FACTOR, SCALE, TELL, HEAR = -1, -2, -3, -4, -5, -6, -7


TUNED = (
    10, 20, 40, 21, 50, -10, 30, 11, 41, 0, 31, 12, 42, 80, 60, 1, 81, 90, 51, 43,
    61, 2, 13, 70, 91, 32, 62, 82, 22, 3, 71, 52, -20, 100, 33, 23, -21, 63, 101, 92,
    72, 110, 83, 102, 73, 53, -22, 93, 103, 120, -23, 130, 111, 121, -30, 112, 104, 122, 131, 105,
    106, 113, 132, 123, -40, 114, 124, 150, 160, 133, 115, 134, 161, 151, 140, 125, 116, -41, 135, 126,
    162, 152, 180, 170, 190, -42, 200, 136, 141, 191, 163, 210, 171, 153, 181, -43, 230, 201, 172, 211,
    250, 182, 240, 220, 142, 192, 164, 154, 212, 241, 251, 202, 183, 242, 173, 155, 231, 143, 184, 213,
    203, 232, 144, 221, 243, 174, 165, 252, 214, 185, 222, 193, 233, 204, 244, 253, 234, 223, 215, 194,
    186, 254, 166, 224, 156, 205, 245, 175, 145, 195, 235, 255, 225, 176, 196, -51, 146, 246, 216, -50,
    256, 236, 206, -53, 226, -52,
)


def tuned_agenda(flows, blocks):
    steps = [divmod(code, 10) if code >= 0 else (-(-code // 10), -code % 10) for code in TUNED]
    plain = agenda(flows, blocks)
    known = sorted(step for step in steps if step[0] > TELL)
    return steps if known == sorted(plain) else plain


def agenda(flows, blocks):
    steps = [(0.5, (BLEND, 0))]
    begun = 9.0 * (blocks - 1) + 17
    for f, (kind, k, _, _, _) in enumerate(flows):
        if kind == "q":
            steps += [(9.0 * k + (0, 6, 10, 16)[stage], (f, stage)) for stage in range(4)]
        elif kind == "g" and k < blocks - 1:
            steps += [(9.0 * k + 17.01 + 3.0 * stage, (f, stage)) for stage in range(7)]
        elif kind == "g":
            late = (0, 3, 12.9, 13, 21.4, 21.5, 29.9)
            steps += [(begun + 0.02 + late[stage], (f, stage)) for stage in range(7)]
        else:
            steps += [(begun + 4.6 + 8.5 * (k + stage), (f, stage)) for stage in range(7)]
    for k in range(blocks):
        steps.append((9.0 * k + 16.5, (PROJECT, k)))
        steps.append((begun + 4 + 8.5 * k, (FACTOR, k)))
        steps.append((begun + 4.7 + 8.5 * (k + 6), (SCALE, k)))
    steps.append((begun + 0.1, (TRACE, 0)))
    steps.sort(key=lambda step: step[0])
    needs = {}
    need = lambda step, other: needs.setdefault(step, []).append(other)
    for f, (kind, k, _, _, _) in enumerate(flows):
        final = 3 if kind == "q" else 6
        for stage in range(final):
            need((f, stage + 1), (f, stage))
        if kind == "q":
            need((PROJECT, k), (f, final))
        elif kind == "g":
            need((f, 0), (PROJECT, k))
            need((FACTOR, k), (f, final))
        else:
            need((f, 0), (FACTOR, k))
            need((SCALE, k), (f, final))
    for k in range(blocks):
        need((PROJECT, k), (BLEND, 0))
        need((TRACE, 0), (PROJECT, k))
        need((FACTOR, k), (TRACE, 0))
        if k:
            need((PROJECT, k), (PROJECT, k - 1))
            need((FACTOR, k), (FACTOR, k - 1))
    order, done = [], set()

    def emit(step):
        if step not in done:
            for other in needs.get(step, ()):
                emit(other)
            done.add(step)
            order.append(step)

    for _, step in steps:
        emit(step)
    return order


def main_kernel(sizes, parts, flows, width, m_ref, g_ref, q_ref, o_ref, t_ref, qn_ref, m_buf, *scratch):
    mine = position(sizes)
    me = lax.axis_index("fsdp")
    devices = math.prod(sizes)
    rows, columns = m_ref.shape
    features, size = q_ref.shape
    blocks = size // width
    refs = list(scratch)
    take = lambda n: [refs.pop(0) for _ in range(n)]
    landing, sums = {}, {}
    for f, flow in enumerate(flows):
        if flow[0] != "q":
            landing[f] = take(3)
            sums[f] = take(2)
    grams = take(blocks)
    spreads = take(blocks)
    (g_buf, q_buf, b_ref, basis, p_ref, trace_own, trace_all, u_ref, x_ref, d_ref) = take(10)
    (terms, ot_ref, own_ref, gram_ref) = take(4)
    (in_sem, trace_send, trace_recv, rs_send, rs_recv, ag_send, ag_recv, pace) = take(8)
    base = [0, sizes[0] - 1, sizes[0] + sizes[1] - 2]
    each = sum(sizes) - 3
    basis_flows = sum(flow[0] == "q" for flow in flows)

    loads = [
        pltpu.make_async_copy(q_ref, q_buf, in_sem.at[0]),
        pltpu.make_async_copy(m_ref, m_buf, in_sem.at[1]),
        pltpu.make_async_copy(g_ref, g_buf, in_sem.at[2]),
    ]
    for load in loads:
        load.start()
    barrier = pltpu.get_barrier_semaphore()
    for off in range(1, devices):
        other = {"fsdp": lax.rem(me + off, devices)}
        pl.semaphore_signal(barrier, inc=1, device_id=other, device_id_type=MESH)
    part = lax.axis_index("mat")
    paired = parts == 2
    if paired:
        pl.semaphore_signal(barrier, inc=1, device_id={"mat": 1 - part}, device_id_type=MESH)
    loads[0].wait()
    for k in range(blocks):
        basis[k, mine[0], mine[1], mine[2]] = q_buf[:, k * width : (k + 1) * width].astype(basis.dtype)
    pl.semaphore_wait(barrier, devices - 1 + paired)
    sent = []

    kinds = ("q", "g", "s")

    def push(source, target, sems, f, d, off):
        summing = sems[0] is rs_send
        at = each * (f - summing * basis_flows) + base[d] + off - 1
        kind = flows[f][0]
        if kind == "g":
            gram_at = each * (2 * (f - basis_flows) + summing) + base[d] + off - 1
            send_sem = rs_send.at[gram_at]
        else:
            send_sem = ag_send.at[kinds.index(kind) + summing]
        copy = pltpu.make_async_remote_copy(
            src_ref=source,
            dst_ref=target,
            send_sem=send_sem,
            recv_sem=sems[1].at[at],
            device_id=device_at(mine, sizes, d, shifted(mine, sizes, d, off)),
            device_id_type=MESH,
        )
        copy.start()
        if kind == "g":
            sent.append(copy)

    def landed(ref, sem, f, d, off):
        at = each * (f - (sem is rs_recv) * basis_flows) + base[d] + off - 1
        pltpu.make_async_copy(ref, ref, sem.at[at]).wait()

    def block(f, phase, coordinate):
        kind, k, start, part, order = flows[f]
        index = list(mine)
        index[order[phase]] = coordinate
        for d in order[:phase]:
            index[d] = slice(None)
        if kind == "q":
            return basis.at[k, index[0], index[1], index[2], pl.ds(start, part)]
        target = spreads[k] if kind == "g" else o_ref
        return target.at[index[0], index[1], index[2], pl.ds(start, part)]

    def spread(f, phase):
        d = flows[f][4][phase]
        here = block(f, phase, mine[d])
        for off in range(1, sizes[d]):
            push(here, here, (ag_send, ag_recv), f, d, off)

    def gathered(f, phase):
        d = flows[f][4][phase]
        for off in range(1, sizes[d]):
            landed(block(f, phase, shifted(mine, sizes, d, sizes[d] - off)), ag_recv, f, d, off)

    def source(f):
        return grams[flows[f][1]] if flows[f][0] == "g" else terms

    def begin(f):
        _, _, start, part, order = flows[f]
        d = order[2]
        for off in range(1, sizes[d]):
            index = [slice(None)] * 3
            index[d] = shifted(mine, sizes, d, off)
            piece = source(f).at[index[0], index[1], index[2], pl.ds(start, part)]
            push(piece, landing[f][0].at[off - 1], (rs_send, rs_recv), f, d, off)

    def first_sums(f):
        _, _, start, part, (a, b, c) = flows[f]
        from_ref = source(f)
        for off in range(1, sizes[c]):
            landed(landing[f][0].at[off - 1], rs_recv, f, c, off)
        low, high = min(a, b), max(a, b)
        for off in list(range(1, sizes[b])) + [0]:
            at_b = shifted(mine, sizes, b, off)

            def one(at_a, _, off=off, at_b=at_b):
                index = [None] * 3
                index[a], index[b], index[c] = at_a, at_b, mine[c]
                total = from_ref[index[0], index[1], index[2], pl.ds(start, part)].astype(jnp.float32)
                for k in range(sizes[c] - 1):
                    total += landing[f][0][k, index[low], index[high]].astype(jnp.float32)
                if off:
                    sums[f][0][off - 1, at_a] = total.astype(from_ref.dtype)
                else:
                    sums[f][1][at_a] = total
                return 0

            lax.fori_loop(0, sizes[a], one, 0)
        for off in range(1, sizes[b]):
            push(sums[f][0].at[off - 1], landing[f][1].at[off - 1], (rs_send, rs_recv), f, b, off)

    def second_sums(f):
        _, _, start, part, (a, b, c) = flows[f]
        for off in range(1, sizes[b]):
            landed(landing[f][1].at[off - 1], rs_recv, f, b, off)
        last = landing[f][2]
        for off in list(range(1, sizes[a])) + [0]:
            at_a = shifted(mine, sizes, a, off)
            total = sums[f][1][at_a]
            for k in range(sizes[b] - 1):
                total += landing[f][1][k, at_a].astype(jnp.float32)
            if off:
                last[sizes[a] - 1 + off - 1] = total.astype(last.dtype)
            else:
                sums[f][1][at_a] = total
        for off in range(1, sizes[a]):
            push(last.at[sizes[a] - 1 + off - 1], last.at[off - 1], (rs_send, rs_recv), f, a, off)

    def last_sums(f):
        kind, k, start, part, (a, b, c) = flows[f]
        for off in range(1, sizes[a]):
            landed(landing[f][2].at[off - 1], rs_recv, f, a, off)
        total = sums[f][1][mine[a]]
        for n in range(sizes[a] - 1):
            total += landing[f][2][n].astype(jnp.float32)
        if kind == "s":
            own_ref[pl.ds(start, part), :] = total
            o_ref[mine[0], mine[1], mine[2], pl.ds(start, part)] = total.astype(o_ref.dtype)
        else:
            spreads[k][mine[0], mine[1], mine[2]] = total

    def spot(i):
        return (
            lax.div(i, sizes[1] * sizes[2]),
            lax.rem(lax.div(i, sizes[2]), sizes[1]),
            lax.rem(i, sizes[2]),
        )

    def lanes_of(i):
        return pl.ds(pl.multiple_of(i * features, features), features)

    def blend():
        loads[1].wait()
        loads[2].wait()

        def one(i, _):
            lanes = lanes_of(i)
            blended = m_buf[:, lanes] + g_buf[:, lanes].astype(jnp.float32)
            m_buf[:, lanes] = blended
            b_ref[:, lanes] = blended.astype(b_ref.dtype)
            return 0

        lax.fori_loop(0, devices, one, 0)

    def project(k):
        top, end = k * width, (k + 1) * width
        right = basis[k].reshape(columns, width)
        p_ref[:, top:end] = jnp.dot(b_ref[...], right, preferred_element_type=jnp.float32)
        if end == size:
            send_trace()
        column = dot_first(p_ref[:, :end], p_ref[:, top:end])
        part = end // devices
        for i in range(devices):
            at = (i // (sizes[1] * sizes[2]), i // sizes[2] % sizes[1], i % sizes[2])
            grams[k][at[0], at[1], at[2]] = column[i * part : (i + 1) * part]

    def send_trace():
        square = p_ref[...] * p_ref[...]
        folded = square[:, :128]
        for i in range(1, size // 128):
            folded = folded + square[:, i * 128 : (i + 1) * 128]
        tile = folded[:8]
        for i in range(1, rows // 8):
            tile = tile + folded[i * 8 : (i + 1) * 8]
        trace_own[...] = tile
        trace_all[me] = tile
        for off in range(1, devices):
            copy = pltpu.make_async_remote_copy(
                src_ref=trace_own,
                dst_ref=trace_all.at[me],
                send_sem=trace_send.at[off],
                recv_sem=trace_recv.at[off],
                device_id={"fsdp": lax.rem(me + off, devices)},
                device_id_type=MESH,
            )
            copy.start()
            sent.append(copy)

    def ridge():
        for off in range(1, devices):
            here = trace_all.at[lax.rem(me + devices - off, devices)]
            pltpu.make_async_copy(here, here, trace_recv.at[off]).wait()
        return jnp.sum(jnp.sum(trace_all[...], axis=0), keepdims=True) * (0.0001 / size)

    small_eye = lax.broadcasted_iota(jnp.int32, (width, width), 0) == lax.broadcasted_iota(
        jnp.int32, (width, width), 1
    )
    shared = {}

    def factor(k):
        top, end = k * width, (k + 1) * width
        if k == 0:
            shared["ridge"] = ridge()
        gram_ref[:end, :] = spreads[k][...].reshape(end, width)
        for j in range(k):
            near, far = j * width, (j + 1) * width
            upper = gram_ref[near:far, :]
            if j:
                upper = upper - dot_first(u_ref[:near, near:far], u_ref[:near, top:end])
            u_ref[near:far, top:end] = jnp.dot(x_ref[near:far, near:far], upper, precision=HIGHEST)
        corner = gram_ref[top:end, :] + jnp.where(small_eye, shared["ridge"], 0.0)
        if k:
            panel = u_ref[:top, top:end]
            corner = corner - dot_first(panel, panel)
        inverse = factor_block(width, d_ref, corner)
        x_ref[top:end, top:end] = inverse
        if k:
            rest = dot_first(u_ref[:top, top:end], x_ref[:top, :top])
            x_ref[top:end, :top] = -jnp.dot(inverse, rest, precision=HIGHEST)
        if end < size:
            x_ref[top:end, end:] = jnp.zeros((width, size - end), jnp.float32)
        ortho = nt_dot(x_ref[top:end, :end], p_ref[:, :end], HIGHEST)
        ot_ref[top:end, :] = ortho
        t_ref[:rows, top:end] = ortho.T.astype(t_ref.dtype)
        low = ortho.astype(jnp.bfloat16)

        each_step = math.gcd(devices, 4)

        def one(i, _):
            for n in range(each_step):
                at = spot(i * each_step + n)
                lanes = lanes_of(i * each_step + n)
                term = jnp.dot(low, b_ref[:, lanes], preferred_element_type=jnp.float32)
                terms[at[0], at[1], at[2], top:end] = term.astype(terms.dtype)
            return 0

        lax.fori_loop(0, devices // each_step, one, 0)

    def scale_block(k):
        top, end = k * width, (k + 1) * width

        def squares(i, total):
            at = spot(i)
            wide = o_ref[at[0], at[1], at[2], top:end].astype(jnp.float32)
            return total + wide * wide

        total = lax.fori_loop(0, devices, squares, jnp.zeros((width, features), jnp.float32))
        mean = jnp.sum(total, axis=1, keepdims=True) / (devices * features)
        column_rms = jnp.sqrt(mean + epsilon)
        qn_ref[top:end, :] = own_ref[top:end, :] / column_rms
        t_ref[rows:, top:end] = (ot_ref[top:end, :] / column_rms).T.astype(t_ref.dtype)

    def serve(f, stage):
        if flows[f][0] != "q":
            if stage < 4:
                (begin, first_sums, second_sums, last_sums)[stage](f)
            if stage < 3:
                return
            stage = stage - 3
        if stage:
            gathered(f, stage - 1)
        if stage < 3:
            spread(f, stage)

    def tell(n):
        if paired:

            @pl.when(part == n % 2)
            def _():
                pl.semaphore_signal(pace.at[n], inc=1, device_id={"mat": 1 - part}, device_id_type=MESH)

    def hear(n):
        if paired:

            @pl.when(part != n % 2)
            def _():
                pl.semaphore_wait(pace.at[n], 1)

    special = {
        BLEND: lambda k: blend(),
        PROJECT: project,
        TRACE: lambda k: None,
        FACTOR: factor,
        SCALE: scale_block,
        TELL: tell,
        HEAR: hear,
    }
    for what, stage in tuned_agenda(flows, blocks):
        if what < 0:
            special[what](stage)
        else:
            serve(what, stage)
        if (what, stage) == (FACTOR, blocks - 1):
            while sent:
                sent.pop().wait_send()
    shares = size // devices * (devices - 1)
    everything = terms.at[:, :, :, pl.ds(0, shares)]
    for n in (0, 2, 3):
        pltpu.make_async_copy(everything, everything, ag_send.at[n]).wait()


def right_factor(momentum, grad, q_basis, sizes, parts, number):
    rows, columns = momentum.shape
    features, size = q_basis.shape
    width = 128
    blocks = size // width
    devices = math.prod(sizes)
    flows = flows_of(blocks, width, features, sizes)
    low_type = jnp.bfloat16
    many = lambda k: max(k, 1)
    scratch = []
    for kind, _, _, part, (a, b, c) in flows:
        if kind == "q":
            continue
        low, high = min(a, b), max(a, b)
        lanes, kept = (width, jnp.float32) if kind == "g" else (features, low_type)
        scratch += [
            pltpu.VMEM((many(sizes[c] - 1), sizes[low], sizes[high], part, lanes), kept),
            pltpu.VMEM((many(sizes[b] - 1), sizes[a], part, lanes), kept),
            pltpu.VMEM((many(2 * (sizes[a] - 1)), part, lanes), kept),
            pltpu.VMEM((many(sizes[b] - 1), sizes[a], part, lanes), kept),
            pltpu.VMEM((sizes[a], part, lanes), jnp.float32),
        ]
    chunks = [pltpu.VMEM(sizes + ((k + 1) * width // devices, width), jnp.float32) for k in range(blocks)]
    sums_flows = sum(flow[0] != "q" for flow in flows)
    sems = pltpu.SemaphoreType.DMA((len(flows) * (sum(sizes) - 3),))
    sum_sems = pltpu.SemaphoreType.DMA((sums_flows * (sum(sizes) - 3),))
    scratch += chunks + chunks
    scratch += [
        pltpu.VMEM((rows, columns), low_type),
        pltpu.VMEM((features, size), jnp.float32),
        pltpu.VMEM((rows, columns), low_type),
        pltpu.VMEM((blocks,) + sizes + (features, width), low_type),
        pltpu.VMEM((rows, size), jnp.float32),
        pltpu.VMEM((8, 128), jnp.float32),
        pltpu.VMEM((devices, 8, 128), jnp.float32),
        pltpu.VMEM((size, size), jnp.float32),
        pltpu.VMEM((size, size), jnp.float32),
        pltpu.VMEM((width, 2 * width), jnp.float32),
        pltpu.VMEM(sizes + (size, features), low_type),
        pltpu.VMEM((size, rows), jnp.float32),
        pltpu.VMEM((size, features), jnp.float32),
        pltpu.VMEM((size, width), jnp.float32),
        pltpu.SemaphoreType.DMA((3,)),
        pltpu.SemaphoreType.DMA((devices,)),
        pltpu.SemaphoreType.DMA((devices,)),
        pltpu.SemaphoreType.DMA((2 * blocks * (sum(sizes) - 3),)),
        sum_sems,
        pltpu.SemaphoreType.DMA((4,)),
        sems,
        pltpu.SemaphoreType.REGULAR((4,)),
    ]
    vmem = pl.BlockSpec(memory_space=pltpu.VMEM)
    return pl.pallas_call(
        functools.partial(main_kernel, sizes, parts, flows, width),
        out_shape=(
            pltpu.VMEM(sizes + (size, features), low_type),
            pltpu.VMEM((2 * rows, size), low_type),
            pltpu.VMEM((size, features), jnp.float32),
            pltpu.VMEM((rows, columns), jnp.float32),
        ),
        in_specs=[pl.BlockSpec(memory_space=pltpu.HBM)] * 3,
        out_specs=(vmem, vmem, vmem, vmem),
        scratch_shapes=scratch,
        compiler_params=pltpu.CompilerParams(
            collective_id=number, has_side_effects=True, vmem_limit_bytes=48 * 2**20
        ),
        name=f"factor_{number}",
    )(momentum, grad, q_basis)


def finish_kernel(step, factor, s_ref, t_ref, q_ref, m_ref, mo_ref, uo_ref, qo_ref, m_buf, u_buf, q_buf, m_sem, u_sem, q_sem):
    rows = m_ref.shape[0]
    blocks, rank, features = s_ref.shape
    q_buf[...] = q_ref[...].T
    q_copy = pltpu.make_async_copy(q_buf, qo_ref, q_sem)
    q_copy.start()

    def copies(slot, i):
        lanes = pl.ds(pl.multiple_of(i * features, features), features)
        return (
            pltpu.make_async_copy(m_buf.at[slot], mo_ref.at[:, lanes], m_sem.at[slot]),
            pltpu.make_async_copy(u_buf.at[slot], uo_ref.at[:, lanes], u_sem.at[slot]),
        )

    slots = m_buf.shape[0]
    wide = math.gcd(blocks, slots // 2)

    def one(step_index, _):
        for n in range(wide):
            i = step_index * wide + n
            slot = lax.rem(i, slots)

            @pl.when(i >= slots)
            def _(slot=slot, i=i):
                for copy in copies(slot, i - slots):
                    copy.wait()

        results = [
            jnp.dot(t_ref[...], s_ref[step_index * wide + n], preferred_element_type=jnp.float32)
            for n in range(wide)
        ]
        for n in range(wide):
            i = step_index * wide + n
            slot = lax.rem(i, slots)
            lanes = pl.ds(pl.multiple_of(i * features, features), features)
            m_buf[slot] = m_ref[:, lanes] - step * results[n][:rows]
            u_buf[slot] = (factor * results[n][rows:]).astype(u_buf.dtype)
            for copy in copies(slot, i):
                copy.start()
        return 0

    lax.fori_loop(0, blocks // wide, one, 0)
    for i in range(max(blocks - slots, 0), blocks):
        for copy in copies(i % slots, i):
            copy.wait()
    q_copy.wait()


def finish(spread, stacked, turned, blended, factor):
    rows, columns = blended.shape
    blocks, rank, features = spread.shape
    vmem = pl.BlockSpec(memory_space=pltpu.VMEM)
    anywhere = pl.BlockSpec(memory_space=pl.ANY)
    slots = 8
    return pl.pallas_call(
        functools.partial(finish_kernel, 1.0 - damping, factor),
        out_shape=(
            jax.ShapeDtypeStruct((rows, columns), jnp.float32),
            jax.ShapeDtypeStruct((rows, columns), jnp.bfloat16),
            jax.ShapeDtypeStruct((features, rank), jnp.float32),
        ),
        in_specs=[vmem] * 4,
        out_specs=(anywhere,) * 3,
        scratch_shapes=[
            pltpu.VMEM((slots, rows, features), jnp.float32),
            pltpu.VMEM((slots, rows, features), jnp.bfloat16),
            pltpu.VMEM((features, rank), jnp.float32),
            pltpu.SemaphoreType.DMA((slots,)),
            pltpu.SemaphoreType.DMA((slots,)),
            pltpu.SemaphoreType.DMA,
        ],
        compiler_params=pltpu.CompilerParams(vmem_limit_bytes=16 * 2**20),
        name="finish",
    )(spread, stacked, turned, blended)


def inverse_kernel(size, width, g_ref, x_ref, a_ref, d_ref):
    eye = lax.broadcasted_iota(jnp.int32, (size, size), 0) == lax.broadcasted_iota(
        jnp.int32, (size, size), 1
    )
    gram = g_ref[...]
    trace = jnp.sum(jnp.where(eye, gram, 0.0), keepdims=True)
    a_ref[...] = gram + jnp.where(eye, 0.0001 * trace / size, 0.0)
    x_ref[...] = jnp.where(eye, 1.0, 0.0)
    strip = lax.broadcasted_iota(jnp.int32, (8, width), 0)
    lane = lax.broadcasted_iota(jnp.int32, (8, width), 1)
    small_eye = jnp.where(
        lax.broadcasted_iota(jnp.int32, (width, width), 0)
        == lax.broadcasted_iota(jnp.int32, (width, width), 1),
        1.0,
        0.0,
    )

    def group(g, _):
        first = pl.multiple_of(g * 8, 8)
        left = d_ref[pl.ds(first, 8), :width]
        right = d_ref[pl.ds(first, 8), width:]
        turned = pltpu.roll(left, lax.rem(width - first, width), 1)
        columns = [jnp.broadcast_to(turned[:, j : j + 1], (8, width)) for j in range(8)]
        for j in range(8):
            scale = lax.rsqrt(columns[j][j : j + 1, :])
            factor = columns[j] * scale
            for m in range(j + 1, 8):
                columns[m] = columns[m] - factor * factor[m : m + 1, :]
            row_left, row_right = left[j : j + 1, :] * scale, right[j : j + 1, :] * scale
            below, here = strip > j, strip == j
            left = jnp.where(here, row_left, jnp.where(below, left - factor * row_left, left))
            right = jnp.where(here, row_right, jnp.where(below, right - factor * row_right, right))
        later = jnp.where(lane >= first + 8, left, 0.0)
        both = jnp.concatenate([left, right], axis=1)
        d_ref[pl.ds(first, 8), :] = both
        d_ref[...] = d_ref[...] - short_dot(later, both)
        return 0

    for k in range(size // width):
        top, end = k * width, (k + 1) * width
        d_ref[:, :width] = a_ref[top:end, top:end]
        d_ref[:, width:] = small_eye
        lax.fori_loop(0, width // 8, group, 0)
        corner = d_ref[:, width:]
        done = jnp.dot(corner, x_ref[top:end, :end], precision=HIGHEST)
        x_ref[top:end, :end] = done
        if end < size:
            panel = jnp.dot(corner, a_ref[top:end, end:], precision=HIGHEST)
            a_ref[end:, end:] = a_ref[end:, end:] - dot_first(panel, panel)
            x_ref[end:, :end] = x_ref[end:, :end] - dot_first(panel, done)


def lower_inverse(gram_total):
    size = gram_total.shape[0]
    width = 128
    return pl.pallas_call(
        functools.partial(inverse_kernel, size, width),
        out_shape=jax.ShapeDtypeStruct((size, size), jnp.float32),
        in_specs=[pl.BlockSpec(memory_space=pltpu.VMEM)],
        out_specs=pl.BlockSpec(memory_space=pltpu.VMEM),
        scratch_shapes=[
            pltpu.VMEM((size, size), jnp.float32),
            pltpu.VMEM((width, 2 * width), jnp.float32),
        ],
        compiler_params=pltpu.CompilerParams(vmem_limit_bytes=24 * 2**20),
        name="lower_inverse",
    )(gram_total)


def narrow_device(sizes, momentum, grad, q_basis):
    own_rows = momentum.shape[0]
    basis_rows, rank = q_basis.shape
    devices = math.prod(sizes)
    features = basis_rows * devices
    blended = momentum + grad.astype(jnp.float32)
    blended_low = blended.astype(jnp.bfloat16)
    basis = gather(q_basis.astype(jnp.bfloat16), sizes, 0)
    projected = jnp.dot(blended_low, basis, preferred_element_type=jnp.float32)
    local_gram = jnp.dot(projected.T, projected, precision=HIGHEST)
    gram_total = gather(reduce_scatter(local_gram, sizes, 1), sizes, 2)
    inverse = lower_inverse(gram_total)
    orthonormal = jnp.dot(projected, inverse.T, precision=HIGHEST)
    ortho_low = orthonormal.astype(jnp.bfloat16)
    terms = jnp.dot(blended_low.T, ortho_low, preferred_element_type=jnp.float32)
    summed = reduce_scatter(terms.astype(jnp.bfloat16), sizes, 3)
    summed_low = gather(summed.astype(jnp.bfloat16), sizes, 4)
    wide = summed_low.astype(jnp.float32)
    column_rms = jnp.sqrt(jnp.mean(wide * wide, axis=0) + epsilon)
    q_next = summed / column_rms
    stacked = jnp.concatenate(
        [ortho_low, (orthonormal / column_rms).astype(jnp.bfloat16)], axis=0
    )
    result = jnp.dot(stacked, summed_low.T, preferred_element_type=jnp.float32)
    total_rows = own_rows * devices
    momentum_next = blended - (1.0 - damping) * result[:own_rows]
    update = (math.sqrt(total_rows * features / rank) * result[own_rows:]).astype(jnp.bfloat16)
    return (momentum_next, update, q_next)


def per_device(sizes, parts, momentum, grad, q_basis):
    own_rows = momentum.shape[0]
    basis_rows, rank = q_basis.shape
    if basis_rows % 128 or rank % 128 or own_rows % 128:
        return narrow_device(sizes, momentum, grad, q_basis)
    devices = math.prod(sizes)
    features = basis_rows * devices
    spread, stacked, turned, blended = right_factor(momentum, grad, q_basis, sizes, parts, 0)
    total_rows = own_rows * devices
    factor = math.sqrt(total_rows * features / rank)
    spread = spread.reshape(devices, rank, basis_rows)
    return finish(spread, stacked, turned, blended, factor)


def solution(mesh):
    spec = P(("mat", "fsdp"), None)
    return jax.shard_map(
        functools.partial(per_device, grid_of(mesh), mesh.shape["mat"]),
        mesh=mesh,
        in_specs=(spec, spec, spec),
        out_specs=(spec, spec, spec),
        check_vma=False,
    )
```

```python
import functools
import math

import jax
import jax.numpy as jnp
from jax import lax
from jax.experimental import pallas as pl
from jax.experimental.pallas import tpu as pltpu
from jax.sharding import PartitionSpec as P

damping = 0.95
epsilon = 1e-06
HIGHEST = lax.Precision.HIGHEST
MESH = pl.DeviceIdType.MESH


def grid_of(mesh):
    n = mesh.shape["fsdp"]
    at = list(mesh.axis_names).index("fsdp")
    try:
        line = mesh.devices.swapaxes(0, at).reshape(n, -1)[:, 0]
        spots = [tuple(d.coords) for d in line]
        axes = []
        for d in range(3):
            size = len({s[d] for s in spots})
            if size > 1:
                stride = next(i for i in range(n) if spots[i][d] != spots[0][d])
                axes.append((stride, size))
        sizes = [size for _, size in sorted(axes, reverse=True)]
        if math.prod(sizes) == n:
            return tuple([1] * (3 - len(sizes)) + sizes)
    except AttributeError:
        pass
    return (n // 4, 2, 2) if n % 4 == 0 else (1, 1, n)


def cut(rows, unit, sizes):
    units = rows // unit
    long_axis = max(range(3), key=lambda d: sizes[d])
    first, second = [d for d in range(3) if d != long_axis]
    tail = units // 8
    pairs = 2 if units >= 8 else 1
    share, extra = divmod(units - tail, 2 * pairs)
    plan = [(tail, (first, second, long_axis), 0)]
    for k in range(2 * pairs):
        short = (first, second) if k % 2 == 0 else (second, first)
        plan.append((share + (k < extra), (long_axis,) + short, k // 2))
    pieces, start = [], 0
    for count, order, wave in plan:
        if count:
            pieces.append((start, count * unit, order, wave))
        start += count * unit
    return pieces


def wavefront(pieces, phases):
    steps = [(piece[3] + phase, phase, p) for p, piece in enumerate(pieces) for phase in range(phases)]
    return [(phase, p) for _, phase, p in sorted(steps)]


def position(sizes):
    me = lax.axis_index("fsdp")
    return [
        lax.div(me, sizes[1] * sizes[2]),
        lax.rem(lax.div(me, sizes[2]), sizes[1]),
        lax.rem(me, sizes[2]),
    ]


def shifted(mine, sizes, d, off):
    return lax.rem(mine[d] + off, sizes[d])


def device_at(mine, sizes, d, coordinate):
    spot = list(mine)
    spot[d] = coordinate
    return {"fsdp": (spot[0] * sizes[1] + spot[1]) * sizes[2] + spot[2]}


def greet(mine, sizes):
    barrier = pltpu.get_barrier_semaphore()
    for d in range(3):
        for off in range(1, sizes[d]):
            target = device_at(mine, sizes, d, shifted(mine, sizes, d, off))
            pl.semaphore_signal(barrier, inc=1, device_id=target, device_id_type=MESH)
    pl.semaphore_wait(barrier, sum(sizes) - 3)


def gather_kernel(sizes, pieces, x_ref, o_ref, own_sem, send_sem, recv_sem):
    mine = position(sizes)
    own = pltpu.make_async_copy(x_ref, o_ref.at[mine[0], mine[1], mine[2]], own_sem)
    own.start()
    greet(mine, sizes)

    def block(piece, phase, coordinate):
        start, rows, order, _ = piece
        index = list(mine)
        index[order[phase]] = coordinate
        for d in order[:phase]:
            index[d] = slice(None)
        return o_ref.at[index[0], index[1], index[2], pl.ds(start, rows)]

    sent = []
    own_here = False
    for phase, p in wavefront(pieces, 3):
        piece = pieces[p]
        if phase:
            if not own_here:
                own.wait()
                own_here = True
            d = piece[2][phase - 1]
            for off in range(1, sizes[d]):
                landed = block(piece, phase - 1, shifted(mine, sizes, d, sizes[d] - off))
                pltpu.make_async_copy(landed, landed, recv_sem.at[p, phase - 1, off]).wait()
        d = piece[2][phase]
        for off in range(1, sizes[d]):
            target = block(piece, phase, mine[d])
            source = x_ref.at[pl.ds(piece[0], piece[1])] if phase == 0 else target
            copy = pltpu.make_async_remote_copy(
                src_ref=source,
                dst_ref=target,
                send_sem=send_sem.at[p, phase, off],
                recv_sem=recv_sem.at[p, phase, off],
                device_id=device_at(mine, sizes, d, shifted(mine, sizes, d, off)),
                device_id_type=MESH,
            )
            copy.start()
            sent.append(copy)
    for p, piece in enumerate(pieces):
        d = piece[2][2]
        for off in range(1, sizes[d]):
            landed = block(piece, 2, shifted(mine, sizes, d, sizes[d] - off))
            pltpu.make_async_copy(landed, landed, recv_sem.at[p, 2, off]).wait()
    for copy in sent:
        copy.wait_send()


def gather(x, sizes, number):
    rows, columns = x.shape
    unit = 8 if x.dtype == jnp.float32 else 16
    pieces = cut(rows, unit, sizes)
    sems = pltpu.SemaphoreType.DMA((len(pieces), 3, max(sizes)))
    out = pl.pallas_call(
        functools.partial(gather_kernel, sizes, pieces),
        out_shape=jax.ShapeDtypeStruct(sizes + (rows, columns), x.dtype),
        in_specs=[pl.BlockSpec(memory_space=pltpu.VMEM)],
        out_specs=pl.BlockSpec(memory_space=pltpu.VMEM),
        scratch_shapes=[pltpu.SemaphoreType.DMA, sems, sems],
        compiler_params=pltpu.CompilerParams(
            collective_id=number, has_side_effects=True, vmem_limit_bytes=32 * 2**20
        ),
        name=f"gather_{number}",
    )(x)
    return out.reshape(math.prod(sizes) * rows, columns)


def reduce_kernel(sizes, pieces, x_ref, o_ref, *scratch):
    mine = position(sizes)
    count = len(pieces)
    landing = scratch[: 3 * count]
    sums = scratch[3 * count : 5 * count]
    send_sem, recv_sem = scratch[5 * count :]
    greet(mine, sizes)
    sent = []

    def send(p, phase, d, off, source):
        copy = pltpu.make_async_remote_copy(
            src_ref=source,
            dst_ref=landing[3 * p + phase].at[off - 1],
            send_sem=send_sem.at[p, phase, off],
            recv_sem=recv_sem.at[p, phase, off],
            device_id=device_at(mine, sizes, d, shifted(mine, sizes, d, off)),
            device_id_type=MESH,
        )
        copy.start()
        sent.append(copy)

    def arrive(p, phase, d):
        for off in range(1, sizes[d]):
            here = landing[3 * p + phase].at[off - 1]
            pltpu.make_async_copy(here, here, recv_sem.at[p, phase, off]).wait()

    def begin(p, start, rows, order):
        d = order[2]
        for off in range(1, sizes[d]):
            index = [slice(None)] * 3
            index[d] = shifted(mine, sizes, d, off)
            send(p, 0, d, off, x_ref.at[index[0], index[1], index[2], pl.ds(start, rows)])

    def first_sums(p, start, rows, order):
        a, b, c = order
        arrive(p, 0, c)
        low, high = min(a, b), max(a, b)
        for off in list(range(1, sizes[b])) + [0]:
            at_b = shifted(mine, sizes, b, off)

            def one(at_a, _, off=off, at_b=at_b):
                index = [None] * 3
                index[a], index[b], index[c] = at_a, at_b, mine[c]
                total = x_ref[index[0], index[1], index[2], pl.ds(start, rows)].astype(jnp.float32)
                for k in range(sizes[c] - 1):
                    total += landing[3 * p][k, index[low], index[high]].astype(jnp.float32)
                if off:
                    sums[2 * p][off - 1, at_a] = total.astype(x_ref.dtype)
                else:
                    sums[2 * p + 1][at_a] = total
                return 0

            lax.fori_loop(0, sizes[a], one, 0)
        for off in range(1, sizes[b]):
            send(p, 1, b, off, sums[2 * p].at[off - 1])

    def second_sums(p, start, rows, order):
        a, b, c = order
        arrive(p, 1, b)
        for off in list(range(1, sizes[a])) + [0]:
            at_a = shifted(mine, sizes, a, off)
            total = sums[2 * p + 1][at_a]
            for k in range(sizes[b] - 1):
                total += landing[3 * p + 1][k, at_a].astype(jnp.float32)
            if off:
                landing[3 * p + 2][sizes[a] - 1 + off - 1] = total.astype(x_ref.dtype)
            else:
                sums[2 * p + 1][at_a] = total
        for off in range(1, sizes[a]):
            send(p, 2, a, off, landing[3 * p + 2].at[sizes[a] - 1 + off - 1])

    def last_sums(p, start, rows, order):
        a = order[0]
        arrive(p, 2, a)
        total = sums[2 * p + 1][mine[a]]
        for k in range(sizes[a] - 1):
            total += landing[3 * p + 2][k].astype(jnp.float32)
        o_ref[pl.ds(start, rows)] = total

    stages = (begin, first_sums, second_sums, last_sums)
    for phase, p in wavefront(pieces, 4):
        stages[phase](p, *pieces[p][:3])
    for copy in sent:
        copy.wait_send()


def reduce_scatter(x, sizes, number):
    n = math.prod(sizes)
    rows, columns = x.shape[0] // n, x.shape[1]
    unit = 8 if x.dtype == jnp.float32 else 16
    pieces = cut(rows, unit, sizes)
    landing, sums = [], []
    for _, part, (a, b, c), _ in pieces:
        low, high = min(a, b), max(a, b)
        many = lambda k: max(k, 1)
        landing += [
            pltpu.VMEM((many(sizes[c] - 1), sizes[low], sizes[high], part, columns), x.dtype),
            pltpu.VMEM((many(sizes[b] - 1), sizes[a], part, columns), x.dtype),
            pltpu.VMEM((many(2 * (sizes[a] - 1)), part, columns), x.dtype),
        ]
        sums += [
            pltpu.VMEM((many(sizes[b] - 1), sizes[a], part, columns), x.dtype),
            pltpu.VMEM((sizes[a], part, columns), jnp.float32),
        ]
    sems = pltpu.SemaphoreType.DMA((len(pieces), 3, max(sizes)))
    return pl.pallas_call(
        functools.partial(reduce_kernel, sizes, pieces),
        out_shape=jax.ShapeDtypeStruct((rows, columns), jnp.float32),
        in_specs=[pl.BlockSpec(memory_space=pltpu.VMEM)],
        out_specs=pl.BlockSpec(memory_space=pltpu.VMEM),
        scratch_shapes=landing + sums + [sems, sems],
        compiler_params=pltpu.CompilerParams(
            collective_id=number, has_side_effects=True, vmem_limit_bytes=40 * 2**20
        ),
        name=f"reduce_{number}",
    )(x.reshape(sizes + (rows, columns)))


def dot_first(left, right):
    return lax.dot_general(
        left, right, (((0,), (0,)), ((), ())), precision=HIGHEST, preferred_element_type=jnp.float32
    )


def three(x):
    high = x.astype(jnp.bfloat16).astype(jnp.float32)
    rest = x - high
    middle = rest.astype(jnp.bfloat16).astype(jnp.float32)
    return high, middle, rest - middle


def short_dot(left, right):
    h, m, l = three(left)
    lefts = jnp.concatenate([h, h, m, m, h, l], axis=0).astype(jnp.bfloat16)
    h, m, l = three(right)
    rights = jnp.concatenate([h, m, h, m, l, h], axis=0).astype(jnp.bfloat16)
    return lax.dot_general(
        lefts, rights, (((0,), (0,)), ((), ())), preferred_element_type=jnp.float32
    )


def nt_dot(left, right, precision=None):
    return lax.dot_general(
        left, right, (((1,), (1,)), ((), ())), precision=precision, preferred_element_type=jnp.float32
    )


def factor_block(width, d_ref, block):
    group = 32
    strip = lax.broadcasted_iota(jnp.int32, (group, width), 0)
    lane = lax.broadcasted_iota(jnp.int32, (group, width), 1)
    d_ref[:, :width] = block
    d_ref[:, width:] = jnp.where(
        lax.broadcasted_iota(jnp.int32, (width, width), 0)
        == lax.broadcasted_iota(jnp.int32, (width, width), 1),
        1.0,
        0.0,
    )
    for first in range(0, width, group):
        end = first + group
        left = d_ref[first:end, :width]
        right = d_ref[first:end, width:]
        columns = [
            jnp.broadcast_to(left[:, first + j : first + j + 1], (group, width)) for j in range(group)
        ]
        for j in range(group):
            scale = lax.rsqrt(columns[j][j : j + 1, :])
            factor = columns[j] * scale
            for m in range(j + 1, group):
                columns[m] = columns[m] - factor * factor[m : m + 1, :]
            row_left, row_right = left[j : j + 1, :] * scale, right[j : j + 1, :] * scale
            below, here = strip > j, strip == j
            left = jnp.where(here, row_left, jnp.where(below, left - factor * row_left, left))
            right = jnp.where(here, row_right, jnp.where(below, right - factor * row_right, right))
        d_ref[first:end, width:] = right
        if end < width:
            later = jnp.where(lane >= end, left, 0.0)
            both = jnp.concatenate([left, right], axis=1)
            d_ref[end:, :] = d_ref[end:, :] - short_dot(later, both)[end:]
    return d_ref[:, width:]


def split(rows, unit, sizes, k, tail):
    long_axis = max(range(3), key=lambda d: sizes[d])
    one, two = [d for d in range(3) if d != long_axis]
    if k % 2:
        one, two = two, one
    share, extra = divmod(rows // unit - tail, 2)
    plan = ((tail, (one, two, long_axis)), (share + extra, (long_axis, one, two)), (share, (long_axis, two, one)))
    pieces, start = [], 0
    for count, order in plan:
        if count:
            pieces.append((start, count * unit, order))
        start += count * unit
    return pieces


def flows_of(blocks, width, basis_rows, sizes):
    long_axis = max(range(3), key=lambda d: sizes[d])
    one, two = [d for d in range(3) if d != long_axis]
    devices = math.prod(sizes)
    flows = []
    for k in range(blocks):
        tail = basis_rows // 64 if 0 < k < blocks - 1 else 0
        flows += [("q", k) + piece for piece in split(basis_rows, 16, sizes, k, tail)]
    for k in range(blocks):
        order = (long_axis, two, one) if k % 2 else (long_axis, one, two)
        flows.append(("g", k, 0, (k + 1) * width // devices, order))
    for k in range(blocks):
        pieces = split(width, 16, sizes, k, width // 128)
        flows += [("s", k, k * width + start, rows, order) for start, rows, order in pieces]
    return flows


BLEND, PROJECT, TRACE, FACTOR, SCALE, TELL, HEAR = -1, -2, -3, -4, -5, -6, -7


TUNED = (
    0, 20, 10, 50, 51, -10, 21, 40, 1, 11, 70, 2, 90, 30, 41, 12, 60, 71, 91, 61,
    80, 31, 13, 52, 42, 3, -20, 32, 22, 81, 100, 43, 62, 72, 101, 73, 23, 82, 33, -21,
    92, 53, 102, 63, 110, -22, 120, 103, 83, 111, 93, -23, 121, 130, -30, 104, 112, 122, 131, 105,
    113, 132, 123, 106, -40, 114, 124, 140, 160, 133, 150, 115, 141, 161, 151, 125, 116, 134, -41, 162,
    126, 135, 170, 180, 152, 190, -42, 136, 200, 191, 163, 181, 220, 210, 153, -43, 240, 201, 192, 250,
    182, 230, 154, 211, 164, 193, 221, 251, 171, 183, 241, 212, 172, 222, 142, 202, 231, 184, 242, 203,
    173, 194, 165, 252, 155, 223, 143, 232, 213, 195, 185, 243, 174, 144, 253, 233, 204, 224, 214, 244,
    234, 196, 166, 254, 215, 225, 145, 175, 205, 245, 235, 255, 216, 176, 146, 226, 156, 186, -51, -50,
    256, 206, -52, 246, 236, -53,
)


def tuned_agenda(flows, blocks):
    steps = [divmod(code, 10) if code >= 0 else (-(-code // 10), -code % 10) for code in TUNED]
    plain = agenda(flows, blocks)
    known = sorted(step for step in steps if step[0] > TELL)
    return steps if known == sorted(plain) else plain


def agenda(flows, blocks):
    steps = [(0.5, (BLEND, 0))]
    begun = 9.0 * (blocks - 1) + 17
    for f, (kind, k, _, _, _) in enumerate(flows):
        if kind == "q":
            steps += [(9.0 * k + (0, 6, 10, 16)[stage], (f, stage)) for stage in range(4)]
        elif kind == "g" and k < blocks - 1:
            steps += [(9.0 * k + 17.01 + 3.0 * stage, (f, stage)) for stage in range(7)]
        elif kind == "g":
            late = (0, 3, 12.9, 13, 21.4, 21.5, 29.9)
            steps += [(begun + 0.02 + late[stage], (f, stage)) for stage in range(7)]
        else:
            steps += [(begun + 4.6 + 8.5 * (k + stage), (f, stage)) for stage in range(7)]
    for k in range(blocks):
        steps.append((9.0 * k + 16.5, (PROJECT, k)))
        steps.append((begun + 4 + 8.5 * k, (FACTOR, k)))
        steps.append((begun + 4.7 + 8.5 * (k + 6), (SCALE, k)))
    steps.append((begun + 0.1, (TRACE, 0)))
    steps.sort(key=lambda step: step[0])
    needs = {}
    need = lambda step, other: needs.setdefault(step, []).append(other)
    for f, (kind, k, _, _, _) in enumerate(flows):
        final = 3 if kind == "q" else 6
        for stage in range(final):
            need((f, stage + 1), (f, stage))
        if kind == "q":
            need((PROJECT, k), (f, final))
        elif kind == "g":
            need((f, 0), (PROJECT, k))
            need((FACTOR, k), (f, final))
        else:
            need((f, 0), (FACTOR, k))
            need((SCALE, k), (f, final))
    for k in range(blocks):
        need((PROJECT, k), (BLEND, 0))
        need((TRACE, 0), (PROJECT, k))
        need((FACTOR, k), (TRACE, 0))
        if k:
            need((PROJECT, k), (PROJECT, k - 1))
            need((FACTOR, k), (FACTOR, k - 1))
    order, done = [], set()

    def emit(step):
        if step not in done:
            for other in needs.get(step, ()):
                emit(other)
            done.add(step)
            order.append(step)

    for _, step in steps:
        emit(step)
    return order


def main_kernel(sizes, parts, flows, width, m_ref, g_ref, q_ref, o_ref, t_ref, qn_ref, m_buf, *scratch):
    mine = position(sizes)
    me = lax.axis_index("fsdp")
    devices = math.prod(sizes)
    rows, columns = m_ref.shape
    features, size = q_ref.shape
    blocks = size // width
    refs = list(scratch)
    take = lambda n: [refs.pop(0) for _ in range(n)]
    landing, sums = {}, {}
    for f, flow in enumerate(flows):
        if flow[0] != "q":
            landing[f] = take(3)
            sums[f] = take(2)
    grams = take(blocks)
    spreads = take(blocks)
    (g_buf, q_buf, b_ref, basis, p_ref, trace_own, trace_all, u_ref, x_ref, d_ref) = take(10)
    (terms, ot_ref, own_ref, gram_ref) = take(4)
    (in_sem, trace_send, trace_recv, rs_send, rs_recv, ag_send, ag_recv, pace) = take(8)
    base = [0, sizes[0] - 1, sizes[0] + sizes[1] - 2]
    each = sum(sizes) - 3
    basis_flows = sum(flow[0] == "q" for flow in flows)
    shared_slots = max(basis_flows, len(flows) - basis_flows - blocks)

    def slot_of(f, summing):
        kind = flows[f][0]
        if summing:
            return f - basis_flows
        return {"q": f, "g": shared_slots + f - basis_flows, "s": f - basis_flows - blocks}[kind]

    loads = [
        pltpu.make_async_copy(q_ref, q_buf, in_sem.at[0]),
        pltpu.make_async_copy(m_ref, m_buf, in_sem.at[1]),
        pltpu.make_async_copy(g_ref, g_buf, in_sem.at[2]),
    ]
    for load in loads:
        load.start()
    barrier = pltpu.get_barrier_semaphore()
    for off in range(1, devices):
        other = {"fsdp": lax.rem(me + off, devices)}
        pl.semaphore_signal(barrier, inc=1, device_id=other, device_id_type=MESH)
    part = lax.axis_index("mat")
    paired = parts == 2
    if paired:
        pl.semaphore_signal(barrier, inc=1, device_id={"mat": 1 - part}, device_id_type=MESH)
    loads[0].wait()
    for k in range(blocks):
        basis[k, mine[0], mine[1], mine[2]] = q_buf[:, k * width : (k + 1) * width].astype(basis.dtype)
    pl.semaphore_wait(barrier, devices - 1 + paired)
    sent = []

    kinds = ("q", "g", "s")

    def push(source, target, sems, f, d, off):
        summing = sems[0] is rs_send
        at = each * slot_of(f, summing) + base[d] + off - 1
        kind = flows[f][0]
        if kind == "g":
            gram_at = each * (2 * (f - basis_flows) + summing) + base[d] + off - 1
            send_sem = rs_send.at[gram_at]
        else:
            send_sem = ag_send.at[kinds.index(kind) + summing]
        copy = pltpu.make_async_remote_copy(
            src_ref=source,
            dst_ref=target,
            send_sem=send_sem,
            recv_sem=sems[1].at[at],
            device_id=device_at(mine, sizes, d, shifted(mine, sizes, d, off)),
            device_id_type=MESH,
        )
        copy.start()
        if kind == "g":
            sent.append(copy)

    def landed(ref, sem, f, d, off):
        at = each * slot_of(f, sem is rs_recv) + base[d] + off - 1
        pltpu.make_async_copy(ref, ref, sem.at[at]).wait()

    def block(f, phase, coordinate):
        kind, k, start, part, order = flows[f]
        index = list(mine)
        index[order[phase]] = coordinate
        for d in order[:phase]:
            index[d] = slice(None)
        if kind == "q":
            return basis.at[k, index[0], index[1], index[2], pl.ds(start, part)]
        target = spreads[k] if kind == "g" else o_ref
        return target.at[index[0], index[1], index[2], pl.ds(start, part)]

    def spread(f, phase):
        d = flows[f][4][phase]
        here = block(f, phase, mine[d])
        for off in range(1, sizes[d]):
            push(here, here, (ag_send, ag_recv), f, d, off)

    def gathered(f, phase):
        d = flows[f][4][phase]
        for off in range(1, sizes[d]):
            landed(block(f, phase, shifted(mine, sizes, d, sizes[d] - off)), ag_recv, f, d, off)

    def source(f):
        return grams[flows[f][1]] if flows[f][0] == "g" else terms

    def begin(f):
        _, _, start, part, order = flows[f]
        d = order[2]
        for off in range(1, sizes[d]):
            index = [slice(None)] * 3
            index[d] = shifted(mine, sizes, d, off)
            piece = source(f).at[index[0], index[1], index[2], pl.ds(start, part)]
            push(piece, landing[f][0].at[off - 1], (rs_send, rs_recv), f, d, off)

    def first_sums(f):
        _, _, start, part, (a, b, c) = flows[f]
        from_ref = source(f)
        for off in range(1, sizes[c]):
            landed(landing[f][0].at[off - 1], rs_recv, f, c, off)
        low, high = min(a, b), max(a, b)
        for off in list(range(1, sizes[b])) + [0]:
            at_b = shifted(mine, sizes, b, off)

            def one(at_a, _, off=off, at_b=at_b):
                index = [None] * 3
                index[a], index[b], index[c] = at_a, at_b, mine[c]
                total = from_ref[index[0], index[1], index[2], pl.ds(start, part)].astype(jnp.float32)
                for k in range(sizes[c] - 1):
                    total += landing[f][0][k, index[low], index[high]].astype(jnp.float32)
                if off:
                    sums[f][0][off - 1, at_a] = total.astype(from_ref.dtype)
                else:
                    sums[f][1][at_a] = total
                return 0

            lax.fori_loop(0, sizes[a], one, 0)
        for off in range(1, sizes[b]):
            push(sums[f][0].at[off - 1], landing[f][1].at[off - 1], (rs_send, rs_recv), f, b, off)

    def second_sums(f):
        _, _, start, part, (a, b, c) = flows[f]
        for off in range(1, sizes[b]):
            landed(landing[f][1].at[off - 1], rs_recv, f, b, off)
        last = landing[f][2]
        for off in list(range(1, sizes[a])) + [0]:
            at_a = shifted(mine, sizes, a, off)
            total = sums[f][1][at_a]
            for k in range(sizes[b] - 1):
                total += landing[f][1][k, at_a].astype(jnp.float32)
            if off:
                last[sizes[a] - 1 + off - 1] = total.astype(last.dtype)
            else:
                sums[f][1][at_a] = total
        for off in range(1, sizes[a]):
            push(last.at[sizes[a] - 1 + off - 1], last.at[off - 1], (rs_send, rs_recv), f, a, off)

    def last_sums(f):
        kind, k, start, part, (a, b, c) = flows[f]
        for off in range(1, sizes[a]):
            landed(landing[f][2].at[off - 1], rs_recv, f, a, off)
        total = sums[f][1][mine[a]]
        for n in range(sizes[a] - 1):
            total += landing[f][2][n].astype(jnp.float32)
        if kind == "s":
            own_ref[pl.ds(start, part), :] = total
            o_ref[mine[0], mine[1], mine[2], pl.ds(start, part)] = total.astype(o_ref.dtype)
        else:
            spreads[k][mine[0], mine[1], mine[2]] = total

    def spot(i):
        return (
            lax.div(i, sizes[1] * sizes[2]),
            lax.rem(lax.div(i, sizes[2]), sizes[1]),
            lax.rem(i, sizes[2]),
        )

    def lanes_of(i):
        return pl.ds(pl.multiple_of(i * features, features), features)

    def blend():
        loads[1].wait()
        loads[2].wait()

        def one(i, _):
            lanes = lanes_of(i)
            blended = m_buf[:, lanes] + g_buf[:, lanes].astype(jnp.float32)
            m_buf[:, lanes] = blended
            b_ref[:, lanes] = blended.astype(b_ref.dtype)
            return 0

        lax.fori_loop(0, devices, one, 0)

    def project(k):
        top, end = k * width, (k + 1) * width
        right = basis[k].reshape(columns, width)
        p_ref[:, top:end] = jnp.dot(b_ref[...], right, preferred_element_type=jnp.float32)
        if end == size:
            send_trace()
        column = dot_first(p_ref[:, :end], p_ref[:, top:end])
        part = end // devices
        for i in range(devices):
            at = (i // (sizes[1] * sizes[2]), i // sizes[2] % sizes[1], i % sizes[2])
            grams[k][at[0], at[1], at[2]] = column[i * part : (i + 1) * part]

    def send_trace():
        square = p_ref[...] * p_ref[...]
        folded = square[:, :128]
        for i in range(1, size // 128):
            folded = folded + square[:, i * 128 : (i + 1) * 128]
        tile = folded[:8]
        for i in range(1, rows // 8):
            tile = tile + folded[i * 8 : (i + 1) * 8]
        trace_own[...] = tile
        trace_all[me] = tile
        for off in range(1, devices):
            copy = pltpu.make_async_remote_copy(
                src_ref=trace_own,
                dst_ref=trace_all.at[me],
                send_sem=trace_send.at[off],
                recv_sem=trace_recv.at[off],
                device_id={"fsdp": lax.rem(me + off, devices)},
                device_id_type=MESH,
            )
            copy.start()
            sent.append(copy)

    def ridge():
        for off in range(1, devices):
            here = trace_all.at[lax.rem(me + devices - off, devices)]
            pltpu.make_async_copy(here, here, trace_recv.at[off]).wait()
        return jnp.sum(jnp.sum(trace_all[...], axis=0), keepdims=True) * (0.0001 / size)

    small_eye = lax.broadcasted_iota(jnp.int32, (width, width), 0) == lax.broadcasted_iota(
        jnp.int32, (width, width), 1
    )
    shared = {}

    def factor(k):
        top, end = k * width, (k + 1) * width
        if k == 0:
            shared["ridge"] = ridge()
        gram_ref[:end, :] = spreads[k][...].reshape(end, width)
        for j in range(k):
            near, far = j * width, (j + 1) * width
            upper = gram_ref[near:far, :]
            if j:
                upper = upper - dot_first(u_ref[:near, near:far], u_ref[:near, top:end])
            u_ref[near:far, top:end] = jnp.dot(x_ref[near:far, near:far], upper, precision=HIGHEST)
        corner = gram_ref[top:end, :] + jnp.where(small_eye, shared["ridge"], 0.0)
        if k:
            panel = u_ref[:top, top:end]
            corner = corner - dot_first(panel, panel)
        inverse = factor_block(width, d_ref, corner)
        x_ref[top:end, top:end] = inverse
        if k:
            rest = dot_first(u_ref[:top, top:end], x_ref[:top, :top])
            x_ref[top:end, :top] = -jnp.dot(inverse, rest, precision=HIGHEST)
        if end < size:
            x_ref[top:end, end:] = jnp.zeros((width, size - end), jnp.float32)
        ortho = nt_dot(x_ref[top:end, :end], p_ref[:, :end], HIGHEST)
        ot_ref[top:end, :] = ortho
        t_ref[:rows, top:end] = ortho.T.astype(t_ref.dtype)
        low = ortho.astype(jnp.bfloat16)

        each_step = math.gcd(devices, 4)

        def one(i, _):
            for n in range(each_step):
                at = spot(i * each_step + n)
                lanes = lanes_of(i * each_step + n)
                term = jnp.dot(low, b_ref[:, lanes], preferred_element_type=jnp.float32)
                terms[at[0], at[1], at[2], top:end] = term.astype(terms.dtype)
            return 0

        lax.fori_loop(0, devices // each_step, one, 0)

    def scale_block(k):
        top, end = k * width, (k + 1) * width

        def squares(i, total):
            at = spot(i)
            wide = o_ref[at[0], at[1], at[2], top:end].astype(jnp.float32)
            return total + wide * wide

        total = lax.fori_loop(0, devices, squares, jnp.zeros((width, features), jnp.float32))
        mean = jnp.sum(total, axis=1, keepdims=True) / (devices * features)
        column_rms = jnp.sqrt(mean + epsilon)
        qn_ref[top:end, :] = own_ref[top:end, :] / column_rms
        t_ref[rows:, top:end] = (ot_ref[top:end, :] / column_rms).T.astype(t_ref.dtype)

    def serve(f, stage):
        if flows[f][0] != "q":
            if stage < 4:
                (begin, first_sums, second_sums, last_sums)[stage](f)
            if stage < 3:
                return
            stage = stage - 3
        if stage:
            gathered(f, stage - 1)
        if stage < 3:
            spread(f, stage)

    def tell(n):
        if paired:

            @pl.when(part == n % 2)
            def _():
                pl.semaphore_signal(pace.at[n], inc=1, device_id={"mat": 1 - part}, device_id_type=MESH)

    def hear(n):
        if paired:

            @pl.when(part != n % 2)
            def _():
                pl.semaphore_wait(pace.at[n], 1)

    special = {
        BLEND: lambda k: blend(),
        PROJECT: project,
        TRACE: lambda k: None,
        FACTOR: factor,
        SCALE: scale_block,
        TELL: tell,
        HEAR: hear,
    }
    for what, stage in tuned_agenda(flows, blocks):
        if what < 0:
            special[what](stage)
        else:
            serve(what, stage)
        if (what, stage) == (FACTOR, blocks - 1):
            while sent:
                sent.pop().wait_send()
    shares = size // devices * (devices - 1)
    everything = terms.at[:, :, :, pl.ds(0, shares)]
    for n in (0, 2, 3):
        pltpu.make_async_copy(everything, everything, ag_send.at[n]).wait()


def right_factor(momentum, grad, q_basis, sizes, parts, number):
    rows, columns = momentum.shape
    features, size = q_basis.shape
    width = 128
    blocks = size // width
    devices = math.prod(sizes)
    flows = flows_of(blocks, width, features, sizes)
    low_type = jnp.bfloat16
    many = lambda k: max(k, 1)
    scratch = []
    for kind, _, _, part, (a, b, c) in flows:
        if kind == "q":
            continue
        low, high = min(a, b), max(a, b)
        lanes, kept = (width, jnp.float32) if kind == "g" else (features, low_type)
        scratch += [
            pltpu.VMEM((many(sizes[c] - 1), sizes[low], sizes[high], part, lanes), kept),
            pltpu.VMEM((many(sizes[b] - 1), sizes[a], part, lanes), kept),
            pltpu.VMEM((many(2 * (sizes[a] - 1)), part, lanes), kept),
            pltpu.VMEM((many(sizes[b] - 1), sizes[a], part, lanes), kept),
            pltpu.VMEM((sizes[a], part, lanes), jnp.float32),
        ]
    chunks = [pltpu.VMEM(sizes + ((k + 1) * width // devices, width), jnp.float32) for k in range(blocks)]
    sums_flows = sum(flow[0] != "q" for flow in flows)
    slots = blocks + max(len(flows) - sums_flows, sums_flows - blocks)
    sems = pltpu.SemaphoreType.DMA((slots * (sum(sizes) - 3),))
    sum_sems = pltpu.SemaphoreType.DMA((sums_flows * (sum(sizes) - 3),))
    scratch += chunks + chunks
    scratch += [
        pltpu.VMEM((rows, columns), low_type),
        pltpu.VMEM((features, size), jnp.float32),
        pltpu.VMEM((rows, columns), low_type),
        pltpu.VMEM((blocks,) + sizes + (features, width), low_type),
        pltpu.VMEM((rows, size), jnp.float32),
        pltpu.VMEM((8, 128), jnp.float32),
        pltpu.VMEM((devices, 8, 128), jnp.float32),
        pltpu.VMEM((size, size), jnp.float32),
        pltpu.VMEM((size, size), jnp.float32),
        pltpu.VMEM((width, 2 * width), jnp.float32),
        pltpu.VMEM(sizes + (size, features), low_type),
        pltpu.VMEM((size, rows), jnp.float32),
        pltpu.VMEM((size, features), jnp.float32),
        pltpu.VMEM((size, width), jnp.float32),
        pltpu.SemaphoreType.DMA((3,)),
        pltpu.SemaphoreType.DMA((devices,)),
        pltpu.SemaphoreType.DMA((devices,)),
        pltpu.SemaphoreType.DMA((2 * blocks * (sum(sizes) - 3),)),
        sum_sems,
        pltpu.SemaphoreType.DMA((4,)),
        sems,
        pltpu.SemaphoreType.REGULAR((4,)),
    ]
    vmem = pl.BlockSpec(memory_space=pltpu.VMEM)
    return pl.pallas_call(
        functools.partial(main_kernel, sizes, parts, flows, width),
        out_shape=(
            pltpu.VMEM(sizes + (size, features), low_type),
            pltpu.VMEM((2 * rows, size), low_type),
            pltpu.VMEM((size, features), jnp.float32),
            pltpu.VMEM((rows, columns), jnp.float32),
        ),
        in_specs=[pl.BlockSpec(memory_space=pltpu.HBM)] * 3,
        out_specs=(vmem, vmem, vmem, vmem),
        scratch_shapes=scratch,
        compiler_params=pltpu.CompilerParams(
            collective_id=number, has_side_effects=True, vmem_limit_bytes=48 * 2**20
        ),
        name=f"factor_{number}",
    )(momentum, grad, q_basis)


def finish_kernel(step, factor, s_ref, t_ref, q_ref, m_ref, mo_ref, uo_ref, qo_ref, m_buf, u_buf, q_buf, m_sem, u_sem, q_sem):
    rows = m_ref.shape[0]
    blocks, rank, features = s_ref.shape
    q_buf[...] = q_ref[...].T
    q_copy = pltpu.make_async_copy(q_buf, qo_ref, q_sem)
    q_copy.start()

    def copies(slot, i):
        lanes = pl.ds(pl.multiple_of(i * features, features), features)
        return (
            pltpu.make_async_copy(m_buf.at[slot], mo_ref.at[:, lanes], m_sem.at[slot]),
            pltpu.make_async_copy(u_buf.at[slot], uo_ref.at[:, lanes], u_sem.at[slot]),
        )

    slots = m_buf.shape[0]
    wide = math.gcd(blocks, slots // 2)

    def one(step_index, _):
        for n in range(wide):
            i = step_index * wide + n
            slot = lax.rem(i, slots)

            @pl.when(i >= slots)
            def _(slot=slot, i=i):
                for copy in copies(slot, i - slots):
                    copy.wait()

        results = [
            jnp.dot(t_ref[...], s_ref[step_index * wide + n], preferred_element_type=jnp.float32)
            for n in range(wide)
        ]
        for n in range(wide):
            i = step_index * wide + n
            slot = lax.rem(i, slots)
            lanes = pl.ds(pl.multiple_of(i * features, features), features)
            m_buf[slot] = m_ref[:, lanes] - step * results[n][:rows]
            u_buf[slot] = (factor * results[n][rows:]).astype(u_buf.dtype)
            for copy in copies(slot, i):
                copy.start()
        return 0

    lax.fori_loop(0, blocks // wide, one, 0)
    for i in range(max(blocks - slots, 0), blocks):
        for copy in copies(i % slots, i):
            copy.wait()
    q_copy.wait()


def finish(spread, stacked, turned, blended, factor):
    rows, columns = blended.shape
    blocks, rank, features = spread.shape
    vmem = pl.BlockSpec(memory_space=pltpu.VMEM)
    anywhere = pl.BlockSpec(memory_space=pl.ANY)
    slots = 8
    return pl.pallas_call(
        functools.partial(finish_kernel, 1.0 - damping, factor),
        out_shape=(
            jax.ShapeDtypeStruct((rows, columns), jnp.float32),
            jax.ShapeDtypeStruct((rows, columns), jnp.bfloat16),
            jax.ShapeDtypeStruct((features, rank), jnp.float32),
        ),
        in_specs=[vmem] * 4,
        out_specs=(anywhere,) * 3,
        scratch_shapes=[
            pltpu.VMEM((slots, rows, features), jnp.float32),
            pltpu.VMEM((slots, rows, features), jnp.bfloat16),
            pltpu.VMEM((features, rank), jnp.float32),
            pltpu.SemaphoreType.DMA((slots,)),
            pltpu.SemaphoreType.DMA((slots,)),
            pltpu.SemaphoreType.DMA,
        ],
        compiler_params=pltpu.CompilerParams(vmem_limit_bytes=16 * 2**20),
        name="finish",
    )(spread, stacked, turned, blended)


def inverse_kernel(size, width, g_ref, x_ref, a_ref, d_ref):
    eye = lax.broadcasted_iota(jnp.int32, (size, size), 0) == lax.broadcasted_iota(
        jnp.int32, (size, size), 1
    )
    gram = g_ref[...]
    trace = jnp.sum(jnp.where(eye, gram, 0.0), keepdims=True)
    a_ref[...] = gram + jnp.where(eye, 0.0001 * trace / size, 0.0)
    x_ref[...] = jnp.where(eye, 1.0, 0.0)
    strip = lax.broadcasted_iota(jnp.int32, (8, width), 0)
    lane = lax.broadcasted_iota(jnp.int32, (8, width), 1)
    small_eye = jnp.where(
        lax.broadcasted_iota(jnp.int32, (width, width), 0)
        == lax.broadcasted_iota(jnp.int32, (width, width), 1),
        1.0,
        0.0,
    )

    def group(g, _):
        first = pl.multiple_of(g * 8, 8)
        left = d_ref[pl.ds(first, 8), :width]
        right = d_ref[pl.ds(first, 8), width:]
        turned = pltpu.roll(left, lax.rem(width - first, width), 1)
        columns = [jnp.broadcast_to(turned[:, j : j + 1], (8, width)) for j in range(8)]
        for j in range(8):
            scale = lax.rsqrt(columns[j][j : j + 1, :])
            factor = columns[j] * scale
            for m in range(j + 1, 8):
                columns[m] = columns[m] - factor * factor[m : m + 1, :]
            row_left, row_right = left[j : j + 1, :] * scale, right[j : j + 1, :] * scale
            below, here = strip > j, strip == j
            left = jnp.where(here, row_left, jnp.where(below, left - factor * row_left, left))
            right = jnp.where(here, row_right, jnp.where(below, right - factor * row_right, right))
        later = jnp.where(lane >= first + 8, left, 0.0)
        both = jnp.concatenate([left, right], axis=1)
        d_ref[pl.ds(first, 8), :] = both
        d_ref[...] = d_ref[...] - short_dot(later, both)
        return 0

    for k in range(size // width):
        top, end = k * width, (k + 1) * width
        d_ref[:, :width] = a_ref[top:end, top:end]
        d_ref[:, width:] = small_eye
        lax.fori_loop(0, width // 8, group, 0)
        corner = d_ref[:, width:]
        done = jnp.dot(corner, x_ref[top:end, :end], precision=HIGHEST)
        x_ref[top:end, :end] = done
        if end < size:
            panel = jnp.dot(corner, a_ref[top:end, end:], precision=HIGHEST)
            a_ref[end:, end:] = a_ref[end:, end:] - dot_first(panel, panel)
            x_ref[end:, :end] = x_ref[end:, :end] - dot_first(panel, done)


def lower_inverse(gram_total):
    size = gram_total.shape[0]
    width = 128
    return pl.pallas_call(
        functools.partial(inverse_kernel, size, width),
        out_shape=jax.ShapeDtypeStruct((size, size), jnp.float32),
        in_specs=[pl.BlockSpec(memory_space=pltpu.VMEM)],
        out_specs=pl.BlockSpec(memory_space=pltpu.VMEM),
        scratch_shapes=[
            pltpu.VMEM((size, size), jnp.float32),
            pltpu.VMEM((width, 2 * width), jnp.float32),
        ],
        compiler_params=pltpu.CompilerParams(vmem_limit_bytes=24 * 2**20),
        name="lower_inverse",
    )(gram_total)


def narrow_device(sizes, momentum, grad, q_basis):
    own_rows = momentum.shape[0]
    basis_rows, rank = q_basis.shape
    devices = math.prod(sizes)
    features = basis_rows * devices
    blended = momentum + grad.astype(jnp.float32)
    blended_low = blended.astype(jnp.bfloat16)
    basis = gather(q_basis.astype(jnp.bfloat16), sizes, 0)
    projected = jnp.dot(blended_low, basis, preferred_element_type=jnp.float32)
    local_gram = jnp.dot(projected.T, projected, precision=HIGHEST)
    gram_total = gather(reduce_scatter(local_gram, sizes, 1), sizes, 2)
    inverse = lower_inverse(gram_total)
    orthonormal = jnp.dot(projected, inverse.T, precision=HIGHEST)
    ortho_low = orthonormal.astype(jnp.bfloat16)
    terms = jnp.dot(blended_low.T, ortho_low, preferred_element_type=jnp.float32)
    summed = reduce_scatter(terms.astype(jnp.bfloat16), sizes, 3)
    summed_low = gather(summed.astype(jnp.bfloat16), sizes, 4)
    wide = summed_low.astype(jnp.float32)
    column_rms = jnp.sqrt(jnp.mean(wide * wide, axis=0) + epsilon)
    q_next = summed / column_rms
    stacked = jnp.concatenate(
        [ortho_low, (orthonormal / column_rms).astype(jnp.bfloat16)], axis=0
    )
    result = jnp.dot(stacked, summed_low.T, preferred_element_type=jnp.float32)
    total_rows = own_rows * devices
    momentum_next = blended - (1.0 - damping) * result[:own_rows]
    update = (math.sqrt(total_rows * features / rank) * result[own_rows:]).astype(jnp.bfloat16)
    return (momentum_next, update, q_next)


def per_device(sizes, parts, momentum, grad, q_basis):
    own_rows = momentum.shape[0]
    basis_rows, rank = q_basis.shape
    if basis_rows % 128 or rank % 128 or own_rows % 128:
        return narrow_device(sizes, momentum, grad, q_basis)
    devices = math.prod(sizes)
    features = basis_rows * devices
    spread, stacked, turned, blended = right_factor(momentum, grad, q_basis, sizes, parts, 0)
    total_rows = own_rows * devices
    factor = math.sqrt(total_rows * features / rank)
    spread = spread.reshape(devices, rank, basis_rows)
    return finish(spread, stacked, turned, blended, factor)


def solution(mesh):
    spec = P(("mat", "fsdp"), None)
    return jax.shard_map(
        functools.partial(per_device, grid_of(mesh), mesh.shape["mat"]),
        mesh=mesh,
        in_specs=(spec, spec, spec),
        out_specs=(spec, spec, spec),
        check_vma=False,
    )
```
